32 devices in a mesh: lat: 2 (over y), lon: 4 (over x, core), lev: 4 (over z).
Axes of the slice: x: 2, y: 2, z: 4, core: 2. Of those that a mesh axis runs over, the one named last changes fastest.
Arguments:
- tracer: float32 [8, 512, 128, 128], P('lat', 'lon', 'lev'), may hold values from 0.5 to 2
- conductance: float32 [8, 512, 128, 128], P('lat', 'lon', 'lev'), may hold values from 0.03 to 0.15
- source: float32 [8, 512, 128, 128], P('lat', 'lon', 'lev'), may hold values from -0.2 to 0.2
Outputs:
- standardized: float32 [8, 512, 128, 128], P('lat', 'lon', 'lev')
- tracer_end: float32 [8, 512, 128, 128], P('lat', 'lon', 'lev')
The draws below stay inside these ranges and needn't reach their ends.
All inputs are finite; a program needn't handle non-finite values.
Results may differ from the reference program's by a relative error of at most 0.00002.
Values sent between devices are 32-bit elements; how exact they have to be, the bound alone decides.
A program may use at most 128 MiB of HBM per device.

```python
import jax
import jax.numpy as jnp
from jax import lax

GRID_J = 8
GRID_I = 512
GRID_K = 128
MEMBERS = 128
STEPS = 3


def shard_levels(stream_key, extent, cuts, smallest, top_value):
    def one(dim, shards_of):
        draws = jax.random.uniform(jax.random.fold_in(jax.random.fold_in(stream_key, 6), dim), (shards_of,), jnp.float32, smallest / len(cuts), top_value / len(cuts))
        return jnp.repeat(jnp.exp(draws), extent[dim] // shards_of).reshape((-1,) + (1,) * (len(extent) - dim - 1))

    level = one(*cuts[0])
    for cut in cuts[1:]:
        level = level * one(*cut)
    return level


def setup_inputs(seed: int = 0) -> dict:
    seeds = jax.random.split(jax.random.key(seed), 4)
    return {
        "tracer": jnp.clip(0.5 + 1.5 * jax.random.uniform(seeds[0], (GRID_J, GRID_I, GRID_K, MEMBERS), jnp.float32) ** shard_levels(seeds[0], (GRID_J, GRID_I, GRID_K, MEMBERS), ((0, 2), (1, 4), (2, 4)), -0.2, 0.2), 0.5, 2.0),
        "conductance": jnp.clip(0.03 + 0.120000007 * jax.random.uniform(seeds[1], (GRID_J, GRID_I, GRID_K, MEMBERS), jnp.float32) ** shard_levels(seeds[1], (GRID_J, GRID_I, GRID_K, MEMBERS), ((0, 2), (1, 4), (2, 4)), -0.2, 0.2), 0.03, 0.15),
        "source": jnp.clip(jax.random.uniform(seeds[2], (GRID_J, GRID_I, GRID_K, MEMBERS), jnp.float32, -0.2, 0.2) * shard_levels(seeds[2], (GRID_J, GRID_I, GRID_K, MEMBERS), ((0, 2), (1, 4), (2, 4)), -0.4, 0.0), -0.2, 0.2),
    }


def inner_cells(values, dims):
    for dim in dims:
        values = lax.slice_in_dim(values, 1, values.shape[dim] - 1, axis=dim)
    return values

def side_cells(values, dim, start, dims):
    others = [other for other in dims if other != dim]
    values = inner_cells(values, others)
    return lax.slice_in_dim(values, start, start + values.shape[dim] - 2, axis=dim)

def advance(padded, conductance, source):
    middle = inner_cells(padded, (0, 1, 2))
    lower = [side_cells(padded, dim, 0, (0, 1, 2)) for dim in (0, 1, 2)]
    upper = [side_cells(padded, dim, 2, (0, 1, 2)) for dim in (0, 1, 2)]
    spread = lower[0] + upper[0] + lower[1] + upper[1] + lower[2] + upper[2] - 6.0 * middle
    return middle + conductance * spread + source

def reference(tracer, conductance, source):
    for step in range(STEPS):
        tracer = advance(jnp.pad(tracer, ((1, 1), (1, 1), (1, 1), (0, 0)), mode='constant'), conductance, source)
    line_mean = lax.optimization_barrier(jnp.mean(tracer, axis=1, keepdims=True))
    centred = tracer - line_mean
    line_variance = lax.optimization_barrier(jnp.mean(centred * centred, axis=1, keepdims=True))
    standardized = centred * lax.rsqrt(line_variance + 0.0001)
    return (standardized, tracer)
```

```python
import functools

import jax
import jax.numpy as jnp
from jax import lax
from jax.experimental import pallas as pl
from jax.experimental.pallas import tpu as pltpu
from jax.sharding import PartitionSpec as P

STEPS = 3
GUESS = 1.0
TILE = 8
ROWS = 8
MESH = pl.DeviceIdType.MESH


def lat_sides(n_lat, lat, J):
    if n_lat == 2:
        return [(jnp.where(lat == 0, J - 1, 0), jnp.where(lat == 0, J - 2, 1), 1 - lat, None, 0)]
    return [(0, 1, lat - 1, lat > 0, 1), (J - 1, J - 2, lat + 1, lat < n_lat - 1, 0)]


def early_planes(n_lat, lat, J):
    if n_lat == 2:
        return jnp.where(lat == 0, 0, 1), J - 1
    return 1, J - 2


def when(condition, act):
    if condition is None:
        act()
    else:
        pl.when(condition)(act)


def kernel(
    sizes, tracer, conductance, source, end, mean_out, scale_out,
    even, odd, cond, sour, base, y_halo, z_lower, z_upper, z_first, z_last,
    sums_early, peer_early, sums_late, peer_late,
    load_sem, y_send, y_recv, x_send, x_recv, z_send, z_recv, early_send, early_recv, late_send, late_recv,
):
    n_lat, n_lon, n_lev = sizes
    J, I, K, M = tracer.shape
    chunks = K // TILE
    blocks = I // ROWS
    count = I * n_lon
    lat, lon, lev = lax.axis_index("lat"), lax.axis_index("lon"), lax.axis_index("lev")
    below = {"lon": lon > 0, "lev": lev > 0}
    above = {"lon": lon < n_lon - 1, "lev": lev < n_lev - 1}
    index = {"lon": lon, "lev": lev}
    field = [even, odd]
    sides = lat_sides(n_lat, lat, J)
    first, number = early_planes(n_lat, lat, J)
    rows_in = pl.ds(1, I)

    def levels(chunk):
        return pl.ds(chunk * TILE, TILE)

    def target(axis, way):
        return {axis: index[axis] + (1 if way == 0 else -1)}

    def y_copy(step, chunk, s):
        plane, _, peer, _, slot = sides[s]
        return pltpu.make_async_remote_copy(
            src_ref=field[step % 2].at[plane, rows_in, levels(chunk), :],
            dst_ref=y_halo.at[step % 2, slot, :, levels(chunk), :],
            send_sem=y_send.at[step, chunk, s], recv_sem=y_recv.at[step, chunk, slot],
            device_id={"lat": peer}, device_id_type=MESH)

    def y_arrival(step, chunk, s):
        plane, _, peer, _, _ = sides[s]
        return pltpu.make_async_remote_copy(
            src_ref=field[step % 2].at[plane, rows_in, levels(chunk), :],
            dst_ref=y_halo.at[step % 2, s, :, levels(chunk), :],
            send_sem=y_send.at[step, chunk, s], recv_sem=y_recv.at[step, chunk, s],
            device_id={"lat": peer}, device_id_type=MESH)

    def x_copy(step, way):
        buf = field[step % 2]
        return pltpu.make_async_remote_copy(
            src_ref=buf.at[:, I if way == 0 else 1],
            dst_ref=buf.at[:, 0 if way == 0 else I + 1],
            send_sem=x_send.at[step, way], recv_sem=x_recv.at[step, way],
            device_id=target("lon", way), device_id_type=MESH)

    def z_copy(step, way):
        src = z_last if way == 0 else z_first
        dst = z_lower if way == 0 else z_upper
        return pltpu.make_async_remote_copy(
            src_ref=src.at[step % 2], dst_ref=dst.at[step % 2],
            send_sem=z_send.at[step, way], recv_sem=z_recv.at[step, way],
            device_id=target("lev", way), device_id_type=MESH)

    def early_copy(shift):
        return pltpu.make_async_remote_copy(
            src_ref=sums_early, dst_ref=peer_early.at[shift - 1],
            send_sem=early_send.at[shift - 1], recv_sem=early_recv.at[shift - 1],
            device_id={"lon": lax.rem(lon + shift, n_lon)}, device_id_type=MESH)

    def late_copy(chunk, shift):
        return pltpu.make_async_remote_copy(
            src_ref=sums_late.at[chunk], dst_ref=peer_late.at[shift - 1, chunk],
            send_sem=late_send.at[chunk, shift - 1], recv_sem=late_recv.at[chunk, shift - 1],
            device_id={"lon": lax.rem(lon + shift, n_lon)}, device_id_type=MESH)

    def sends(axis, way, act):
        pl.when((above if way == 0 else below)[axis])(act)

    def arrives(axis, way, act):
        pl.when((below if way == 0 else above)[axis])(act)

    barrier = pltpu.get_barrier_semaphore()
    met = n_lon - 1
    for _, _, peer, exists, _ in sides:
        when(exists, lambda: pl.semaphore_signal(
            barrier, inc=1, device_id={"lat": peer}, device_id_type=MESH))
        met = met + (1 if exists is None else exists.astype(jnp.int32))
    for way in (0, 1):
        sends("lev", way, lambda: pl.semaphore_signal(
            barrier, inc=1, device_id=target("lev", way), device_id_type=MESH))
        met = met + (above if way == 0 else below)["lev"].astype(jnp.int32)
    for shift in range(1, n_lon):
        pl.semaphore_signal(barrier, inc=1, device_id={"lon": lax.rem(lon + shift, n_lon)},
                            device_id_type=MESH)

    loads = [
        pltpu.make_async_copy(tracer.at[plane], even.at[plane, rows_in], load_sem.at[3 + s])
        for s, (plane, _, _, _, _) in enumerate(sides)
    ]
    loads.append(pltpu.make_async_copy(
        tracer.at[pl.ds(first, number)], even.at[pl.ds(first, number), rows_in], load_sem.at[0]))
    loads.append(pltpu.make_async_copy(conductance, cond, load_sem.at[1]))
    loads.append(pltpu.make_async_copy(source, sour, load_sem.at[2]))
    for load in loads[:-2]:
        load.start()
    for load in loads[:-3]:
        load.wait()
    pl.semaphore_wait(barrier, met)

    for chunk in range(chunks):
        for s, side in enumerate(sides):
            when(side[3], lambda: y_copy(0, chunk, s).start())
    loads[-2].start()
    loads[-1].start()

    for s, side in enumerate(sides):
        if side[3] is not None:
            def no_y():
                @pl.loop(0, blocks)
                def _(b):
                    for p in range(2):
                        y_halo[p, s, pl.ds(b * ROWS, ROWS)] = jnp.zeros((ROWS, K, M), jnp.float32)
            pl.when(jnp.logical_not(side[3]))(no_y)
    for way in (0, 1):
        def no_x():
            for buf in field:
                for j in range(J):
                    buf[j, 0 if way == 0 else I + 1] = jnp.zeros((K, M), jnp.float32)
        pl.when(jnp.logical_not((below if way == 0 else above)["lon"]))(no_x)

        def no_z():
            @pl.loop(0, blocks)
            def _(b):
                for p in range(2):
                    for j in range(J):
                        (z_lower if way == 0 else z_upper)[p, j, pl.ds(b * ROWS, ROWS)] = (
                            jnp.zeros((ROWS, 1, M), jnp.float32))
        pl.when(jnp.logical_not((below if way == 0 else above)["lev"]))(no_z)

    def pack_and_send(step):
        buf = field[step % 2]
        for way in (0, 1):
            sends("lon", way, lambda: x_copy(step, way).start())

        @pl.loop(0, J * blocks)
        def _(q):
            j, r = q // blocks, (q % blocks) * ROWS
            z_first[step % 2, j, pl.ds(r, ROWS)] = buf[j, pl.ds(1 + r, ROWS), pl.ds(0, 1), :]
            z_last[step % 2, j, pl.ds(r, ROWS)] = buf[j, pl.ds(1 + r, ROWS), pl.ds(K - 1, 1), :]

        for way in (0, 1):
            sends("lev", way, lambda: z_copy(step, way).start())

    def next_rows(step, chunk, j, r, inward):
        buf = field[step % 2]
        here = levels(chunk)
        rows = pl.ds(1 + r, ROWS)
        mid = buf[j, rows, here, :]
        k = lax.broadcasted_iota(jnp.int32, mid.shape, 1)
        if chunk == 0:
            edge = jnp.broadcast_to(z_lower[step % 2, j, pl.ds(r, ROWS)], mid.shape)
        else:
            edge = pltpu.roll(buf[j, rows, levels(chunk - 1), :], 1, 1)
        k_lower = jnp.where(k == 0, edge, pltpu.roll(mid, 1, 1))
        if chunk == chunks - 1:
            edge = jnp.broadcast_to(z_upper[step % 2, j, pl.ds(r, ROWS)], mid.shape)
        else:
            edge = pltpu.roll(buf[j, rows, levels(chunk + 1), :], TILE - 1, 1)
        k_upper = jnp.where(k == TILE - 1, edge, pltpu.roll(mid, TILE - 1, 1))
        if inward is None:
            across = buf[j - 1, rows, here, :] + buf[j + 1, rows, here, :]
        else:
            across = buf[inward, rows, here, :]
        spread = (
            across + buf[j, pl.ds(r, ROWS), here, :] + buf[j, pl.ds(2 + r, ROWS), here, :]
            + k_lower + k_upper - 6.0 * mid)
        return mid + cond[j, pl.ds(r, ROWS), here, :] * spread + sour[j, pl.ds(r, ROWS), here, :]

    zero = jnp.zeros((TILE, M), jnp.float32)

    def tally(new, totals):
        moved = new - GUESS
        return totals[0] + jnp.sum(moved, axis=0), totals[1] + jnp.sum(moved * moved, axis=0)

    def early_plane(step, chunk, j, inward):
        def body(b, totals):
            r = b * ROWS
            new = next_rows(step, chunk, j, r, inward)
            if step < STEPS - 1:
                field[(step + 1) % 2][j, pl.ds(1 + r, ROWS), levels(chunk), :] = new
                return totals
            end[j, pl.ds(r, ROWS), levels(chunk), :] = new
            return tally(new, totals)

        if step < STEPS - 1:
            lax.fori_loop(0, blocks, lambda b, _: body(b, 0), 0)
        else:
            totals = lax.fori_loop(0, blocks, body, (zero, zero))
            for q in range(2):
                sums_early[j - first, q, levels(chunk), :] = totals[q]

    def early_part(step, chunk):
        @pl.loop(1, J - 1)
        def _(j):
            early_plane(step, chunk, j, None)

        if n_lat == 2:
            early_plane(step, chunk, jnp.where(lat == 0, 0, J - 1), jnp.where(lat == 0, 1, J - 2))
        for s, (plane, inward, _, _, _) in enumerate(sides):
            @pl.loop(0, blocks)
            def _(b):
                r = b * ROWS
                base[s, pl.ds(r, ROWS), levels(chunk), :] = next_rows(step, chunk, plane, r, inward)

    def late_part(step, chunk, s):
        plane = sides[s][0]
        here = levels(chunk)

        def body(b, totals):
            r = pl.ds(b * ROWS, ROWS)
            new = base[s, r, here, :] + cond[plane, r, here, :] * y_halo[step % 2, s, r, here, :]
            if step < STEPS - 1:
                field[(step + 1) % 2][plane, pl.ds(1 + b * ROWS, ROWS), here, :] = new
                return totals
            end[plane, r, here, :] = new
            return tally(new, totals)

        if step < STEPS - 1:
            lax.fori_loop(0, blocks, lambda b, _: body(b, 0), 0)
        else:
            totals = lax.fori_loop(0, blocks, body, (zero, zero))
            for q in range(2):
                sums_late[chunk, s, q] = totals[q]

    loads[-3].wait()
    pack_and_send(0)
    loads[-2].wait()
    loads[-1].wait()
    for step in range(STEPS):
        if step >= 1:
            for way in (0, 1):
                sends("lon", way, lambda: x_copy(step - 1, way).wait_send())
                sends("lev", way, lambda: z_copy(step - 1, way).wait_send())
            for s, side in enumerate(sides):
                for chunk in range(chunks):
                    when(side[3], lambda: y_copy(step - 1, chunk, s).wait_send())
        for way in (0, 1):
            arrives("lon", way, lambda: x_copy(step, way).wait_recv())
            arrives("lev", way, lambda: z_copy(step, way).wait_recv())
        if step == STEPS - 1:
            for way in (0, 1):
                sends("lon", way, lambda: x_copy(step, way).wait_send())
                sends("lev", way, lambda: z_copy(step, way).wait_send())
            for chunk in range(chunks):
                early_part(step, chunk)
            for shift in range(1, n_lon):
                early_copy(shift).start()
        for chunk in range(chunks):
            if step < STEPS - 1:
                early_part(step, chunk)
            for s, side in enumerate(sides):
                when(side[3], lambda: y_arrival(step, chunk, s).wait_recv())
                late_part(step, chunk, s)
                if step < STEPS - 1:
                    when(side[3], lambda: y_copy(step + 1, chunk, s).start())
            if step == STEPS - 1:
                for shift in range(1, n_lon):
                    late_copy(chunk, shift).start()
        if step < STEPS - 1:
            pack_and_send(step + 1)

    def close(total):
        offset = total[0] / count
        variance = total[1] / count - offset * offset
        return GUESS + offset, lax.rsqrt(variance + 0.0001)

    for shift in range(1, n_lon):
        early_copy(shift).wait_recv()

    @pl.loop(0, number)
    def _(p):
        total = [sums_early[p, q] for q in range(2)]
        for shift in range(1, n_lon):
            total = [total[q] + peer_early[shift - 1, p, q] for q in range(2)]
        mean_out[first + p], scale_out[first + p] = close(total)

    for shift in range(1, n_lon):
        early_copy(shift).wait_send()
    for chunk in range(chunks):
        for s, side in enumerate(sides):
            when(side[3], lambda: y_copy(STEPS - 1, chunk, s).wait_send())
    for chunk in range(chunks):
        for shift in range(1, n_lon):
            if chunk < chunks - 1:
                late_copy(chunk, shift).wait_send()
            late_copy(chunk, shift).wait_recv()
        for s, side in enumerate(sides):
            total = [sums_late[chunk, s, q] for q in range(2)]
            for shift in range(1, n_lon):
                total = [total[q] + peer_late[shift - 1, chunk, s, q] for q in range(2)]
            mean_out[side[0], levels(chunk), :], scale_out[side[0], levels(chunk), :] = close(total)
    for shift in range(1, n_lon):
        late_copy(chunks - 1, shift).wait_send()


def write_out(end, mean, scale, standardized, end_out, held, sem):
    J, I, K, M = end.shape
    copies = [pltpu.make_async_copy(end.at[j], end_out.at[j], sem.at[J + j]) for j in range(J)]
    for copy in copies:
        copy.start()
    for j in range(J):
        offset, factor = mean[j], scale[j]

        @pl.loop(0, I // ROWS)
        def _(b):
            rows = pl.ds(b * ROWS, ROWS)
            held[j, rows] = (end[j, rows] - offset) * factor

        copies.append(pltpu.make_async_copy(held.at[j], standardized.at[j], sem.at[j]))
        copies[-1].start()
    for copy in copies:
        copy.wait()


def shards(sizes, tracer, conductance, source):
    n_lat, n_lon, n_lev = sizes
    J, I, K, M = tracer.shape
    chunks = K // TILE
    f32 = jnp.float32
    dma = pltpu.SemaphoreType.DMA
    peers = max(n_lon - 1, 1)
    late = len(lat_sides(n_lat, 0, J))
    early = early_planes(n_lat, 0, J)[1]
    end, mean, scale = pl.pallas_call(
        functools.partial(kernel, sizes),
        out_shape=[
            pltpu.VMEM((J, I, K, M), f32),
            pltpu.VMEM((J, K, M), f32),
            pltpu.VMEM((J, K, M), f32),
        ],
        in_specs=[pl.BlockSpec(memory_space=pltpu.HBM)] * 3,
        out_specs=[pl.BlockSpec(memory_space=pltpu.VMEM)] * 3,
        scratch_shapes=[
            pltpu.VMEM((J, I + 2, K, M), f32),
            pltpu.VMEM((J, I + 2, K, M), f32),
            pltpu.VMEM((J, I, K, M), f32),
            pltpu.VMEM((J, I, K, M), f32),
            pltpu.VMEM((late, I, K, M), f32),
            pltpu.VMEM((2, late, I, K, M), f32),
            pltpu.VMEM((2, J, I, 1, M), f32),
            pltpu.VMEM((2, J, I, 1, M), f32),
            pltpu.VMEM((2, J, I, 1, M), f32),
            pltpu.VMEM((2, J, I, 1, M), f32),
            pltpu.VMEM((early, 2, K, M), f32),
            pltpu.VMEM((peers, early, 2, K, M), f32),
            pltpu.VMEM((chunks, late, 2, TILE, M), f32),
            pltpu.VMEM((peers, chunks, late, 2, TILE, M), f32),
            dma((3 + late,)),
            dma((STEPS, chunks, late)),
            dma((STEPS, chunks, late)),
            dma((STEPS, 2)),
            dma((STEPS, 2)),
            dma((STEPS, 2)),
            dma((STEPS, 2)),
            dma((peers,)),
            dma((peers,)),
            dma((chunks, peers)),
            dma((chunks, peers)),
        ],
        compiler_params=pltpu.CompilerParams(
            collective_id=0, has_side_effects=True, vmem_limit_bytes=50 * 1024 * 1024),
    )(tracer, conductance, source)
    return pl.pallas_call(
        write_out,
        out_shape=[jax.ShapeDtypeStruct((J, I, K, M), f32)] * 2,
        in_specs=[pl.BlockSpec(memory_space=pltpu.VMEM)] * 3,
        out_specs=[pl.BlockSpec(memory_space=pltpu.HBM)] * 2,
        scratch_shapes=[pltpu.VMEM((J, I, K, M), f32), dma((2 * J,))],
        compiler_params=pltpu.CompilerParams(vmem_limit_bytes=32 * 1024 * 1024),
    )(end, mean, scale)


def solution(mesh):
    placed = P("lat", "lon", "lev", None)
    sizes = tuple(mesh.shape[axis] for axis in ("lat", "lon", "lev"))
    return jax.shard_map(
        functools.partial(shards, sizes),
        mesh=mesh,
        in_specs=(placed, placed, placed),
        out_specs=(placed, placed),
        check_vma=False,
    )
```

```python
import functools
import math

import jax
import jax.numpy as jnp
from jax import lax
from jax.experimental import pallas as pl
from jax.experimental.pallas import tpu as pltpu
from jax.sharding import PartitionSpec as P

STEPS = 3
GUESS = 1.0
TILE = 8
ROWS = 8
MESH = pl.DeviceIdType.MESH


def lat_sides(n_lat, lat, J):
    if n_lat == 2:
        return [(jnp.where(lat == 0, J - 1, 0), jnp.where(lat == 0, J - 2, 1), 1 - lat, None, 0)]
    return [(0, 1, lat - 1, lat > 0, 1), (J - 1, J - 2, lat + 1, lat < n_lat - 1, 0)]


def early_planes(n_lat, lat, J):
    if n_lat == 2:
        return jnp.where(lat == 0, 0, 1), J - 1
    return 1, J - 2


def shares(K):
    chunks = K // TILE
    even = chunks // 2
    return even, max(even, min(even + max(chunks // 4, 1), chunks - 1))


def close(total, count):
    offset = total[0] / count
    variance = total[1] / count - offset * offset
    return GUESS + offset, lax.rsqrt(variance + 0.0001)


def tally(new, totals):
    moved = new - GUESS
    return totals[0] + jnp.sum(moved, axis=0), totals[1] + jnp.sum(moved * moved, axis=0)


def when(condition, act):
    if condition is None:
        act()
    else:
        pl.when(condition)(act)


def kernel(
    sizes, tracer, conductance, source, end, mean_out, scale_out, base, factor, out_even, out_odd, sums_late,
    even, odd, cond, sour, y_halo, z_lower, z_upper, z_first, z_last, sums_early, peer_early,
    load_sem, y_send, y_recv, x_send, x_recv, z_send, z_recv, early_send, early_recv,
):
    n_lat, n_lon, n_lev = sizes
    J, I, K, M = tracer.shape
    chunks = K // TILE
    blocks = I // ROWS
    count = I * n_lon
    lat, lon, lev = lax.axis_index("lat"), lax.axis_index("lon"), lax.axis_index("lev")
    below = {"lon": lon > 0, "lev": lev > 0}
    above = {"lon": lon < n_lon - 1, "lev": lev < n_lev - 1}
    index = {"lon": lon, "lev": lev}
    field = [even, odd]
    sides = lat_sides(n_lat, lat, J)
    first, number = early_planes(n_lat, lat, J)
    kept_even, kept_odd = shares(K)
    odd_lon = lon % 2 == 1
    rows_in = pl.ds(1, I)

    def levels(chunk):
        return pl.ds(chunk * TILE, TILE)

    def target(axis, way):
        return {axis: index[axis] + (1 if way == 0 else -1)}

    def y_copy(step, chunk, s):
        plane, _, peer, _, slot = sides[s]
        return pltpu.make_async_remote_copy(
            src_ref=field[step % 2].at[plane, rows_in, levels(chunk), :],
            dst_ref=y_halo.at[step % 2, slot, :, levels(chunk), :],
            send_sem=y_send.at[step, chunk, s], recv_sem=y_recv.at[step, chunk, slot],
            device_id={"lat": peer}, device_id_type=MESH)

    def y_arrival(step, chunk, s):
        plane, _, peer, _, _ = sides[s]
        return pltpu.make_async_remote_copy(
            src_ref=field[step % 2].at[plane, rows_in, levels(chunk), :],
            dst_ref=y_halo.at[step % 2, s, :, levels(chunk), :],
            send_sem=y_send.at[step, chunk, s], recv_sem=y_recv.at[step, chunk, s],
            device_id={"lat": peer}, device_id_type=MESH)

    def x_copy(step, way):
        buf = field[step % 2]
        return pltpu.make_async_remote_copy(
            src_ref=buf.at[:, I if way == 0 else 1],
            dst_ref=buf.at[:, 0 if way == 0 else I + 1],
            send_sem=x_send.at[step, way], recv_sem=x_recv.at[step, way],
            device_id=target("lon", way), device_id_type=MESH)

    def z_copy(step, way):
        src = z_last if way == 0 else z_first
        dst = z_lower if way == 0 else z_upper
        return pltpu.make_async_remote_copy(
            src_ref=src.at[step % 2], dst_ref=dst.at[step % 2],
            send_sem=z_send.at[step, way], recv_sem=z_recv.at[step, way],
            device_id=target("lev", way), device_id_type=MESH)

    def early_copy(shift):
        return pltpu.make_async_remote_copy(
            src_ref=sums_early, dst_ref=peer_early.at[shift - 1],
            send_sem=early_send.at[shift - 1], recv_sem=early_recv.at[shift - 1],
            device_id={"lon": lax.rem(lon + shift, n_lon)}, device_id_type=MESH)

    def sends(axis, way, act):
        pl.when((above if way == 0 else below)[axis])(act)

    def arrives(axis, way, act):
        pl.when((below if way == 0 else above)[axis])(act)

    barrier = pltpu.get_barrier_semaphore()
    met = n_lon - 1
    for _, _, peer, exists, _ in sides:
        when(exists, lambda: pl.semaphore_signal(
            barrier, inc=1, device_id={"lat": peer}, device_id_type=MESH))
        met = met + (1 if exists is None else exists.astype(jnp.int32))
    for way in (0, 1):
        sends("lev", way, lambda: pl.semaphore_signal(
            barrier, inc=1, device_id=target("lev", way), device_id_type=MESH))
        met = met + (above if way == 0 else below)["lev"].astype(jnp.int32)
    for shift in range(1, n_lon):
        pl.semaphore_signal(barrier, inc=1, device_id={"lon": lax.rem(lon + shift, n_lon)},
                            device_id_type=MESH)

    loads = [
        pltpu.make_async_copy(tracer.at[plane], even.at[plane, rows_in], load_sem.at[3 + s])
        for s, (plane, _, _, _, _) in enumerate(sides)
    ]
    loads.append(pltpu.make_async_copy(
        tracer.at[pl.ds(first, number)], even.at[pl.ds(first, number), rows_in], load_sem.at[0]))
    loads.append(pltpu.make_async_copy(conductance, cond, load_sem.at[1]))
    loads.append(pltpu.make_async_copy(source, sour, load_sem.at[2]))
    for load in loads[:-2]:
        load.start()
    for load in loads[:-3]:
        load.wait()
    pl.semaphore_wait(barrier, met)

    for chunk in range(chunks):
        for s, side in enumerate(sides):
            when(side[3], lambda: y_copy(0, chunk, s).start())
    loads[-2].start()
    loads[-1].start()

    for s, side in enumerate(sides):
        if side[3] is not None:
            def no_y():
                @pl.loop(0, blocks)
                def _(b):
                    for p in range(2):
                        y_halo[p, s, pl.ds(b * ROWS, ROWS)] = jnp.zeros((ROWS, K, M), jnp.float32)
            pl.when(jnp.logical_not(side[3]))(no_y)
    for way in (0, 1):
        def no_x():
            for buf in field:
                for j in range(J):
                    buf[j, 0 if way == 0 else I + 1] = jnp.zeros((K, M), jnp.float32)
        pl.when(jnp.logical_not((below if way == 0 else above)["lon"]))(no_x)

        def no_z():
            @pl.loop(0, blocks)
            def _(b):
                for p in range(2):
                    for j in range(J):
                        (z_lower if way == 0 else z_upper)[p, j, pl.ds(b * ROWS, ROWS)] = (
                            jnp.zeros((ROWS, 1, M), jnp.float32))
        pl.when(jnp.logical_not((below if way == 0 else above)["lev"]))(no_z)

    def pack_and_send(step):
        buf = field[step % 2]
        for way in (0, 1):
            sends("lon", way, lambda: x_copy(step, way).start())

        @pl.loop(0, J * blocks)
        def _(q):
            j, r = q // blocks, (q % blocks) * ROWS
            z_first[step % 2, j, pl.ds(r, ROWS)] = buf[j, pl.ds(1 + r, ROWS), pl.ds(0, 1), :]
            z_last[step % 2, j, pl.ds(r, ROWS)] = buf[j, pl.ds(1 + r, ROWS), pl.ds(K - 1, 1), :]

        for way in (0, 1):
            sends("lev", way, lambda: z_copy(step, way).start())

    def next_rows(step, chunk, j, r, inward):
        buf = field[step % 2]
        here = levels(chunk)
        rows = pl.ds(1 + r, ROWS)
        mid = buf[j, rows, here, :]
        k = lax.broadcasted_iota(jnp.int32, mid.shape, 1)
        if chunk == 0:
            edge = jnp.broadcast_to(z_lower[step % 2, j, pl.ds(r, ROWS)], mid.shape)
        else:
            edge = pltpu.roll(buf[j, rows, levels(chunk - 1), :], 1, 1)
        k_lower = jnp.where(k == 0, edge, pltpu.roll(mid, 1, 1))
        if chunk == chunks - 1:
            edge = jnp.broadcast_to(z_upper[step % 2, j, pl.ds(r, ROWS)], mid.shape)
        else:
            edge = pltpu.roll(buf[j, rows, levels(chunk + 1), :], TILE - 1, 1)
        k_upper = jnp.where(k == TILE - 1, edge, pltpu.roll(mid, TILE - 1, 1))
        if inward is None:
            across = buf[j - 1, rows, here, :] + buf[j + 1, rows, here, :]
        else:
            across = buf[inward, rows, here, :]
        spread = (
            across + buf[j, pl.ds(r, ROWS), here, :] + buf[j, pl.ds(2 + r, ROWS), here, :]
            + k_lower + k_upper - 6.0 * mid)
        return mid + cond[j, pl.ds(r, ROWS), here, :] * spread + sour[j, pl.ds(r, ROWS), here, :]

    zero = jnp.zeros((TILE, M), jnp.float32)

    def early_plane(step, chunk, j, inward):
        def body(b, totals):
            r = b * ROWS
            new = next_rows(step, chunk, j, r, inward)
            if step < STEPS - 1:
                field[(step + 1) % 2][j, pl.ds(1 + r, ROWS), levels(chunk), :] = new
                return totals
            end[j, pl.ds(r, ROWS), levels(chunk), :] = new
            return tally(new, totals)

        if step < STEPS - 1:
            lax.fori_loop(0, blocks, lambda b, _: body(b, 0), 0)
        else:
            totals = lax.fori_loop(0, blocks, body, (zero, zero))
            for q in range(2):
                sums_early[j - first, q, levels(chunk), :] = totals[q]

    def early_part(step, chunk):
        @pl.loop(1, J - 1)
        def _(j):
            early_plane(step, chunk, j, None)

        if n_lat == 2:
            early_plane(step, chunk, jnp.where(lat == 0, 0, J - 1), jnp.where(lat == 0, 1, J - 2))
        for s, (plane, inward, _, _, _) in enumerate(sides):
            @pl.loop(0, blocks)
            def _(b):
                r = b * ROWS
                base[s, pl.ds(r, ROWS), levels(chunk), :] = next_rows(step, chunk, plane, r, inward)

    def late_part(step, chunk, s):
        plane = sides[s][0]
        here = levels(chunk)

        def body(b, totals):
            r = pl.ds(b * ROWS, ROWS)
            new = base[s, r, here, :] + cond[plane, r, here, :] * y_halo[step % 2, s, r, here, :]
            if step < STEPS - 1:
                field[(step + 1) % 2][plane, pl.ds(1 + b * ROWS, ROWS), here, :] = new
                if step == STEPS - 2 and chunk >= kept_even:
                    out_even[s, r, levels(chunk - kept_even), :] = new
                if step == STEPS - 2 and chunk >= kept_odd:
                    out_odd[s, r, levels(chunk - kept_odd), :] = new
                return totals
            end[plane, r, here, :] = new
            return tally(new, totals)

        if step < STEPS - 1:
            lax.fori_loop(0, blocks, lambda b, _: body(b, 0), 0)
        else:
            totals = lax.fori_loop(0, blocks, body, (zero, zero))
            for q in range(2):
                sums_late[chunk, s, q] = totals[q]

    def stays(step, chunk, act):
        if step < STEPS - 1 or chunk < kept_even:
            act()
        elif chunk < kept_odd:
            pl.when(odd_lon)(act)

    def y_act(step, chunk, s, act):
        stays(step, chunk, lambda: when(sides[s][3], act))

    loads[-3].wait()
    pack_and_send(0)
    loads[-2].wait()
    loads[-1].wait()
    for step in range(STEPS):
        if step >= 1:
            for way in (0, 1):
                sends("lon", way, lambda: x_copy(step - 1, way).wait_send())
                sends("lev", way, lambda: z_copy(step - 1, way).wait_send())
            for s in range(len(sides)):
                for chunk in range(chunks):
                    y_act(step - 1, chunk, s, lambda: y_copy(step - 1, chunk, s).wait_send())
        for way in (0, 1):
            arrives("lon", way, lambda: x_copy(step, way).wait_recv())
            arrives("lev", way, lambda: z_copy(step, way).wait_recv())
        if step == STEPS - 1:
            for chunk in range(chunks):
                early_part(step, chunk)
            for shift in range(1, n_lon):
                early_copy(shift).start()
            for s, side in enumerate(sides):
                @pl.loop(0, blocks)
                def _(b):
                    rows = pl.ds(b * ROWS, ROWS)
                    factor[s, rows] = cond[side[0], rows, pl.ds(kept_even * TILE, K - kept_even * TILE), :]
            for way in (0, 1):
                sends("lon", way, lambda: x_copy(step, way).wait_send())
                sends("lev", way, lambda: z_copy(step, way).wait_send())
            for shift in range(1, n_lon):
                early_copy(shift).wait_recv()

            @pl.loop(0, number)
            def _(p):
                total = [sums_early[p, q] for q in range(2)]
                for shift in range(1, n_lon):
                    total = [total[q] + peer_early[shift - 1, p, q] for q in range(2)]
                mean_out[first + p], scale_out[first + p] = close(total, count)

            for shift in range(1, n_lon):
                early_copy(shift).wait_send()
        for chunk in range(chunks):
            if step < STEPS - 1:
                early_part(step, chunk)
            for s in range(len(sides)):
                y_act(step, chunk, s, lambda: y_arrival(step, chunk, s).wait_recv())
                stays(step, chunk, lambda: late_part(step, chunk, s))
                if step < STEPS - 1:
                    y_act(step + 1, chunk, s, lambda: y_copy(step + 1, chunk, s).start())
        if step < STEPS - 1:
            pack_and_send(step + 1)
    for s in range(len(sides)):
        for chunk in range(chunks):
            y_act(STEPS - 1, chunk, s, lambda: y_copy(STEPS - 1, chunk, s).wait_send())


def finish(
    sizes, end, base, factor, sums_in, in_even, in_odd, tail, mean_out, scale_out,
    sums, peer_sums, send_sem, recv_sem,
):
    n_lat, n_lon, _ = sizes
    J, I, K, M = end.shape
    chunks, blocks = K // TILE, I // ROWS
    kept_even, kept_odd = shares(K)
    lat, lon = lax.axis_index("lat"), lax.axis_index("lon")
    sides = lat_sides(n_lat, lat, J)

    barrier = pltpu.get_barrier_semaphore()
    for shift in range(1, n_lon):
        pl.semaphore_signal(barrier, inc=1, device_id={"lon": lax.rem(lon + shift, n_lon)},
                            device_id_type=MESH)

    def copy(shift):
        return pltpu.make_async_remote_copy(
            src_ref=sums, dst_ref=peer_sums.at[shift - 1],
            send_sem=send_sem.at[shift - 1], recv_sem=recv_sem.at[shift - 1],
            device_id={"lon": lax.rem(lon + shift, n_lon)}, device_id_type=MESH)

    def levels(chunk):
        return pl.ds(chunk * TILE, TILE)

    def add(chunk, s, halo, kept):
        zero = jnp.zeros((TILE, M), jnp.float32)

        def body(b, totals):
            r = pl.ds(b * ROWS, ROWS)
            new = base[s, r, levels(chunk), :] + (
                factor[s, r, levels(chunk - kept_even), :] * halo[s, r, levels(chunk - kept), :])
            tail[s, r, levels(chunk - kept_even), :] = new
            return tally(new, totals)

        totals = lax.fori_loop(0, blocks, body, (zero, zero))
        for q in range(2):
            sums[chunk, s, q] = totals[q]

    def take(chunk, s):
        @pl.loop(0, blocks)
        def _(b):
            r = pl.ds(b * ROWS, ROWS)
            tail[s, r, levels(chunk - kept_even), :] = end[sides[s][0], r, levels(chunk), :]
        for q in range(2):
            sums[chunk, s, q] = sums_in[chunk, s, q]

    for s in range(len(sides)):
        for chunk in range(kept_even):
            for q in range(2):
                sums[chunk, s, q] = sums_in[chunk, s, q]

        @pl.when(lon % 2 == 0)
        def _():
            for chunk in range(kept_even, chunks):
                add(chunk, s, in_even, kept_even)

        @pl.when(lon % 2 == 1)
        def _():
            for chunk in range(kept_even, kept_odd):
                take(chunk, s)
            for chunk in range(kept_odd, chunks):
                add(chunk, s, in_odd, kept_odd)

    pl.semaphore_wait(barrier, n_lon - 1)
    for shift in range(1, n_lon):
        copy(shift).start()
    for shift in range(1, n_lon):
        copy(shift).wait_recv()
    for s in range(len(sides)):
        for chunk in range(chunks):
            total = [sums[chunk, s, q] for q in range(2)]
            for shift in range(1, n_lon):
                total = [total[q] + peer_sums[shift - 1, chunk, s, q] for q in range(2)]
            mean_out[s, levels(chunk), :], scale_out[s, levels(chunk), :] = close(total, I * n_lon)
    for shift in range(1, n_lon):
        copy(shift).wait_send()


def write_early(sizes, end, mean, scale, standardized, end_out, held, sem):
    J, I, K, M = end.shape
    first, number = early_planes(sizes[0], lax.axis_index("lat"), J)
    copies = [pltpu.make_async_copy(
        end.at[pl.ds(first, number)], end_out.at[pl.ds(first, number)], sem.at[number])]
    copies[0].start()
    for p in range(number):
        j = first + p
        offset, factor = mean[j], scale[j]

        @pl.loop(0, I // ROWS)
        def _(b):
            rows = pl.ds(b * ROWS, ROWS)
            held[p, rows] = (end[j, rows] - offset) * factor

        copies.append(pltpu.make_async_copy(held.at[p], standardized.at[j], sem.at[p]))
        copies[-1].start()
    for copy in copies:
        copy.wait()


def write_late(sizes, end, tail, mean, scale, old_standardized, old_end, standardized, end_out, held, sem):
    J, I, K, M = end.shape
    kept = shares(K)[0] * TILE
    sides = lat_sides(sizes[0], lax.axis_index("lat"), J)
    pieces = ((end, pl.ds(0, kept)), (tail, pl.ds(kept, K - kept)))
    copies = []
    for s, (j, _, _, _, _) in enumerate(sides):
        sources = (end.at[j, :, pieces[0][1], :], tail.at[s])
        for n, (_, cut) in enumerate(pieces):
            copies.append(pltpu.make_async_copy(sources[n], end_out.at[j, :, cut, :], sem.at[s, n]))
            copies[-1].start()
    for s, (j, _, _, _, _) in enumerate(sides):
        for n, (_, cut) in enumerate(pieces):
            offset, scaling = mean[s, cut, :], scale[s, cut, :]

            @pl.loop(0, I // ROWS)
            def _(b):
                rows = pl.ds(b * ROWS, ROWS)
                new = end[j, rows, cut, :] if n == 0 else tail[s, rows]
                held[s, rows, cut, :] = (new - offset) * scaling

            copies.append(pltpu.make_async_copy(
                held.at[s, :, cut, :], standardized.at[j, :, cut, :], sem.at[s, 2 + n]))
            copies[-1].start()
    for copy in copies:
        copy.wait()


def cross(sizes, parity, block):
    n_lat, n_lon, _ = sizes

    def sent(piece, ways):
        pairs = [(a * n_lon + lon, b * n_lon + lon) for a, b in ways for lon in range(parity, n_lon, 2)]
        return lax.ppermute(piece, ("lat", "lon"), pairs)

    if n_lat == 2:
        return sent(block, [(0, 1), (1, 0)])
    up = sent(block[1:], [(a, a + 1) for a in range(n_lat - 1)])
    down = sent(block[:1], [(a + 1, a) for a in range(n_lat - 1)])
    return jnp.concatenate([up, down])


def shards(sizes, tracer, conductance, source):
    n_lat, n_lon, n_lev = sizes
    J, I, K, M = tracer.shape
    chunks = K // TILE
    f32 = jnp.float32
    dma = pltpu.SemaphoreType.DMA
    peers = max(n_lon - 1, 1)
    late = len(lat_sides(n_lat, 0, J))
    early = early_planes(n_lat, 0, J)[1]
    kept_even, kept_odd = shares(K)
    hbm, vmem = pl.BlockSpec(memory_space=pltpu.HBM), pl.BlockSpec(memory_space=pltpu.VMEM)
    out_of = (late, I, K - kept_even * TILE, M)
    scratch = [
        (J, I + 2, K, M), (J, I + 2, K, M), (J, I, K, M), (J, I, K, M), (2, late, I, K, M),
        (2, J, I, 1, M), (2, J, I, 1, M), (2, J, I, 1, M), (2, J, I, 1, M),
        (early, 2, K, M), (peers, early, 2, K, M),
    ]
    limit = sum(4 * math.prod(shape) for shape in scratch) + (2 << 20)
    end, mean, scale, base, factor, out_even, out_odd, sums = pl.pallas_call(
        functools.partial(kernel, sizes),
        out_shape=[
            pltpu.VMEM((J, I, K, M), f32),
            pltpu.VMEM((J, K, M), f32),
            pltpu.VMEM((J, K, M), f32),
            pltpu.VMEM((late, I, K, M), f32),
            pltpu.VMEM(out_of, f32),
            pltpu.VMEM(out_of, f32),
            pltpu.VMEM((late, I, K - kept_odd * TILE, M), f32),
            pltpu.VMEM((chunks, late, 2, TILE, M), f32),
        ],
        in_specs=[hbm] * 3,
        out_specs=[vmem] * 8,
        scratch_shapes=[pltpu.VMEM(shape, f32) for shape in scratch] + [
            dma((3 + late,)),
            dma((STEPS, chunks, late)),
            dma((STEPS, chunks, late)),
            dma((STEPS, 2)),
            dma((STEPS, 2)),
            dma((STEPS, 2)),
            dma((STEPS, 2)),
            dma((peers,)),
            dma((peers,)),
        ],
        compiler_params=pltpu.CompilerParams(
            collective_id=0, has_side_effects=True, vmem_limit_bytes=limit),
    )(tracer, conductance, source)
    in_even = cross(sizes, 0, out_even)
    in_odd = cross(sizes, 1, out_odd)
    whole = jax.ShapeDtypeStruct((J, I, K, M), f32)
    standardized, end_out = pl.pallas_call(
        functools.partial(write_early, sizes),
        out_shape=[whole] * 2,
        in_specs=[vmem] * 3,
        out_specs=[hbm] * 2,
        scratch_shapes=[pltpu.VMEM((early, I, K, M), f32), dma((early + 1,))],
        compiler_params=pltpu.CompilerParams(vmem_limit_bytes=16 << 20),
        cost_estimate=pl.CostEstimate(
            flops=1 << 32, bytes_accessed=8 * early * I * K * M, transcendentals=0),
    )(end, mean, scale)
    tail, mean, scale = pl.pallas_call(
        functools.partial(finish, sizes),
        out_shape=[
            pltpu.VMEM(out_of, f32), pltpu.VMEM((late, K, M), f32), pltpu.VMEM((late, K, M), f32)],
        in_specs=[vmem] * 6,
        out_specs=[vmem] * 3,
        scratch_shapes=[
            pltpu.VMEM((chunks, late, 2, TILE, M), f32),
            pltpu.VMEM((peers, chunks, late, 2, TILE, M), f32),
            dma((peers,)),
            dma((peers,)),
        ],
        compiler_params=pltpu.CompilerParams(
            collective_id=1, has_side_effects=True, vmem_limit_bytes=4 << 20),
    )(end, base, factor, sums, in_even, in_odd)
    return pl.pallas_call(
        functools.partial(write_late, sizes),
        out_shape=[whole] * 2,
        in_specs=[vmem] * 4 + [hbm] * 2,
        out_specs=[hbm] * 2,
        input_output_aliases={4: 0, 5: 1},
        scratch_shapes=[pltpu.VMEM((late, I, K, M), f32), dma((late, 4))],
        compiler_params=pltpu.CompilerParams(vmem_limit_bytes=8 << 20),
    )(end, tail, mean, scale, standardized, end_out)


def solution(mesh):
    placed = P("lat", "lon", "lev", None)
    sizes = tuple(mesh.shape[axis] for axis in ("lat", "lon", "lev"))
    return jax.shard_map(
        functools.partial(shards, sizes),
        mesh=mesh,
        in_specs=(placed, placed, placed),
        out_specs=(placed, placed),
        check_vma=False,
    )
```

```python
import functools
import math

import jax
import jax.numpy as jnp
from jax import lax
from jax.experimental import pallas as pl
from jax.experimental.pallas import tpu as pltpu
from jax.sharding import PartitionSpec as P

STEPS = 3
GUESS = 1.0
TILE = 8
ROWS = 8
MESH = pl.DeviceIdType.MESH


def lat_sides(n_lat, lat, J):
    if n_lat == 2:
        return [(jnp.where(lat == 0, J - 1, 0), jnp.where(lat == 0, J - 2, 1), 1 - lat, None, 0)]
    return [(0, 1, lat - 1, lat > 0, 1), (J - 1, J - 2, lat + 1, lat < n_lat - 1, 0)]


def early_planes(n_lat, lat, J):
    if n_lat == 2:
        return jnp.where(lat == 0, 0, 1), J - 1
    return 1, J - 2


def kept(K):
    return K // TILE // 2


def close(total, count):
    offset = total[0] / count
    variance = total[1] / count - offset * offset
    return GUESS + offset, lax.rsqrt(variance + 0.0001)


def tally(new, totals):
    moved = new - GUESS
    return totals[0] + jnp.sum(moved, axis=0), totals[1] + jnp.sum(moved * moved, axis=0)


def when(condition, act):
    if condition is None:
        act()
    else:
        pl.when(condition)(act)


def kernel(
    sizes, tracer, conductance, source, end, mean_out, scale_out, base, factor, out, sums_late,
    even, odd, cond, sour, y_halo, z_lower, z_upper, z_first, z_last, sums_early, peer_early,
    load_sem, y_send, y_recv, x_send, x_recv, z_send, z_recv, early_send, early_recv,
):
    n_lat, n_lon, n_lev = sizes
    J, I, K, M = tracer.shape
    chunks = K // TILE
    blocks = I // ROWS
    count = I * n_lon
    lat, lon, lev = lax.axis_index("lat"), lax.axis_index("lon"), lax.axis_index("lev")
    below = {"lon": lon > 0, "lev": lev > 0}
    above = {"lon": lon < n_lon - 1, "lev": lev < n_lev - 1}
    index = {"lon": lon, "lev": lev}
    field = [even, odd]
    sides = lat_sides(n_lat, lat, J)
    first, number = early_planes(n_lat, lat, J)
    stay = kept(K)
    odd_lon = lon % 2 == 1
    rows_in = pl.ds(1, I)

    def levels(chunk):
        return pl.ds(chunk * TILE, TILE)

    def target(axis, way):
        return {axis: index[axis] + (1 if way == 0 else -1)}

    def y_copy(step, chunk, s):
        plane, _, peer, _, slot = sides[s]
        return pltpu.make_async_remote_copy(
            src_ref=field[step % 2].at[plane, rows_in, levels(chunk), :],
            dst_ref=y_halo.at[step % 2, slot, :, levels(chunk), :],
            send_sem=y_send.at[step, chunk, s], recv_sem=y_recv.at[step, chunk, slot],
            device_id={"lat": peer}, device_id_type=MESH)

    def y_arrival(step, chunk, s):
        plane, _, peer, _, _ = sides[s]
        return pltpu.make_async_remote_copy(
            src_ref=field[step % 2].at[plane, rows_in, levels(chunk), :],
            dst_ref=y_halo.at[step % 2, s, :, levels(chunk), :],
            send_sem=y_send.at[step, chunk, s], recv_sem=y_recv.at[step, chunk, s],
            device_id={"lat": peer}, device_id_type=MESH)

    faces = [pl.ds(first, number)] + [pl.ds(side[0], 1) for side in sides]

    def x_copy(step, way, part):
        buf = field[step % 2]
        return pltpu.make_async_remote_copy(
            src_ref=buf.at[faces[part], I if way == 0 else 1],
            dst_ref=buf.at[faces[part], 0 if way == 0 else I + 1],
            send_sem=x_send.at[step, way, part], recv_sem=x_recv.at[step, way, part],
            device_id=target("lon", way), device_id_type=MESH)

    def z_copy(step, way, part):
        src = z_last if way == 0 else z_first
        dst = z_lower if way == 0 else z_upper
        return pltpu.make_async_remote_copy(
            src_ref=src.at[step % 2, faces[part]], dst_ref=dst.at[step % 2, faces[part]],
            send_sem=z_send.at[step, way, part], recv_sem=z_recv.at[step, way, part],
            device_id=target("lev", way), device_id_type=MESH)

    def early_copy(shift):
        return pltpu.make_async_remote_copy(
            src_ref=sums_early, dst_ref=peer_early.at[shift - 1],
            send_sem=early_send.at[shift - 1], recv_sem=early_recv.at[shift - 1],
            device_id={"lon": lax.rem(lon + shift, n_lon)}, device_id_type=MESH)

    def sends(axis, way, act):
        pl.when((above if way == 0 else below)[axis])(act)

    def arrives(axis, way, act):
        pl.when((below if way == 0 else above)[axis])(act)

    barrier = pltpu.get_barrier_semaphore()
    met = n_lon - 1
    for _, _, peer, exists, _ in sides:
        when(exists, lambda: pl.semaphore_signal(
            barrier, inc=1, device_id={"lat": peer}, device_id_type=MESH))
        met = met + (1 if exists is None else exists.astype(jnp.int32))
    for way in (0, 1):
        sends("lev", way, lambda: pl.semaphore_signal(
            barrier, inc=1, device_id=target("lev", way), device_id_type=MESH))
        met = met + (above if way == 0 else below)["lev"].astype(jnp.int32)
    for shift in range(1, n_lon):
        pl.semaphore_signal(barrier, inc=1, device_id={"lon": lax.rem(lon + shift, n_lon)},
                            device_id_type=MESH)

    loads = [
        pltpu.make_async_copy(tracer.at[plane], even.at[plane, rows_in], load_sem.at[3 + s])
        for s, (plane, _, _, _, _) in enumerate(sides)
    ]
    loads.append(pltpu.make_async_copy(
        tracer.at[pl.ds(first, number)], even.at[pl.ds(first, number), rows_in], load_sem.at[0]))
    loads.append(pltpu.make_async_copy(conductance, cond, load_sem.at[1]))
    loads.append(pltpu.make_async_copy(source, sour, load_sem.at[2]))
    for load in loads[:-2]:
        load.start()
    for load in loads[:-3]:
        load.wait()
    pl.semaphore_wait(barrier, met)

    for chunk in range(chunks):
        for s, side in enumerate(sides):
            when(side[3], lambda: y_copy(0, chunk, s).start())
    loads[-2].start()
    loads[-1].start()

    for s, side in enumerate(sides):
        if side[3] is not None:
            def no_y():
                @pl.loop(0, blocks)
                def _(b):
                    for p in range(2):
                        y_halo[p, s, pl.ds(b * ROWS, ROWS)] = jnp.zeros((ROWS, K, M), jnp.float32)
            pl.when(jnp.logical_not(side[3]))(no_y)
    for way in (0, 1):
        def no_x():
            for buf in field:
                for j in range(J):
                    buf[j, 0 if way == 0 else I + 1] = jnp.zeros((K, M), jnp.float32)
        pl.when(jnp.logical_not((below if way == 0 else above)["lon"]))(no_x)

        def no_z():
            @pl.loop(0, blocks)
            def _(b):
                for p in range(2):
                    for j in range(J):
                        (z_lower if way == 0 else z_upper)[p, j, pl.ds(b * ROWS, ROWS)] = (
                            jnp.zeros((ROWS, 1, M), jnp.float32))
        pl.when(jnp.logical_not((below if way == 0 else above)["lev"]))(no_z)

    def pack_and_send(step, part):
        buf = field[step % 2]
        start, extent = (first, number) if part == 0 else (sides[part - 1][0], 1)
        for way in (0, 1):
            sends("lon", way, lambda: x_copy(step, way, part).start())

        @pl.loop(0, extent * blocks)
        def _(q):
            j, r = start + q // blocks, (q % blocks) * ROWS
            z_first[step % 2, j, pl.ds(r, ROWS)] = buf[j, pl.ds(1 + r, ROWS), pl.ds(0, 1), :]
            z_last[step % 2, j, pl.ds(r, ROWS)] = buf[j, pl.ds(1 + r, ROWS), pl.ds(K - 1, 1), :]

        for way in (0, 1):
            sends("lev", way, lambda: z_copy(step, way, part).start())

    def faces_sent(step):
        for part in range(len(faces)):
            for way in (0, 1):
                sends("lon", way, lambda: x_copy(step, way, part).wait_send())
                sends("lev", way, lambda: z_copy(step, way, part).wait_send())

    def faces_arrive(step, part):
        for way in (0, 1):
            arrives("lon", way, lambda: x_copy(step, way, part).wait_recv())
            arrives("lev", way, lambda: z_copy(step, way, part).wait_recv())

    def next_rows(step, chunk, j, r, inward):
        buf = field[step % 2]
        here = levels(chunk)
        rows = pl.ds(1 + r, ROWS)
        mid = buf[j, rows, here, :]
        k = lax.broadcasted_iota(jnp.int32, mid.shape, 1)
        if chunk == 0:
            edge = jnp.broadcast_to(z_lower[step % 2, j, pl.ds(r, ROWS)], mid.shape)
        else:
            edge = pltpu.roll(buf[j, rows, levels(chunk - 1), :], 1, 1)
        k_lower = jnp.where(k == 0, edge, pltpu.roll(mid, 1, 1))
        if chunk == chunks - 1:
            edge = jnp.broadcast_to(z_upper[step % 2, j, pl.ds(r, ROWS)], mid.shape)
        else:
            edge = pltpu.roll(buf[j, rows, levels(chunk + 1), :], TILE - 1, 1)
        k_upper = jnp.where(k == TILE - 1, edge, pltpu.roll(mid, TILE - 1, 1))
        if inward is None:
            across = buf[j - 1, rows, here, :] + buf[j + 1, rows, here, :]
        else:
            across = buf[inward, rows, here, :]
        spread = (
            across + buf[j, pl.ds(r, ROWS), here, :] + buf[j, pl.ds(2 + r, ROWS), here, :]
            + k_lower + k_upper - 6.0 * mid)
        return mid + cond[j, pl.ds(r, ROWS), here, :] * spread + sour[j, pl.ds(r, ROWS), here, :]

    zero = jnp.zeros((TILE, M), jnp.float32)

    def early_plane(step, chunk, j, inward):
        def body(b, totals):
            r = b * ROWS
            new = next_rows(step, chunk, j, r, inward)
            if step < STEPS - 1:
                field[(step + 1) % 2][j, pl.ds(1 + r, ROWS), levels(chunk), :] = new
                return totals
            end[j, pl.ds(r, ROWS), levels(chunk), :] = new
            return tally(new, totals)

        if step < STEPS - 1:
            lax.fori_loop(0, blocks, lambda b, _: body(b, 0), 0)
        else:
            totals = lax.fori_loop(0, blocks, body, (zero, zero))
            for q in range(2):
                sums_early[j - first, q, levels(chunk), :] = totals[q]

    def early_part(step, chunk):
        @pl.loop(1, J - 1)
        def _(j):
            early_plane(step, chunk, j, None)

        if n_lat == 2:
            early_plane(step, chunk, jnp.where(lat == 0, 0, J - 1), jnp.where(lat == 0, 1, J - 2))

    def base_part(step, chunk):
        for s, (plane, inward, _, _, _) in enumerate(sides):
            @pl.loop(0, blocks)
            def _(b):
                r = b * ROWS
                base[s, pl.ds(r, ROWS), levels(chunk), :] = next_rows(step, chunk, plane, r, inward)

    def late_part(step, chunk, s):
        plane = sides[s][0]
        here = levels(chunk)

        def body(b, totals):
            r = pl.ds(b * ROWS, ROWS)
            new = base[s, r, here, :] + cond[plane, r, here, :] * y_halo[step % 2, s, r, here, :]
            if step < STEPS - 1:
                field[(step + 1) % 2][plane, pl.ds(1 + b * ROWS, ROWS), here, :] = new
                if step == STEPS - 2 and chunk >= stay:
                    out[s, r, levels(chunk - stay), :] = new
                return totals
            end[plane, r, here, :] = new
            return tally(new, totals)

        if step < STEPS - 1:
            lax.fori_loop(0, blocks, lambda b, _: body(b, 0), 0)
        else:
            totals = lax.fori_loop(0, blocks, body, (zero, zero))
            for q in range(2):
                sums_late[chunk, s, q] = totals[q]

    def y_start(step, chunk, s, condition=None):
        exists = sides[s][3]
        if condition is not None and exists is not None:
            condition = jnp.logical_and(condition, exists)
        when(exists if condition is None else condition, lambda: y_copy(step, chunk, s).start())

    loads[-3].wait()
    for part in range(len(faces)):
        pack_and_send(0, part)
    loads[-2].wait()
    loads[-1].wait()
    for step in range(STEPS):
        last = step == STEPS - 1
        if step >= 1:
            faces_sent(step - 1)
        faces_arrive(step, 0)
        for chunk in range(chunks):
            early_part(step, chunk)
            if last and chunk == max(chunks - 2, 0):
                for held in range(stay):
                    for s in range(len(sides)):
                        y_start(step, held, s, odd_lon)
        if last:
            for shift in range(1, n_lon):
                early_copy(shift).start()
        else:
            pack_and_send(step + 1, 0)
        for part in range(1, len(faces)):
            faces_arrive(step, part)
        for chunk in range(chunks):
            base_part(step, chunk)
        if step >= 1:
            for s, side in enumerate(sides):
                for chunk in range(chunks):
                    when(side[3], lambda: y_copy(step - 1, chunk, s).wait_send())
        if last:
            for s, side in enumerate(sides):
                @pl.loop(0, blocks)
                def _(b):
                    rows = pl.ds(b * ROWS, ROWS)
                    factor[s, rows] = cond[side[0], rows, pl.ds(stay * TILE, K - stay * TILE), :]
            faces_sent(step)
            for shift in range(1, n_lon):
                early_copy(shift).wait_recv()

            @pl.loop(0, number)
            def _(p):
                total = [sums_early[p, q] for q in range(2)]
                for shift in range(1, n_lon):
                    total = [total[q] + peer_early[shift - 1, p, q] for q in range(2)]
                mean_out[first + p], scale_out[first + p] = close(total, count)

            for shift in range(1, n_lon):
                early_copy(shift).wait_send()
        for chunk in range(stay if last else chunks):
            for s, side in enumerate(sides):
                when(side[3], lambda: y_arrival(step, chunk, s).wait_recv())
                late_part(step, chunk, s)
                if step < STEPS - 2:
                    y_start(step + 1, chunk, s)
                elif not last and chunk < stay:
                    y_start(step + 1, chunk, s, jnp.logical_not(odd_lon))
        if not last:
            for part in range(1, len(faces)):
                pack_and_send(step + 1, part)
    for s, side in enumerate(sides):
        for chunk in range(stay):
            when(side[3], lambda: y_copy(STEPS - 1, chunk, s).wait_send())


def finish(
    sizes, base, factor, sums_in, halo, tail, mean_out, scale_out, sums, peer_sums, send_sem, recv_sem,
):
    n_lat, n_lon, _ = sizes
    late, I, K, M = base.shape
    chunks, blocks, stay = K // TILE, I // ROWS, kept(K)
    lon = lax.axis_index("lon")

    barrier = pltpu.get_barrier_semaphore()
    for shift in range(1, n_lon):
        pl.semaphore_signal(barrier, inc=1, device_id={"lon": lax.rem(lon + shift, n_lon)},
                            device_id_type=MESH)

    def copy(shift):
        return pltpu.make_async_remote_copy(
            src_ref=sums, dst_ref=peer_sums.at[shift - 1],
            send_sem=send_sem.at[shift - 1], recv_sem=recv_sem.at[shift - 1],
            device_id={"lon": lax.rem(lon + shift, n_lon)}, device_id_type=MESH)

    zero = jnp.zeros((TILE, M), jnp.float32)
    for s in range(late):
        for chunk in range(stay):
            for q in range(2):
                sums[chunk, s, q] = sums_in[chunk, s, q]
        for chunk in range(stay, chunks):
            here, there = pl.ds(chunk * TILE, TILE), pl.ds((chunk - stay) * TILE, TILE)

            def body(b, totals):
                r = pl.ds(b * ROWS, ROWS)
                new = base[s, r, here, :] + factor[s, r, there, :] * halo[s, r, there, :]
                tail[s, r, there, :] = new
                return tally(new, totals)

            totals = lax.fori_loop(0, blocks, body, (zero, zero))
            for q in range(2):
                sums[chunk, s, q] = totals[q]

    pl.semaphore_wait(barrier, n_lon - 1)
    for shift in range(1, n_lon):
        copy(shift).start()
    for shift in range(1, n_lon):
        copy(shift).wait_recv()
    for s in range(late):
        for chunk in range(chunks):
            total = [sums[chunk, s, q] for q in range(2)]
            for shift in range(1, n_lon):
                total = [total[q] + peer_sums[shift - 1, chunk, s, q] for q in range(2)]
            here = pl.ds(chunk * TILE, TILE)
            mean_out[s, here, :], scale_out[s, here, :] = close(total, I * n_lon)
    for shift in range(1, n_lon):
        copy(shift).wait_send()


def write_early(sizes, end, mean, scale, standardized, end_out, held, sem):
    J, I, K, M = end.shape
    lat = lax.axis_index("lat")
    first, number = early_planes(sizes[0], lat, J)
    done = pl.ds(0, kept(K) * TILE)
    copies = [pltpu.make_async_copy(
        end.at[pl.ds(first, number)], end_out.at[pl.ds(first, number)], sem.at[number])]
    for s, side in enumerate(lat_sides(sizes[0], lat, J)):
        copies.append(pltpu.make_async_copy(
            end.at[side[0], :, done, :], end_out.at[side[0], :, done, :], sem.at[number + 1 + s]))
    for copy in copies:
        copy.start()
    for p in range(number):
        j = first + p
        offset, factor = mean[j], scale[j]

        @pl.loop(0, I // ROWS)
        def _(b):
            rows = pl.ds(b * ROWS, ROWS)
            held[p, rows] = (end[j, rows] - offset) * factor

        copies.append(pltpu.make_async_copy(held.at[p], standardized.at[j], sem.at[p]))
        copies[-1].start()
    for copy in copies:
        copy.wait()


def write_late(sizes, end, tail, mean, scale, old_standardized, old_end, standardized, end_out, held, sem):
    J, I, K, M = end.shape
    cut = kept(K) * TILE
    low, high = pl.ds(0, cut), pl.ds(cut, K - cut)
    copies = []
    for s, side in enumerate(lat_sides(sizes[0], lax.axis_index("lat"), J)):
        j = side[0]
        copies.append(pltpu.make_async_copy(tail.at[s], end_out.at[j, :, high, :], sem.at[s, 0]))
        copies[-1].start()
        for n, here in enumerate((low, high)):
            offset, scaling = mean[s, here, :], scale[s, here, :]

            @pl.loop(0, I // ROWS)
            def _(b):
                rows = pl.ds(b * ROWS, ROWS)
                new = end[j, rows, here, :] if n == 0 else tail[s, rows]
                held[s, rows, here, :] = (new - offset) * scaling

            copies.append(pltpu.make_async_copy(
                held.at[s, :, here, :], standardized.at[j, :, here, :], sem.at[s, 1 + n]))
            copies[-1].start()
    for copy in copies:
        copy.wait()


def cross(sizes, block):
    n_lat = sizes[0]
    if n_lat == 2:
        return lax.ppermute(block, "lat", [(0, 1), (1, 0)])
    up = lax.ppermute(block[1:], "lat", [(a, a + 1) for a in range(n_lat - 1)])
    down = lax.ppermute(block[:1], "lat", [(a + 1, a) for a in range(n_lat - 1)])
    return jnp.concatenate([up, down])


def shards(sizes, tracer, conductance, source):
    n_lat, n_lon, n_lev = sizes
    J, I, K, M = tracer.shape
    chunks = K // TILE
    f32 = jnp.float32
    dma = pltpu.SemaphoreType.DMA
    peers = max(n_lon - 1, 1)
    late = len(lat_sides(n_lat, 0, J))
    early = early_planes(n_lat, 0, J)[1]
    stay = kept(K)
    hbm, vmem = pl.BlockSpec(memory_space=pltpu.HBM), pl.BlockSpec(memory_space=pltpu.VMEM)
    out_of = (late, I, K - stay * TILE, M)
    scratch = [
        (J, I + 2, K, M), (J, I + 2, K, M), (J, I, K, M), (J, I, K, M), (2, late, I, K, M),
        (2, J, I, 1, M), (2, J, I, 1, M), (2, J, I, 1, M), (2, J, I, 1, M),
        (early, 2, K, M), (peers, early, 2, K, M),
    ]
    limit = sum(4 * math.prod(shape) for shape in scratch) + (2 << 20)
    end, mean, scale, base, factor, out, sums = pl.pallas_call(
        functools.partial(kernel, sizes),
        out_shape=[
            pltpu.VMEM((J, I, K, M), f32),
            pltpu.VMEM((J, K, M), f32),
            pltpu.VMEM((J, K, M), f32),
            pltpu.VMEM((late, I, K, M), f32),
            pltpu.VMEM(out_of, f32),
            pltpu.VMEM(out_of, f32),
            pltpu.VMEM((chunks, late, 2, TILE, M), f32),
        ],
        in_specs=[hbm] * 3,
        out_specs=[vmem] * 7,
        scratch_shapes=[pltpu.VMEM(shape, f32) for shape in scratch] + [
            dma((3 + late,)),
            dma((STEPS, chunks, late)),
            dma((STEPS, chunks, late)),
            dma((STEPS, 2, 1 + late)),
            dma((STEPS, 2, 1 + late)),
            dma((STEPS, 2, 1 + late)),
            dma((STEPS, 2, 1 + late)),
            dma((peers,)),
            dma((peers,)),
        ],
        compiler_params=pltpu.CompilerParams(
            collective_id=0, has_side_effects=True, vmem_limit_bytes=limit),
    )(tracer, conductance, source)
    halo = cross(sizes, out)
    whole = jax.ShapeDtypeStruct((J, I, K, M), f32)
    standardized, end_out = pl.pallas_call(
        functools.partial(write_early, sizes),
        out_shape=[whole] * 2,
        in_specs=[vmem] * 3,
        out_specs=[hbm] * 2,
        scratch_shapes=[pltpu.VMEM((early, I, K, M), f32), dma((early + 1 + late,))],
        compiler_params=pltpu.CompilerParams(vmem_limit_bytes=16 << 20),
        cost_estimate=pl.CostEstimate(
            flops=1 << 32, bytes_accessed=8 * early * I * K * M, transcendentals=0),
    )(end, mean, scale)
    tail, mean, scale = pl.pallas_call(
        functools.partial(finish, sizes),
        out_shape=[
            pltpu.VMEM(out_of, f32), pltpu.VMEM((late, K, M), f32), pltpu.VMEM((late, K, M), f32)],
        in_specs=[vmem] * 4,
        out_specs=[vmem] * 3,
        scratch_shapes=[
            pltpu.VMEM((chunks, late, 2, TILE, M), f32),
            pltpu.VMEM((peers, chunks, late, 2, TILE, M), f32),
            dma((peers,)),
            dma((peers,)),
        ],
        compiler_params=pltpu.CompilerParams(
            collective_id=1, has_side_effects=True, vmem_limit_bytes=4 << 20),
    )(base, factor, sums, halo)
    return pl.pallas_call(
        functools.partial(write_late, sizes),
        out_shape=[whole] * 2,
        in_specs=[vmem] * 4 + [hbm] * 2,
        out_specs=[hbm] * 2,
        input_output_aliases={4: 0, 5: 1},
        scratch_shapes=[pltpu.VMEM((late, I, K, M), f32), dma((late, 3))],
        compiler_params=pltpu.CompilerParams(vmem_limit_bytes=8 << 20),
    )(end, tail, mean, scale, standardized, end_out)


def solution(mesh):
    placed = P("lat", "lon", "lev", None)
    sizes = tuple(mesh.shape[axis] for axis in ("lat", "lon", "lev"))
    return jax.shard_map(
        functools.partial(shards, sizes),
        mesh=mesh,
        in_specs=(placed, placed, placed),
        out_specs=(placed, placed),
        check_vma=False,
    )
```

```python
import functools
import math

import jax
import jax.numpy as jnp
from jax import lax
from jax.experimental import pallas as pl
from jax.experimental.pallas import tpu as pltpu
from jax.sharding import PartitionSpec as P

STEPS = 3
GUESS = 1.0
TILE = 8
ROWS = 8
MESH = pl.DeviceIdType.MESH


def lat_sides(n_lat, lat, J):
    if n_lat == 2:
        return [(jnp.where(lat == 0, J - 1, 0), jnp.where(lat == 0, J - 2, 1), 1 - lat, None, 0)]
    return [(0, 1, lat - 1, lat > 0, 1), (J - 1, J - 2, lat + 1, lat < n_lat - 1, 0)]


def early_planes(n_lat, lat, J):
    if n_lat == 2:
        return jnp.where(lat == 0, 0, 1), J - 1
    return 1, J - 2


def kept(K):
    return K // TILE // 2


def close(total, count):
    offset = total[0] / count
    variance = total[1] / count - offset * offset
    return GUESS + offset, lax.rsqrt(variance + 0.0001)


def tally(new, totals):
    moved = new - GUESS
    return totals[0] + jnp.sum(moved, axis=0), totals[1] + jnp.sum(moved * moved, axis=0)


def when(condition, act):
    if condition is None:
        act()
    else:
        pl.when(condition)(act)


def kernel(
    sizes, tracer, conductance, source, end, mean_out, scale_out, base, factor, out, sums_late,
    even, odd, cond, sour, y_halo, z_lower, z_upper, z_first, z_last, sums_early, peer_early,
    load_sem, y_send, y_recv, x_send, x_recv, z_send, z_recv, early_send, early_recv,
):
    n_lat, n_lon, n_lev = sizes
    J, I, K, M = tracer.shape
    chunks = K // TILE
    blocks = I // ROWS
    count = I * n_lon
    lat, lon, lev = lax.axis_index("lat"), lax.axis_index("lon"), lax.axis_index("lev")
    below = {"lon": lon > 0, "lev": lev > 0}
    above = {"lon": lon < n_lon - 1, "lev": lev < n_lev - 1}
    index = {"lon": lon, "lev": lev}
    field = [even, odd]
    sides = lat_sides(n_lat, lat, J)
    first, number = early_planes(n_lat, lat, J)
    stay = kept(K)
    odd_lon = lon % 2 == 1
    rows_in = pl.ds(1, I)

    def levels(chunk):
        return pl.ds(chunk * TILE, TILE)

    def target(axis, way):
        return {axis: index[axis] + (1 if way == 0 else -1)}

    def y_copy(step, chunk, s):
        plane, _, peer, _, slot = sides[s]
        return pltpu.make_async_remote_copy(
            src_ref=field[step % 2].at[plane, rows_in, levels(chunk), :],
            dst_ref=y_halo.at[step % 2, slot, :, levels(chunk), :],
            send_sem=y_send.at[step, chunk, s], recv_sem=y_recv.at[step, chunk, slot],
            device_id={"lat": peer}, device_id_type=MESH)

    def y_arrival(step, chunk, s):
        plane, _, peer, _, _ = sides[s]
        return pltpu.make_async_remote_copy(
            src_ref=field[step % 2].at[plane, rows_in, levels(chunk), :],
            dst_ref=y_halo.at[step % 2, s, :, levels(chunk), :],
            send_sem=y_send.at[step, chunk, s], recv_sem=y_recv.at[step, chunk, s],
            device_id={"lat": peer}, device_id_type=MESH)

    faces = [pl.ds(first, number)] + [pl.ds(side[0], 1) for side in sides]

    def x_copy(step, way, part):
        buf = field[step % 2]
        return pltpu.make_async_remote_copy(
            src_ref=buf.at[faces[part], I if way == 0 else 1],
            dst_ref=buf.at[faces[part], 0 if way == 0 else I + 1],
            send_sem=x_send.at[step, way, part], recv_sem=x_recv.at[step, way, part],
            device_id=target("lon", way), device_id_type=MESH)

    def z_copy(step, way, part):
        src = z_last if way == 0 else z_first
        dst = z_lower if way == 0 else z_upper
        return pltpu.make_async_remote_copy(
            src_ref=src.at[step % 2, faces[part]], dst_ref=dst.at[step % 2, faces[part]],
            send_sem=z_send.at[step, way, part], recv_sem=z_recv.at[step, way, part],
            device_id=target("lev", way), device_id_type=MESH)

    def early_copy(shift):
        return pltpu.make_async_remote_copy(
            src_ref=sums_early, dst_ref=peer_early.at[shift - 1],
            send_sem=early_send.at[shift - 1], recv_sem=early_recv.at[shift - 1],
            device_id={"lon": lax.rem(lon + shift, n_lon)}, device_id_type=MESH)

    def sends(axis, way, act):
        pl.when((above if way == 0 else below)[axis])(act)

    def arrives(axis, way, act):
        pl.when((below if way == 0 else above)[axis])(act)

    barrier = pltpu.get_barrier_semaphore()
    met = n_lon - 1
    for _, _, peer, exists, _ in sides:
        when(exists, lambda: pl.semaphore_signal(
            barrier, inc=1, device_id={"lat": peer}, device_id_type=MESH))
        met = met + (1 if exists is None else exists.astype(jnp.int32))
    for way in (0, 1):
        sends("lev", way, lambda: pl.semaphore_signal(
            barrier, inc=1, device_id=target("lev", way), device_id_type=MESH))
        met = met + (above if way == 0 else below)["lev"].astype(jnp.int32)
    for shift in range(1, n_lon):
        pl.semaphore_signal(barrier, inc=1, device_id={"lon": lax.rem(lon + shift, n_lon)},
                            device_id_type=MESH)

    loads = [
        pltpu.make_async_copy(tracer.at[plane], even.at[plane, rows_in], load_sem.at[3 + s])
        for s, (plane, _, _, _, _) in enumerate(sides)
    ]
    loads.append(pltpu.make_async_copy(
        tracer.at[pl.ds(first, number)], even.at[pl.ds(first, number), rows_in], load_sem.at[0]))
    loads.append(pltpu.make_async_copy(conductance, cond, load_sem.at[1]))
    loads.append(pltpu.make_async_copy(source, sour, load_sem.at[2]))
    for load in loads[:-2]:
        load.start()
    for load in loads[:-3]:
        load.wait()
    pl.semaphore_wait(barrier, met)

    for chunk in range(chunks):
        for s, side in enumerate(sides):
            when(side[3], lambda: y_copy(0, chunk, s).start())
    loads[-2].start()
    loads[-1].start()

    for s, side in enumerate(sides):
        if side[3] is not None:
            def no_y():
                @pl.loop(0, blocks)
                def _(b):
                    for p in range(2):
                        y_halo[p, s, pl.ds(b * ROWS, ROWS)] = jnp.zeros((ROWS, K, M), jnp.float32)
            pl.when(jnp.logical_not(side[3]))(no_y)
    for way in (0, 1):
        def no_x():
            for buf in field:
                for j in range(J):
                    buf[j, 0 if way == 0 else I + 1] = jnp.zeros((K, M), jnp.float32)
        pl.when(jnp.logical_not((below if way == 0 else above)["lon"]))(no_x)

        def no_z():
            @pl.loop(0, blocks)
            def _(b):
                for p in range(2):
                    for j in range(J):
                        (z_lower if way == 0 else z_upper)[p, j, pl.ds(b * ROWS, ROWS)] = (
                            jnp.zeros((ROWS, 1, M), jnp.float32))
        pl.when(jnp.logical_not((below if way == 0 else above)["lev"]))(no_z)

    def pack_and_send(step, part):
        buf = field[step % 2]
        start, extent = (first, number) if part == 0 else (sides[part - 1][0], 1)
        for way in (0, 1):
            sends("lon", way, lambda: x_copy(step, way, part).start())

        @pl.loop(0, extent * blocks)
        def _(q):
            j, r = start + q // blocks, (q % blocks) * ROWS
            z_first[step % 2, j, pl.ds(r, ROWS)] = buf[j, pl.ds(1 + r, ROWS), pl.ds(0, 1), :]
            z_last[step % 2, j, pl.ds(r, ROWS)] = buf[j, pl.ds(1 + r, ROWS), pl.ds(K - 1, 1), :]

        for way in (0, 1):
            sends("lev", way, lambda: z_copy(step, way, part).start())

    def faces_sent(step):
        for part in range(len(faces)):
            for way in (0, 1):
                sends("lon", way, lambda: x_copy(step, way, part).wait_send())
                sends("lev", way, lambda: z_copy(step, way, part).wait_send())

    def faces_arrive(step, part):
        for way in (0, 1):
            arrives("lon", way, lambda: x_copy(step, way, part).wait_recv())
            arrives("lev", way, lambda: z_copy(step, way, part).wait_recv())

    def next_rows(step, chunk, j, r, inward):
        buf = field[step % 2]
        here = levels(chunk)
        rows = pl.ds(1 + r, ROWS)
        mid = buf[j, rows, here, :]
        k = lax.broadcasted_iota(jnp.int32, mid.shape, 1)
        if chunk == 0:
            edge = jnp.broadcast_to(z_lower[step % 2, j, pl.ds(r, ROWS)], mid.shape)
        else:
            edge = pltpu.roll(buf[j, rows, levels(chunk - 1), :], 1, 1)
        k_lower = jnp.where(k == 0, edge, pltpu.roll(mid, 1, 1))
        if chunk == chunks - 1:
            edge = jnp.broadcast_to(z_upper[step % 2, j, pl.ds(r, ROWS)], mid.shape)
        else:
            edge = pltpu.roll(buf[j, rows, levels(chunk + 1), :], TILE - 1, 1)
        k_upper = jnp.where(k == TILE - 1, edge, pltpu.roll(mid, TILE - 1, 1))
        if inward is None:
            across = buf[j - 1, rows, here, :] + buf[j + 1, rows, here, :]
        else:
            across = buf[inward, rows, here, :]
        spread = (
            across + buf[j, pl.ds(r, ROWS), here, :] + buf[j, pl.ds(2 + r, ROWS), here, :]
            + k_lower + k_upper - 6.0 * mid)
        return mid + cond[j, pl.ds(r, ROWS), here, :] * spread + sour[j, pl.ds(r, ROWS), here, :]

    zero = jnp.zeros((TILE, M), jnp.float32)

    def early_plane(step, chunk, j, inward):
        def body(b, totals):
            r = b * ROWS
            new = next_rows(step, chunk, j, r, inward)
            if step < STEPS - 1:
                field[(step + 1) % 2][j, pl.ds(1 + r, ROWS), levels(chunk), :] = new
                return totals
            end[j, pl.ds(r, ROWS), levels(chunk), :] = new
            return tally(new, totals)

        if step < STEPS - 1:
            lax.fori_loop(0, blocks, lambda b, _: body(b, 0), 0)
        else:
            totals = lax.fori_loop(0, blocks, body, (zero, zero))
            for q in range(2):
                sums_early[j - first, q, levels(chunk), :] = totals[q]

    def early_part(step, chunk):
        @pl.loop(1, J - 1)
        def _(j):
            early_plane(step, chunk, j, None)

        if n_lat == 2:
            early_plane(step, chunk, jnp.where(lat == 0, 0, J - 1), jnp.where(lat == 0, 1, J - 2))

    def base_part(step, chunk):
        for s, (plane, inward, _, _, _) in enumerate(sides):
            @pl.loop(0, blocks)
            def _(b):
                r = b * ROWS
                base[s, pl.ds(r, ROWS), levels(chunk), :] = next_rows(step, chunk, plane, r, inward)

    def late_part(step, chunk, s):
        plane = sides[s][0]
        here = levels(chunk)

        def body(b, totals):
            r = pl.ds(b * ROWS, ROWS)
            new = base[s, r, here, :] + cond[plane, r, here, :] * y_halo[step % 2, s, r, here, :]
            if step < STEPS - 1:
                field[(step + 1) % 2][plane, pl.ds(1 + b * ROWS, ROWS), here, :] = new
                if step == STEPS - 2 and chunk >= stay:
                    out[s, r, levels(chunk - stay), :] = new
                return totals
            end[plane, r, here, :] = new
            return tally(new, totals)

        if step < STEPS - 1:
            lax.fori_loop(0, blocks, lambda b, _: body(b, 0), 0)
        else:
            totals = lax.fori_loop(0, blocks, body, (zero, zero))
            for q in range(2):
                sums_late[chunk, s, q] = totals[q]

    def y_start(step, chunk, s, condition=None):
        exists = sides[s][3]
        if condition is not None and exists is not None:
            condition = jnp.logical_and(condition, exists)
        when(exists if condition is None else condition, lambda: y_copy(step, chunk, s).start())

    loads[-3].wait()
    for part in range(len(faces)):
        pack_and_send(0, part)
    loads[-2].wait()
    loads[-1].wait()
    for step in range(STEPS):
        last = step == STEPS - 1
        if step >= 1:
            faces_sent(step - 1)
        faces_arrive(step, 0)
        for chunk in range(chunks):
            early_part(step, chunk)
            if last and chunk == max(chunks - 2, 0):
                for held in range(stay):
                    for s in range(len(sides)):
                        y_start(step, held, s, odd_lon)
        if last:
            for shift in range(1, n_lon):
                early_copy(shift).start()
        else:
            pack_and_send(step + 1, 0)
        for part in range(1, len(faces)):
            faces_arrive(step, part)
        for chunk in range(chunks):
            base_part(step, chunk)
        if step >= 1:
            for s, side in enumerate(sides):
                for chunk in range(chunks):
                    when(side[3], lambda: y_copy(step - 1, chunk, s).wait_send())
        if last:
            for s, side in enumerate(sides):
                @pl.loop(0, blocks)
                def _(b):
                    rows = pl.ds(b * ROWS, ROWS)
                    factor[s, rows] = cond[side[0], rows, pl.ds(stay * TILE, K - stay * TILE), :]
            faces_sent(step)
            for shift in range(1, n_lon):
                early_copy(shift).wait_recv()

            @pl.loop(0, number)
            def _(p):
                total = [sums_early[p, q] for q in range(2)]
                for shift in range(1, n_lon):
                    total = [total[q] + peer_early[shift - 1, p, q] for q in range(2)]
                mean_out[first + p], scale_out[first + p] = close(total, count)

            for shift in range(1, n_lon):
                early_copy(shift).wait_send()
        for chunk in range(stay if last else chunks):
            for s, side in enumerate(sides):
                when(side[3], lambda: y_arrival(step, chunk, s).wait_recv())
                late_part(step, chunk, s)
                if step < STEPS - 2:
                    y_start(step + 1, chunk, s)
                elif not last and chunk < stay:
                    y_start(step + 1, chunk, s, jnp.logical_not(odd_lon))
        if not last:
            for part in range(1, len(faces)):
                pack_and_send(step + 1, part)
    for s, side in enumerate(sides):
        for chunk in range(stay):
            when(side[3], lambda: y_copy(STEPS - 1, chunk, s).wait_send())


def settle(sizes, sums, mean_out, scale_out, peer_sums, send_sem, recv_sem, count, between):
    n_lon = sizes[1]
    lon = lax.axis_index("lon")
    barrier = pltpu.get_barrier_semaphore()
    for shift in range(1, n_lon):
        pl.semaphore_signal(barrier, inc=1, device_id={"lon": lax.rem(lon + shift, n_lon)},
                            device_id_type=MESH)

    def copy(shift):
        return pltpu.make_async_remote_copy(
            src_ref=sums, dst_ref=peer_sums.at[shift - 1],
            send_sem=send_sem.at[shift - 1], recv_sem=recv_sem.at[shift - 1],
            device_id={"lon": lax.rem(lon + shift, n_lon)}, device_id_type=MESH)

    between()
    pl.semaphore_wait(barrier, n_lon - 1)
    for shift in range(1, n_lon):
        copy(shift).start()
    for shift in range(1, n_lon):
        copy(shift).wait_recv()
    for chunk in range(sums.shape[0]):
        for s in range(sums.shape[1]):
            total = [sums[chunk, s, q] for q in range(2)]
            for shift in range(1, n_lon):
                total = [total[q] + peer_sums[shift - 1, chunk, s, q] for q in range(2)]
            here = pl.ds(chunk * TILE, TILE)
            mean_out[s, here, :], scale_out[s, here, :] = close(total, count)
    for shift in range(1, n_lon):
        copy(shift).wait_send()


def settle_kept(sizes, count, sums_in, mean_out, scale_out, sums, peer_sums, send_sem, recv_sem):
    def between():
        sums[...] = sums_in[...]

    settle(sizes, sums, mean_out, scale_out, peer_sums, send_sem, recv_sem, count, between)


def finish(sizes, count, base, factor, halo, tail, mean_out, scale_out, sums, peer_sums, send_sem, recv_sem):
    late, I, K, M = base.shape
    high = halo.shape[2]

    def between():
        zero = jnp.zeros((TILE, M), jnp.float32)
        for s in range(late):
            for chunk in range(high // TILE):
                here, there = pl.ds(K - high + chunk * TILE, TILE), pl.ds(chunk * TILE, TILE)

                def body(b, totals):
                    r = pl.ds(b * ROWS, ROWS)
                    new = base[s, r, here, :] + factor[s, r, there, :] * halo[s, r, there, :]
                    tail[s, r, there, :] = new
                    return tally(new, totals)

                totals = lax.fori_loop(0, I // ROWS, body, (zero, zero))
                for q in range(2):
                    sums[chunk, s, q] = totals[q]

    settle(sizes, sums, mean_out, scale_out, peer_sums, send_sem, recv_sem, count, between)


def write_early(
    sizes, end, mean, scale, mean_kept, scale_kept, standardized, end_out, held, held_kept, sem,
):
    J, I, K, M = end.shape
    lat = lax.axis_index("lat")
    first, number = early_planes(sizes[0], lat, J)
    sides = lat_sides(sizes[0], lat, J)
    done = pl.ds(0, kept(K) * TILE)
    copies = [pltpu.make_async_copy(
        end.at[pl.ds(first, number)], end_out.at[pl.ds(first, number)], sem.at[0])]
    for s, side in enumerate(sides):
        copies.append(pltpu.make_async_copy(
            end.at[side[0], :, done, :], end_out.at[side[0], :, done, :], sem.at[1 + s]))
    for copy in copies:
        copy.start()
    for p in range(number):
        j = first + p
        offset, factor = mean[j], scale[j]

        @pl.loop(0, I // ROWS)
        def _(b):
            rows = pl.ds(b * ROWS, ROWS)
            held[p, rows] = (end[j, rows] - offset) * factor

        copies.append(pltpu.make_async_copy(
            held.at[p], standardized.at[j], sem.at[1 + len(sides) + p]))
        copies[-1].start()
    for s, side in enumerate(sides):
        offset, factor = mean_kept[s], scale_kept[s]

        @pl.loop(0, I // ROWS)
        def _(b):
            rows = pl.ds(b * ROWS, ROWS)
            held_kept[s, rows] = (end[side[0], rows, done, :] - offset) * factor

        copies.append(pltpu.make_async_copy(
            held_kept.at[s], standardized.at[side[0], :, done, :], sem.at[1 + len(sides) + number + s]))
        copies[-1].start()
    for copy in copies:
        copy.wait()


def write_late(sizes, tail, mean, scale, old_standardized, old_end, standardized, end_out, held, sem):
    late, I, high, M = tail.shape
    J, K = end_out.shape[0], end_out.shape[2]
    here = pl.ds(K - high, high)
    half = I // 2
    copies = []
    for s, side in enumerate(lat_sides(sizes[0], lax.axis_index("lat"), J)):
        j = side[0]
        copies.append(pltpu.make_async_copy(tail.at[s], end_out.at[j, :, here, :], sem.at[s, 0]))
        copies[-1].start()
        offset, scaling = mean[s], scale[s]
        for n in range(2):
            @pl.loop(0, half // ROWS)
            def _(b):
                rows = pl.ds(n * half + b * ROWS, ROWS)
                held[s, rows] = (tail[s, rows] - offset) * scaling

            part = pl.ds(n * half, half)
            copies.append(pltpu.make_async_copy(
                held.at[s, part], standardized.at[j, part, here, :], sem.at[s, 1 + n]))
            copies[-1].start()
    for copy in copies:
        copy.wait()


def cross(sizes, block):
    n_lat = sizes[0]
    if n_lat == 2:
        return lax.ppermute(block, "lat", [(0, 1), (1, 0)])
    up = lax.ppermute(block[1:], "lat", [(a, a + 1) for a in range(n_lat - 1)])
    down = lax.ppermute(block[:1], "lat", [(a + 1, a) for a in range(n_lat - 1)])
    return jnp.concatenate([up, down])


def shards(sizes, tracer, conductance, source):
    n_lat, n_lon, n_lev = sizes
    J, I, K, M = tracer.shape
    chunks = K // TILE
    f32 = jnp.float32
    dma = pltpu.SemaphoreType.DMA
    peers = max(n_lon - 1, 1)
    late = len(lat_sides(n_lat, 0, J))
    early = early_planes(n_lat, 0, J)[1]
    stay = kept(K)
    hbm, vmem = pl.BlockSpec(memory_space=pltpu.HBM), pl.BlockSpec(memory_space=pltpu.VMEM)
    out_of = (late, I, K - stay * TILE, M)
    scratch = [
        (J, I + 2, K, M), (J, I + 2, K, M), (J, I, K, M), (J, I, K, M), (2, late, I, K, M),
        (2, J, I, 1, M), (2, J, I, 1, M), (2, J, I, 1, M), (2, J, I, 1, M),
        (early, 2, K, M), (peers, early, 2, K, M),
    ]
    limit = sum(4 * math.prod(shape) for shape in scratch) + (2 << 20)
    end, mean, scale, base, factor, out, sums = pl.pallas_call(
        functools.partial(kernel, sizes),
        out_shape=[
            pltpu.VMEM((J, I, K, M), f32),
            pltpu.VMEM((J, K, M), f32),
            pltpu.VMEM((J, K, M), f32),
            pltpu.VMEM((late, I, K, M), f32),
            pltpu.VMEM(out_of, f32),
            pltpu.VMEM(out_of, f32),
            pltpu.VMEM((stay, late, 2, TILE, M), f32),
        ],
        in_specs=[hbm] * 3,
        out_specs=[vmem] * 7,
        scratch_shapes=[pltpu.VMEM(shape, f32) for shape in scratch] + [
            dma((3 + late,)),
            dma((STEPS, chunks, late)),
            dma((STEPS, chunks, late)),
            dma((STEPS, 2, 1 + late)),
            dma((STEPS, 2, 1 + late)),
            dma((STEPS, 2, 1 + late)),
            dma((STEPS, 2, 1 + late)),
            dma((peers,)),
            dma((peers,)),
        ],
        compiler_params=pltpu.CompilerParams(
            collective_id=0, has_side_effects=True, vmem_limit_bytes=limit),
    )(tracer, conductance, source)
    halo = cross(sizes, out)
    whole = jax.ShapeDtypeStruct((J, I, K, M), f32)

    def exchange_of(pieces):
        return [
            pltpu.VMEM((pieces, late, 2, TILE, M), f32),
            pltpu.VMEM((peers, pieces, late, 2, TILE, M), f32),
            dma((peers,)),
            dma((peers,)),
        ]

    mean_kept, scale_kept = pl.pallas_call(
        functools.partial(settle_kept, sizes, I * n_lon),
        out_shape=[pltpu.VMEM((late, stay * TILE, M), f32)] * 2,
        in_specs=[vmem],
        out_specs=[vmem] * 2,
        scratch_shapes=exchange_of(stay),
        compiler_params=pltpu.CompilerParams(
            collective_id=1, has_side_effects=True, vmem_limit_bytes=4 << 20),
        cost_estimate=pl.CostEstimate(flops=1 << 31, bytes_accessed=1 << 16, transcendentals=0),
    )(sums)
    standardized, end_out = pl.pallas_call(
        functools.partial(write_early, sizes),
        out_shape=[whole] * 2,
        in_specs=[vmem] * 5,
        out_specs=[hbm] * 2,
        scratch_shapes=[
            pltpu.VMEM((early, I, K, M), f32), pltpu.VMEM((late, I, stay * TILE, M), f32),
            dma((1 + early + 2 * late,)),
        ],
        compiler_params=pltpu.CompilerParams(vmem_limit_bytes=16 << 20),
        cost_estimate=pl.CostEstimate(
            flops=1 << 32, bytes_accessed=8 * early * I * K * M, transcendentals=0),
    )(end, mean, scale, mean_kept, scale_kept)
    tail, mean, scale = pl.pallas_call(
        functools.partial(finish, sizes, I * n_lon),
        out_shape=[pltpu.VMEM(out_of, f32)] + [pltpu.VMEM((late, K - stay * TILE, M), f32)] * 2,
        in_specs=[vmem] * 3,
        out_specs=[vmem] * 3,
        scratch_shapes=exchange_of(chunks - stay),
        compiler_params=pltpu.CompilerParams(
            collective_id=2, has_side_effects=True, vmem_limit_bytes=4 << 20),
    )(base, factor, halo)
    return pl.pallas_call(
        functools.partial(write_late, sizes),
        out_shape=[whole] * 2,
        in_specs=[vmem] * 3 + [hbm] * 2,
        out_specs=[hbm] * 2,
        input_output_aliases={3: 0, 4: 1},
        scratch_shapes=[pltpu.VMEM(out_of, f32), dma((late, 3))],
        compiler_params=pltpu.CompilerParams(vmem_limit_bytes=8 << 20),
    )(tail, mean, scale, standardized, end_out)


def solution(mesh):
    placed = P("lat", "lon", "lev", None)
    sizes = tuple(mesh.shape[axis] for axis in ("lat", "lon", "lev"))
    return jax.shard_map(
        functools.partial(shards, sizes),
        mesh=mesh,
        in_specs=(placed, placed, placed),
        out_specs=(placed, placed),
        check_vma=False,
    )
```

```python
import functools
import math

import jax
import jax.numpy as jnp
from jax import lax
from jax.experimental import pallas as pl
from jax.experimental.pallas import tpu as pltpu
from jax.sharding import PartitionSpec as P

STEPS = 3
GUESS = 1.0
TILE = 8
ROWS = 8
MESH = pl.DeviceIdType.MESH


def lat_sides(n_lat, lat, J):
    if n_lat == 2:
        return [(jnp.where(lat == 0, J - 1, 0), jnp.where(lat == 0, J - 2, 1), 1 - lat, None, 0)]
    return [(0, 1, lat - 1, lat > 0, 1), (J - 1, J - 2, lat + 1, lat < n_lat - 1, 0)]


def early_planes(n_lat, lat, J):
    if n_lat == 2:
        return jnp.where(lat == 0, 0, 1), J - 1
    return 1, J - 2


def kept(K):
    return K // TILE // 2


def close(total, count):
    offset = total[0] / count
    variance = total[1] / count - offset * offset
    return GUESS + offset, lax.rsqrt(variance + 0.0001)


def tally(new, totals):
    moved = new - GUESS
    return totals[0] + jnp.sum(moved, axis=0), totals[1] + jnp.sum(moved * moved, axis=0)


def when(condition, act):
    if condition is None:
        act()
    else:
        pl.when(condition)(act)


def kernel(
    sizes, tracer, conductance, source, end, mean_out, scale_out, base, factor, out, sums_late,
    even, odd, cond, sour, y_halo, z_lower, z_upper, z_first, z_last, sums_early, peer_early,
    peer_in, all_in,
    load_sem, first_sem, y_send, y_recv, x_send, x_recv, z_send, z_recv, early_send, early_recv,
):
    n_lat, n_lon, n_lev = sizes
    J, I, K, M = tracer.shape
    chunks = K // TILE
    blocks = I // ROWS
    count = I * n_lon
    lat, lon, lev = lax.axis_index("lat"), lax.axis_index("lon"), lax.axis_index("lev")
    below = {"lon": lon > 0, "lev": lev > 0}
    above = {"lon": lon < n_lon - 1, "lev": lev < n_lev - 1}
    index = {"lon": lon, "lev": lev}
    field = [even, odd]
    sides = lat_sides(n_lat, lat, J)
    first, number = early_planes(n_lat, lat, J)
    stay = kept(K)
    odd_lon = lon % 2 == 1
    rows_in = pl.ds(1, I)

    def levels(chunk):
        return pl.ds(chunk * TILE, TILE)

    def target(axis, way):
        return {axis: index[axis] + (1 if way == 0 else -1)}

    def y_copy(step, chunk, s):
        plane, _, peer, _, slot = sides[s]
        return pltpu.make_async_remote_copy(
            src_ref=field[step % 2].at[plane, rows_in, levels(chunk), :],
            dst_ref=y_halo.at[step % 2, slot, :, levels(chunk), :],
            send_sem=y_send.at[step, chunk, s], recv_sem=y_recv.at[step, chunk, slot],
            device_id={"lat": peer}, device_id_type=MESH)

    def y_arrival(step, chunk, s):
        plane, _, peer, _, _ = sides[s]
        return pltpu.make_async_remote_copy(
            src_ref=field[step % 2].at[plane, rows_in, levels(chunk), :],
            dst_ref=y_halo.at[step % 2, s, :, levels(chunk), :],
            send_sem=y_send.at[step, chunk, s], recv_sem=y_recv.at[step, chunk, s],
            device_id={"lat": peer}, device_id_type=MESH)

    faces = [pl.ds(first, number)] + [pl.ds(side[0], 1) for side in sides]

    def x_copy(step, way, part):
        buf = field[step % 2]
        return pltpu.make_async_remote_copy(
            src_ref=buf.at[faces[part], I if way == 0 else 1],
            dst_ref=buf.at[faces[part], 0 if way == 0 else I + 1],
            send_sem=x_send.at[step, way, part], recv_sem=x_recv.at[step, way, part],
            device_id=target("lon", way), device_id_type=MESH)

    def z_copy(step, way, part):
        src = z_last if way == 0 else z_first
        dst = z_lower if way == 0 else z_upper
        return pltpu.make_async_remote_copy(
            src_ref=src.at[step % 2, faces[part]], dst_ref=dst.at[step % 2, faces[part]],
            send_sem=z_send.at[step, way, part], recv_sem=z_recv.at[step, way, part],
            device_id=target("lev", way), device_id_type=MESH)

    def early_copy(shift):
        return pltpu.make_async_remote_copy(
            src_ref=sums_early, dst_ref=peer_early.at[shift - 1],
            send_sem=early_send.at[shift - 1], recv_sem=early_recv.at[shift - 1],
            device_id={"lon": lax.rem(lon + shift, n_lon)}, device_id_type=MESH)

    def sends(axis, way, act):
        pl.when((above if way == 0 else below)[axis])(act)

    def arrives(axis, way, act):
        pl.when((below if way == 0 else above)[axis])(act)

    first_loads = [[
        pltpu.make_async_copy(
            tracer.at[side[0], :, levels(chunk), :], even.at[side[0], rows_in, levels(chunk), :],
            first_sem.at[chunk, s])
        for s, side in enumerate(sides)] for chunk in range(chunks)]
    loads = [
        pltpu.make_async_copy(
            tracer.at[pl.ds(first, number)], even.at[pl.ds(first, number), rows_in], load_sem.at[0]),
        pltpu.make_async_copy(conductance, cond, load_sem.at[1]),
        pltpu.make_async_copy(source, sour, load_sem.at[2]),
    ]
    for chunk in range(chunks):
        for load in first_loads[chunk]:
            load.start()
    even_lat = lat % 2 == 0
    around = n_lon - 1 + below["lev"].astype(jnp.int32) + above["lev"].astype(jnp.int32)
    met = jnp.where(even_lat, around, 0)
    barrier = pltpu.get_barrier_semaphore()

    def signal_around(semaphore):
        for shift in range(1, n_lon):
            pl.semaphore_signal(semaphore, inc=1, device_id={"lon": lax.rem(lon + shift, n_lon)},
                                device_id_type=MESH)
        for way in (0, 1):
            sends("lev", way, lambda: pl.semaphore_signal(
                semaphore, inc=1, device_id=target("lev", way), device_id_type=MESH))

    for _, _, peer, exists, _ in sides:
        when(exists, lambda: pl.semaphore_signal(
            barrier, inc=1, device_id={"lat": peer}, device_id_type=MESH))
        met = met + (1 if exists is None else exists.astype(jnp.int32))
    pl.when(even_lat)(lambda: signal_around(barrier))
    loads[0].start()
    pl.semaphore_wait(barrier, met)

    for chunk in range(chunks):
        for s, side in enumerate(sides):
            first_loads[chunk][s].wait()
            when(side[3], lambda: y_copy(0, chunk, s).start())
    loads[1].start()
    loads[2].start()

    @pl.when(even_lat)
    def _():
        signal_around(peer_in)

    for s, side in enumerate(sides):
        if side[3] is not None:
            def no_y():
                @pl.loop(0, blocks)
                def _(b):
                    for p in range(2):
                        y_halo[p, s, pl.ds(b * ROWS, ROWS)] = jnp.zeros((ROWS, K, M), jnp.float32)
            pl.when(jnp.logical_not(side[3]))(no_y)
    for way in (0, 1):
        def no_x():
            for buf in field:
                for j in range(J):
                    buf[j, 0 if way == 0 else I + 1] = jnp.zeros((K, M), jnp.float32)
        pl.when(jnp.logical_not((below if way == 0 else above)["lon"]))(no_x)

        def no_z():
            @pl.loop(0, blocks)
            def _(b):
                for p in range(2):
                    for j in range(J):
                        (z_lower if way == 0 else z_upper)[p, j, pl.ds(b * ROWS, ROWS)] = (
                            jnp.zeros((ROWS, 1, M), jnp.float32))
        pl.when(jnp.logical_not((below if way == 0 else above)["lev"]))(no_z)

    def pack_and_send(step, part):
        buf = field[step % 2]
        start, extent = (first, number) if part == 0 else (sides[part - 1][0], 1)
        for way in (0, 1):
            sends("lon", way, lambda: x_copy(step, way, part).start())

        @pl.loop(0, extent * blocks)
        def _(q):
            j, r = start + q // blocks, (q % blocks) * ROWS
            z_first[step % 2, j, pl.ds(r, ROWS)] = buf[j, pl.ds(1 + r, ROWS), pl.ds(0, 1), :]
            z_last[step % 2, j, pl.ds(r, ROWS)] = buf[j, pl.ds(1 + r, ROWS), pl.ds(K - 1, 1), :]

        for way in (0, 1):
            sends("lev", way, lambda: z_copy(step, way, part).start())

    def faces_sent(step):
        for part in range(len(faces)):
            for way in (0, 1):
                sends("lon", way, lambda: x_copy(step, way, part).wait_send())
                sends("lev", way, lambda: z_copy(step, way, part).wait_send())

    def faces_arrive(step, part):
        for way in (0, 1):
            arrives("lon", way, lambda: x_copy(step, way, part).wait_recv())
            arrives("lev", way, lambda: z_copy(step, way, part).wait_recv())

    def next_rows(step, chunk, j, r, inward):
        buf = field[step % 2]
        here = levels(chunk)
        rows = pl.ds(1 + r, ROWS)
        mid = buf[j, rows, here, :]
        k = lax.broadcasted_iota(jnp.int32, mid.shape, 1)
        if chunk == 0:
            edge = jnp.broadcast_to(z_lower[step % 2, j, pl.ds(r, ROWS)], mid.shape)
        else:
            edge = pltpu.roll(buf[j, rows, levels(chunk - 1), :], 1, 1)
        k_lower = jnp.where(k == 0, edge, pltpu.roll(mid, 1, 1))
        if chunk == chunks - 1:
            edge = jnp.broadcast_to(z_upper[step % 2, j, pl.ds(r, ROWS)], mid.shape)
        else:
            edge = pltpu.roll(buf[j, rows, levels(chunk + 1), :], TILE - 1, 1)
        k_upper = jnp.where(k == TILE - 1, edge, pltpu.roll(mid, TILE - 1, 1))
        if inward is None:
            across = buf[j - 1, rows, here, :] + buf[j + 1, rows, here, :]
        else:
            across = buf[inward, rows, here, :]
        spread = (
            across + buf[j, pl.ds(r, ROWS), here, :] + buf[j, pl.ds(2 + r, ROWS), here, :]
            + k_lower + k_upper - 6.0 * mid)
        return mid + cond[j, pl.ds(r, ROWS), here, :] * spread + sour[j, pl.ds(r, ROWS), here, :]

    zero = jnp.zeros((TILE, M), jnp.float32)

    def early_plane(step, chunk, j, inward):
        def body(b, totals):
            r = b * ROWS
            new = next_rows(step, chunk, j, r, inward)
            if step < STEPS - 1:
                field[(step + 1) % 2][j, pl.ds(1 + r, ROWS), levels(chunk), :] = new
                return totals
            end[j, pl.ds(r, ROWS), levels(chunk), :] = new
            return tally(new, totals)

        if step < STEPS - 1:
            lax.fori_loop(0, blocks, lambda b, _: body(b, 0), 0)
        else:
            totals = lax.fori_loop(0, blocks, body, (zero, zero))
            for q in range(2):
                sums_early[j - first, q, levels(chunk), :] = totals[q]

    def early_part(step, chunk):
        @pl.loop(1, J - 1)
        def _(j):
            early_plane(step, chunk, j, None)

        if n_lat == 2:
            early_plane(step, chunk, jnp.where(lat == 0, 0, J - 1), jnp.where(lat == 0, 1, J - 2))

    def base_part(step, chunk):
        for s, (plane, inward, _, _, _) in enumerate(sides):
            @pl.loop(0, blocks)
            def _(b):
                r = b * ROWS
                base[s, pl.ds(r, ROWS), levels(chunk), :] = next_rows(step, chunk, plane, r, inward)

    def late_part(step, chunk, s):
        plane = sides[s][0]
        here = levels(chunk)

        def body(b, totals):
            r = pl.ds(b * ROWS, ROWS)
            new = base[s, r, here, :] + cond[plane, r, here, :] * y_halo[step % 2, s, r, here, :]
            if step < STEPS - 1:
                field[(step + 1) % 2][plane, pl.ds(1 + b * ROWS, ROWS), here, :] = new
                if step == STEPS - 2 and chunk >= stay:
                    out[s, r, levels(chunk - stay), :] = new
                return totals
            end[plane, r, here, :] = new
            return tally(new, totals)

        if step < STEPS - 1:
            lax.fori_loop(0, blocks, lambda b, _: body(b, 0), 0)
        else:
            totals = lax.fori_loop(0, blocks, body, (zero, zero))
            for q in range(2):
                sums_late[chunk, s, q] = totals[q]

    def y_start(step, chunk, s, condition=None):
        exists = sides[s][3]
        if condition is not None and exists is not None:
            condition = jnp.logical_and(condition, exists)
        when(exists if condition is None else condition, lambda: y_copy(step, chunk, s).start())

    @pl.when(even_lat)
    def _():
        pl.semaphore_wait(peer_in, around)
        pl.when(lat < n_lat - 1)(lambda: pl.semaphore_signal(
            all_in, inc=1, device_id={"lat": lat + 1}, device_id_type=MESH))

    @pl.when(jnp.logical_not(even_lat))
    def _():
        pl.semaphore_wait(all_in, 1)

    loads[0].wait()
    for part in range(len(faces)):
        pack_and_send(0, part)
    loads[1].wait()
    loads[2].wait()
    for step in range(STEPS):
        last = step == STEPS - 1
        if step >= 1:
            faces_sent(step - 1)
        faces_arrive(step, 0)
        for chunk in range(chunks):
            early_part(step, chunk)
            if last and chunk == max(chunks - 2, 0):
                for held in range(stay):
                    for s in range(len(sides)):
                        y_start(step, held, s, odd_lon)
        if last:
            for shift in range(1, n_lon):
                early_copy(shift).start()
        else:
            pack_and_send(step + 1, 0)
        for part in range(1, len(faces)):
            faces_arrive(step, part)
        for chunk in range(chunks):
            base_part(step, chunk)
        if step >= 1:
            for s, side in enumerate(sides):
                for chunk in range(chunks):
                    when(side[3], lambda: y_copy(step - 1, chunk, s).wait_send())
        if last:
            for s, side in enumerate(sides):
                @pl.loop(0, blocks)
                def _(b):
                    rows = pl.ds(b * ROWS, ROWS)
                    factor[s, rows] = cond[side[0], rows, pl.ds(stay * TILE, K - stay * TILE), :]
            faces_sent(step)
            for shift in range(1, n_lon):
                early_copy(shift).wait_recv()

            @pl.loop(0, number)
            def _(p):
                total = [sums_early[p, q] for q in range(2)]
                for shift in range(1, n_lon):
                    total = [total[q] + peer_early[shift - 1, p, q] for q in range(2)]
                mean_out[first + p], scale_out[first + p] = close(total, count)

            for shift in range(1, n_lon):
                early_copy(shift).wait_send()
        for chunk in range(stay if last else chunks):
            for s, side in enumerate(sides):
                when(side[3], lambda: y_arrival(step, chunk, s).wait_recv())
                late_part(step, chunk, s)
                if step < STEPS - 2:
                    y_start(step + 1, chunk, s)
                elif not last and chunk < stay:
                    y_start(step + 1, chunk, s, jnp.logical_not(odd_lon))
        if not last:
            for part in range(1, len(faces)):
                pack_and_send(step + 1, part)
    for s, side in enumerate(sides):
        for chunk in range(stay):
            when(side[3], lambda: y_copy(STEPS - 1, chunk, s).wait_send())


def settle(sizes, sums, mean_out, scale_out, peer_sums, send_sem, recv_sem, count, between):
    n_lon = sizes[1]
    lon = lax.axis_index("lon")
    barrier = pltpu.get_barrier_semaphore()
    for shift in range(1, n_lon):
        pl.semaphore_signal(barrier, inc=1, device_id={"lon": lax.rem(lon + shift, n_lon)},
                            device_id_type=MESH)

    def copy(shift):
        return pltpu.make_async_remote_copy(
            src_ref=sums, dst_ref=peer_sums.at[shift - 1],
            send_sem=send_sem.at[shift - 1], recv_sem=recv_sem.at[shift - 1],
            device_id={"lon": lax.rem(lon + shift, n_lon)}, device_id_type=MESH)

    between()
    pl.semaphore_wait(barrier, n_lon - 1)
    for shift in range(1, n_lon):
        copy(shift).start()
    for shift in range(1, n_lon):
        copy(shift).wait_recv()
    for chunk in range(sums.shape[0]):
        for s in range(sums.shape[1]):
            total = [sums[chunk, s, q] for q in range(2)]
            for shift in range(1, n_lon):
                total = [total[q] + peer_sums[shift - 1, chunk, s, q] for q in range(2)]
            here = pl.ds(chunk * TILE, TILE)
            mean_out[s, here, :], scale_out[s, here, :] = close(total, count)
    for shift in range(1, n_lon):
        copy(shift).wait_send()


def settle_kept(sizes, count, sums_in, mean_out, scale_out, sums, peer_sums, send_sem, recv_sem):
    def between():
        sums[...] = sums_in[...]

    settle(sizes, sums, mean_out, scale_out, peer_sums, send_sem, recv_sem, count, between)


def finish(sizes, count, base, factor, halo, tail, mean_out, scale_out, sums, peer_sums, send_sem, recv_sem):
    late, I, K, M = base.shape
    high = halo.shape[2]

    def between():
        zero = jnp.zeros((TILE, M), jnp.float32)
        for s in range(late):
            for chunk in range(high // TILE):
                here, there = pl.ds(K - high + chunk * TILE, TILE), pl.ds(chunk * TILE, TILE)

                def body(b, totals):
                    r = pl.ds(b * ROWS, ROWS)
                    new = base[s, r, here, :] + factor[s, r, there, :] * halo[s, r, there, :]
                    tail[s, r, there, :] = new
                    return tally(new, totals)

                totals = lax.fori_loop(0, I // ROWS, body, (zero, zero))
                for q in range(2):
                    sums[chunk, s, q] = totals[q]

    settle(sizes, sums, mean_out, scale_out, peer_sums, send_sem, recv_sem, count, between)


def write_early(
    sizes, end, mean, scale, mean_kept, scale_kept, standardized, end_out, held, held_kept, sem,
):
    J, I, K, M = end.shape
    lat = lax.axis_index("lat")
    first, number = early_planes(sizes[0], lat, J)
    sides = lat_sides(sizes[0], lat, J)
    done = pl.ds(0, kept(K) * TILE)
    copies = [pltpu.make_async_copy(
        end.at[pl.ds(first, number)], end_out.at[pl.ds(first, number)], sem.at[0])]
    for s, side in enumerate(sides):
        copies.append(pltpu.make_async_copy(
            end.at[side[0], :, done, :], end_out.at[side[0], :, done, :], sem.at[1 + s]))
    for copy in copies:
        copy.start()
    for p in range(number):
        j = first + p
        offset, factor = mean[j], scale[j]

        @pl.loop(0, I // ROWS)
        def _(b):
            rows = pl.ds(b * ROWS, ROWS)
            held[p, rows] = (end[j, rows] - offset) * factor

        copies.append(pltpu.make_async_copy(
            held.at[p], standardized.at[j], sem.at[1 + len(sides) + p]))
        copies[-1].start()
    for s, side in enumerate(sides):
        offset, factor = mean_kept[s], scale_kept[s]

        @pl.loop(0, I // ROWS)
        def _(b):
            rows = pl.ds(b * ROWS, ROWS)
            held_kept[s, rows] = (end[side[0], rows, done, :] - offset) * factor

        copies.append(pltpu.make_async_copy(
            held_kept.at[s], standardized.at[side[0], :, done, :], sem.at[1 + len(sides) + number + s]))
        copies[-1].start()
    for copy in copies:
        copy.wait()


def write_late(sizes, tail, mean, scale, old_standardized, old_end, standardized, end_out, held, sem):
    late, I, high, M = tail.shape
    J, K = end_out.shape[0], end_out.shape[2]
    here = pl.ds(K - high, high)
    half = I // 2
    copies = []
    for s, side in enumerate(lat_sides(sizes[0], lax.axis_index("lat"), J)):
        j = side[0]
        copies.append(pltpu.make_async_copy(tail.at[s], end_out.at[j, :, here, :], sem.at[s, 0]))
        copies[-1].start()
        offset, scaling = mean[s], scale[s]
        for n in range(2):
            @pl.loop(0, half // ROWS)
            def _(b):
                rows = pl.ds(n * half + b * ROWS, ROWS)
                held[s, rows] = (tail[s, rows] - offset) * scaling

            part = pl.ds(n * half, half)
            copies.append(pltpu.make_async_copy(
                held.at[s, part], standardized.at[j, part, here, :], sem.at[s, 1 + n]))
            copies[-1].start()
    for copy in copies:
        copy.wait()


def cross(sizes, block):
    n_lat = sizes[0]
    if n_lat == 2:
        return lax.ppermute(block, "lat", [(0, 1), (1, 0)])
    up = lax.ppermute(block[1:], "lat", [(a, a + 1) for a in range(n_lat - 1)])
    down = lax.ppermute(block[:1], "lat", [(a + 1, a) for a in range(n_lat - 1)])
    return jnp.concatenate([up, down])


def shards(sizes, tracer, conductance, source):
    n_lat, n_lon, n_lev = sizes
    J, I, K, M = tracer.shape
    chunks = K // TILE
    f32 = jnp.float32
    dma = pltpu.SemaphoreType.DMA
    peers = max(n_lon - 1, 1)
    late = len(lat_sides(n_lat, 0, J))
    early = early_planes(n_lat, 0, J)[1]
    stay = kept(K)
    hbm, vmem = pl.BlockSpec(memory_space=pltpu.HBM), pl.BlockSpec(memory_space=pltpu.VMEM)
    out_of = (late, I, K - stay * TILE, M)
    scratch = [
        (J, I + 2, K, M), (J, I + 2, K, M), (J, I, K, M), (J, I, K, M), (2, late, I, K, M),
        (2, J, I, 1, M), (2, J, I, 1, M), (2, J, I, 1, M), (2, J, I, 1, M),
        (early, 2, K, M), (peers, early, 2, K, M),
    ]
    limit = sum(4 * math.prod(shape) for shape in scratch) + (2 << 20)
    end, mean, scale, base, factor, out, sums = pl.pallas_call(
        functools.partial(kernel, sizes),
        out_shape=[
            pltpu.VMEM((J, I, K, M), f32),
            pltpu.VMEM((J, K, M), f32),
            pltpu.VMEM((J, K, M), f32),
            pltpu.VMEM((late, I, K, M), f32),
            pltpu.VMEM(out_of, f32),
            pltpu.VMEM(out_of, f32),
            pltpu.VMEM((stay, late, 2, TILE, M), f32),
        ],
        in_specs=[hbm] * 3,
        out_specs=[vmem] * 7,
        scratch_shapes=[pltpu.VMEM(shape, f32) for shape in scratch] + [
            pltpu.SemaphoreType.REGULAR,
            pltpu.SemaphoreType.REGULAR,
            dma((3,)),
            dma((chunks, late)),
            dma((STEPS, chunks, late)),
            dma((STEPS, chunks, late)),
            dma((STEPS, 2, 1 + late)),
            dma((STEPS, 2, 1 + late)),
            dma((STEPS, 2, 1 + late)),
            dma((STEPS, 2, 1 + late)),
            dma((peers,)),
            dma((peers,)),
        ],
        compiler_params=pltpu.CompilerParams(
            collective_id=0, has_side_effects=True, vmem_limit_bytes=limit),
    )(tracer, conductance, source)
    halo = cross(sizes, out)
    whole = jax.ShapeDtypeStruct((J, I, K, M), f32)

    def exchange_of(pieces):
        return [
            pltpu.VMEM((pieces, late, 2, TILE, M), f32),
            pltpu.VMEM((peers, pieces, late, 2, TILE, M), f32),
            dma((peers,)),
            dma((peers,)),
        ]

    mean_kept, scale_kept = pl.pallas_call(
        functools.partial(settle_kept, sizes, I * n_lon),
        out_shape=[pltpu.VMEM((late, stay * TILE, M), f32)] * 2,
        in_specs=[vmem],
        out_specs=[vmem] * 2,
        scratch_shapes=exchange_of(stay),
        compiler_params=pltpu.CompilerParams(
            collective_id=1, has_side_effects=True, vmem_limit_bytes=4 << 20),
        cost_estimate=pl.CostEstimate(flops=1 << 31, bytes_accessed=1 << 16, transcendentals=0),
    )(sums)
    standardized, end_out = pl.pallas_call(
        functools.partial(write_early, sizes),
        out_shape=[whole] * 2,
        in_specs=[vmem] * 5,
        out_specs=[hbm] * 2,
        scratch_shapes=[
            pltpu.VMEM((early, I, K, M), f32), pltpu.VMEM((late, I, stay * TILE, M), f32),
            dma((1 + early + 2 * late,)),
        ],
        compiler_params=pltpu.CompilerParams(vmem_limit_bytes=16 << 20),
        cost_estimate=pl.CostEstimate(
            flops=1 << 32, bytes_accessed=8 * early * I * K * M, transcendentals=0),
    )(end, mean, scale, mean_kept, scale_kept)
    tail, mean, scale = pl.pallas_call(
        functools.partial(finish, sizes, I * n_lon),
        out_shape=[pltpu.VMEM(out_of, f32)] + [pltpu.VMEM((late, K - stay * TILE, M), f32)] * 2,
        in_specs=[vmem] * 3,
        out_specs=[vmem] * 3,
        scratch_shapes=exchange_of(chunks - stay),
        compiler_params=pltpu.CompilerParams(
            collective_id=2, has_side_effects=True, vmem_limit_bytes=4 << 20),
    )(base, factor, halo)
    return pl.pallas_call(
        functools.partial(write_late, sizes),
        out_shape=[whole] * 2,
        in_specs=[vmem] * 3 + [hbm] * 2,
        out_specs=[hbm] * 2,
        input_output_aliases={3: 0, 4: 1},
        scratch_shapes=[pltpu.VMEM(out_of, f32), dma((late, 3))],
        compiler_params=pltpu.CompilerParams(vmem_limit_bytes=8 << 20),
    )(tail, mean, scale, standardized, end_out)


def solution(mesh):
    placed = P("lat", "lon", "lev", None)
    sizes = tuple(mesh.shape[axis] for axis in ("lat", "lon", "lev"))
    return jax.shard_map(
        functools.partial(shards, sizes),
        mesh=mesh,
        in_specs=(placed, placed, placed),
        out_specs=(placed, placed),
        check_vma=False,
    )
```

```python
import functools
import math

import jax
import jax.numpy as jnp
from jax import lax
from jax.experimental import pallas as pl
from jax.experimental.pallas import tpu as pltpu
from jax.sharding import PartitionSpec as P

STEPS = 3
GUESS = 1.0
TILE = 8
ROWS = 8
MESH = pl.DeviceIdType.MESH


def lat_sides(n_lat, lat, J):
    if n_lat == 2:
        return [(jnp.where(lat == 0, J - 1, 0), jnp.where(lat == 0, J - 2, 1), 1 - lat, None, 0)]
    return [(0, 1, lat - 1, lat > 0, 1), (J - 1, J - 2, lat + 1, lat < n_lat - 1, 0)]


def early_planes(n_lat, lat, J):
    if n_lat == 2:
        return jnp.where(lat == 0, 0, 1), J - 1
    return 1, J - 2


def kept(K):
    return K // TILE // 2


def spans(K):
    start, last = kept(K) * TILE, K - TILE
    return [(low, high) for low, high in ((start, last), (last, K)) if high > low]


def close(total, count):
    offset = total[0] / count
    variance = total[1] / count - offset * offset
    return GUESS + offset, lax.rsqrt(variance + 0.0001)


def tally(new, totals):
    moved = new - GUESS
    return totals[0] + jnp.sum(moved, axis=0), totals[1] + jnp.sum(moved * moved, axis=0)


def when(condition, act):
    if condition is None:
        act()
    else:
        pl.when(condition)(act)


def kernel(sizes, tracer, conductance, source, end, mean_out, scale_out, base, factor, sums_late, *rest):
    cuts = spans(tracer.shape[2])
    outs = rest[:len(cuts)]
    (
        even, odd, cond, sour, y_halo, z_lower, z_upper, z_first, z_last, sums_early, peer_early,
        peer_in, all_in,
        load_sem, first_sem, y_send, y_recv, x_send, x_recv, z_send, z_recv, early_send, early_recv,
    ) = rest[len(cuts):]
    n_lat, n_lon, n_lev = sizes
    J, I, K, M = tracer.shape
    chunks = K // TILE
    blocks = I // ROWS
    count = I * n_lon
    lat, lon, lev = lax.axis_index("lat"), lax.axis_index("lon"), lax.axis_index("lev")
    below = {"lon": lon > 0, "lev": lev > 0}
    above = {"lon": lon < n_lon - 1, "lev": lev < n_lev - 1}
    index = {"lon": lon, "lev": lev}
    field = [even, odd]
    sides = lat_sides(n_lat, lat, J)
    first, number = early_planes(n_lat, lat, J)
    stay = kept(K)
    odd_lon = lon % 2 == 1
    rows_in = pl.ds(1, I)

    def levels(chunk):
        return pl.ds(chunk * TILE, TILE)

    def target(axis, way):
        return {axis: index[axis] + (1 if way == 0 else -1)}

    def y_copy(step, chunk, s):
        plane, _, peer, _, slot = sides[s]
        return pltpu.make_async_remote_copy(
            src_ref=field[step % 2].at[plane, rows_in, levels(chunk), :],
            dst_ref=y_halo.at[step % 2, slot, :, levels(chunk), :],
            send_sem=y_send.at[step, chunk, s], recv_sem=y_recv.at[step, chunk, slot],
            device_id={"lat": peer}, device_id_type=MESH)

    def y_arrival(step, chunk, s):
        plane, _, peer, _, _ = sides[s]
        return pltpu.make_async_remote_copy(
            src_ref=field[step % 2].at[plane, rows_in, levels(chunk), :],
            dst_ref=y_halo.at[step % 2, s, :, levels(chunk), :],
            send_sem=y_send.at[step, chunk, s], recv_sem=y_recv.at[step, chunk, s],
            device_id={"lat": peer}, device_id_type=MESH)

    faces = [pl.ds(first, number)] + [pl.ds(side[0], 1) for side in sides]

    def x_copy(step, way, part):
        buf = field[step % 2]
        return pltpu.make_async_remote_copy(
            src_ref=buf.at[faces[part], I if way == 0 else 1],
            dst_ref=buf.at[faces[part], 0 if way == 0 else I + 1],
            send_sem=x_send.at[step, way, part], recv_sem=x_recv.at[step, way, part],
            device_id=target("lon", way), device_id_type=MESH)

    def z_copy(step, way, part):
        src = z_last if way == 0 else z_first
        dst = z_lower if way == 0 else z_upper
        return pltpu.make_async_remote_copy(
            src_ref=src.at[step % 2, faces[part]], dst_ref=dst.at[step % 2, faces[part]],
            send_sem=z_send.at[step, way, part], recv_sem=z_recv.at[step, way, part],
            device_id=target("lev", way), device_id_type=MESH)

    def early_copy(shift):
        return pltpu.make_async_remote_copy(
            src_ref=sums_early, dst_ref=peer_early.at[shift - 1],
            send_sem=early_send.at[shift - 1], recv_sem=early_recv.at[shift - 1],
            device_id={"lon": lax.rem(lon + shift, n_lon)}, device_id_type=MESH)

    def sends(axis, way, act):
        pl.when((above if way == 0 else below)[axis])(act)

    def arrives(axis, way, act):
        pl.when((below if way == 0 else above)[axis])(act)

    first_loads = [[
        pltpu.make_async_copy(
            tracer.at[side[0], :, levels(chunk), :], even.at[side[0], rows_in, levels(chunk), :],
            first_sem.at[chunk, s])
        for s, side in enumerate(sides)] for chunk in range(chunks)]
    loads = [
        pltpu.make_async_copy(
            tracer.at[pl.ds(first, number)], even.at[pl.ds(first, number), rows_in], load_sem.at[0]),
        pltpu.make_async_copy(conductance, cond, load_sem.at[1]),
        pltpu.make_async_copy(source, sour, load_sem.at[2]),
    ]
    for chunk in range(chunks):
        for load in first_loads[chunk]:
            load.start()
    even_lat = lat % 2 == 0
    around = n_lon - 1 + below["lev"].astype(jnp.int32) + above["lev"].astype(jnp.int32)
    met = jnp.where(even_lat, around, 0)
    barrier = pltpu.get_barrier_semaphore()

    def signal_around(semaphore):
        for shift in range(1, n_lon):
            pl.semaphore_signal(semaphore, inc=1, device_id={"lon": lax.rem(lon + shift, n_lon)},
                                device_id_type=MESH)
        for way in (0, 1):
            sends("lev", way, lambda: pl.semaphore_signal(
                semaphore, inc=1, device_id=target("lev", way), device_id_type=MESH))

    for _, _, peer, exists, _ in sides:
        when(exists, lambda: pl.semaphore_signal(
            barrier, inc=1, device_id={"lat": peer}, device_id_type=MESH))
        met = met + (1 if exists is None else exists.astype(jnp.int32))
    pl.when(even_lat)(lambda: signal_around(barrier))
    loads[0].start()
    pl.semaphore_wait(barrier, met)

    for chunk in range(chunks):
        for s, side in enumerate(sides):
            first_loads[chunk][s].wait()
            when(side[3], lambda: y_copy(0, chunk, s).start())
    loads[1].start()
    loads[2].start()

    @pl.when(even_lat)
    def _():
        signal_around(peer_in)

    for s, side in enumerate(sides):
        if side[3] is not None:
            def no_y():
                @pl.loop(0, blocks)
                def _(b):
                    for p in range(2):
                        y_halo[p, s, pl.ds(b * ROWS, ROWS)] = jnp.zeros((ROWS, K, M), jnp.float32)
            pl.when(jnp.logical_not(side[3]))(no_y)
    for way in (0, 1):
        def no_x():
            for buf in field:
                for j in range(J):
                    buf[j, 0 if way == 0 else I + 1] = jnp.zeros((K, M), jnp.float32)
        pl.when(jnp.logical_not((below if way == 0 else above)["lon"]))(no_x)

        def no_z():
            @pl.loop(0, blocks)
            def _(b):
                for p in range(2):
                    for j in range(J):
                        (z_lower if way == 0 else z_upper)[p, j, pl.ds(b * ROWS, ROWS)] = (
                            jnp.zeros((ROWS, 1, M), jnp.float32))
        pl.when(jnp.logical_not((below if way == 0 else above)["lev"]))(no_z)

    def pack_and_send(step, part):
        buf = field[step % 2]
        start, extent = (first, number) if part == 0 else (sides[part - 1][0], 1)
        for way in (0, 1):
            sends("lon", way, lambda: x_copy(step, way, part).start())

        @pl.loop(0, extent * blocks)
        def _(q):
            j, r = start + q // blocks, (q % blocks) * ROWS
            z_first[step % 2, j, pl.ds(r, ROWS)] = buf[j, pl.ds(1 + r, ROWS), pl.ds(0, 1), :]
            z_last[step % 2, j, pl.ds(r, ROWS)] = buf[j, pl.ds(1 + r, ROWS), pl.ds(K - 1, 1), :]

        for way in (0, 1):
            sends("lev", way, lambda: z_copy(step, way, part).start())

    def faces_sent(step):
        for part in range(len(faces)):
            for way in (0, 1):
                sends("lon", way, lambda: x_copy(step, way, part).wait_send())
                sends("lev", way, lambda: z_copy(step, way, part).wait_send())

    def faces_arrive(step, part):
        for way in (0, 1):
            arrives("lon", way, lambda: x_copy(step, way, part).wait_recv())
            arrives("lev", way, lambda: z_copy(step, way, part).wait_recv())

    def next_rows(step, chunk, j, r, inward):
        buf = field[step % 2]
        here = levels(chunk)
        rows = pl.ds(1 + r, ROWS)
        mid = buf[j, rows, here, :]
        k = lax.broadcasted_iota(jnp.int32, mid.shape, 1)
        if chunk == 0:
            edge = jnp.broadcast_to(z_lower[step % 2, j, pl.ds(r, ROWS)], mid.shape)
        else:
            edge = pltpu.roll(buf[j, rows, levels(chunk - 1), :], 1, 1)
        k_lower = jnp.where(k == 0, edge, pltpu.roll(mid, 1, 1))
        if chunk == chunks - 1:
            edge = jnp.broadcast_to(z_upper[step % 2, j, pl.ds(r, ROWS)], mid.shape)
        else:
            edge = pltpu.roll(buf[j, rows, levels(chunk + 1), :], TILE - 1, 1)
        k_upper = jnp.where(k == TILE - 1, edge, pltpu.roll(mid, TILE - 1, 1))
        if inward is None:
            across = buf[j - 1, rows, here, :] + buf[j + 1, rows, here, :]
        else:
            across = buf[inward, rows, here, :]
        spread = (
            across + buf[j, pl.ds(r, ROWS), here, :] + buf[j, pl.ds(2 + r, ROWS), here, :]
            + k_lower + k_upper - 6.0 * mid)
        return mid + cond[j, pl.ds(r, ROWS), here, :] * spread + sour[j, pl.ds(r, ROWS), here, :]

    zero = jnp.zeros((TILE, M), jnp.float32)

    def early_plane(step, chunk, j, inward):
        def body(b, totals):
            r = b * ROWS
            new = next_rows(step, chunk, j, r, inward)
            if step < STEPS - 1:
                field[(step + 1) % 2][j, pl.ds(1 + r, ROWS), levels(chunk), :] = new
                return totals
            end[j, pl.ds(r, ROWS), levels(chunk), :] = new
            return tally(new, totals)

        if step < STEPS - 1:
            lax.fori_loop(0, blocks, lambda b, _: body(b, 0), 0)
        else:
            totals = lax.fori_loop(0, blocks, body, (zero, zero))
            for q in range(2):
                sums_early[j - first, q, levels(chunk), :] = totals[q]

    def early_part(step, chunk):
        @pl.loop(1, J - 1)
        def _(j):
            early_plane(step, chunk, j, None)

        if step == STEPS - 1 and chunk == max(chunks - 2, 0):
            for held in range(stay):
                for s in range(len(sides)):
                    y_start(step, held, s, odd_lon)
        if n_lat == 2:
            early_plane(step, chunk, jnp.where(lat == 0, 0, J - 1), jnp.where(lat == 0, 1, J - 2))

    def base_part(step, chunk):
        for s, (plane, inward, _, _, _) in enumerate(sides):
            @pl.loop(0, blocks)
            def _(b):
                r = b * ROWS
                base[s, pl.ds(r, ROWS), levels(chunk), :] = next_rows(step, chunk, plane, r, inward)

    def late_part(step, chunk, s):
        plane = sides[s][0]
        here = levels(chunk)

        def body(b, totals):
            r = pl.ds(b * ROWS, ROWS)
            new = base[s, r, here, :] + cond[plane, r, here, :] * y_halo[step % 2, s, r, here, :]
            if step < STEPS - 1:
                field[(step + 1) % 2][plane, pl.ds(1 + b * ROWS, ROWS), here, :] = new
                if step == STEPS - 2:
                    for out, (low, high) in zip(outs, cuts):
                        if low <= chunk * TILE < high:
                            out[s, r, pl.ds(chunk * TILE - low, TILE), :] = new
                return totals
            end[plane, r, here, :] = new
            return tally(new, totals)

        if step < STEPS - 1:
            lax.fori_loop(0, blocks, lambda b, _: body(b, 0), 0)
        else:
            totals = lax.fori_loop(0, blocks, body, (zero, zero))
            for q in range(2):
                sums_late[chunk, s, q] = totals[q]

    def y_start(step, chunk, s, condition=None):
        exists = sides[s][3]
        if condition is not None and exists is not None:
            condition = jnp.logical_and(condition, exists)
        when(exists if condition is None else condition, lambda: y_copy(step, chunk, s).start())

    @pl.when(even_lat)
    def _():
        pl.semaphore_wait(peer_in, around)
        pl.when(lat < n_lat - 1)(lambda: pl.semaphore_signal(
            all_in, inc=1, device_id={"lat": lat + 1}, device_id_type=MESH))

    @pl.when(jnp.logical_not(even_lat))
    def _():
        pl.semaphore_wait(all_in, 1)

    loads[0].wait()
    for part in range(len(faces)):
        pack_and_send(0, part)
    loads[1].wait()
    loads[2].wait()
    for step in range(STEPS):
        last = step == STEPS - 1
        if step >= 1:
            faces_sent(step - 1)
        faces_arrive(step, 0)
        for chunk in range(chunks):
            early_part(step, chunk)
        if last:
            for shift in range(1, n_lon):
                early_copy(shift).start()
        else:
            pack_and_send(step + 1, 0)
        for part in range(1, len(faces)):
            faces_arrive(step, part)
        for chunk in range(chunks):
            base_part(step, chunk)
        if step >= 1:
            for s, side in enumerate(sides):
                for chunk in range(chunks):
                    when(side[3], lambda: y_copy(step - 1, chunk, s).wait_send())
        if last:
            for s, side in enumerate(sides):
                @pl.loop(0, blocks)
                def _(b):
                    rows = pl.ds(b * ROWS, ROWS)
                    factor[s, rows] = cond[side[0], rows, pl.ds(stay * TILE, K - stay * TILE), :]
            faces_sent(step)
            for shift in range(1, n_lon):
                early_copy(shift).wait_recv()

            @pl.loop(0, number)
            def _(p):
                total = [sums_early[p, q] for q in range(2)]
                for shift in range(1, n_lon):
                    total = [total[q] + peer_early[shift - 1, p, q] for q in range(2)]
                mean_out[first + p], scale_out[first + p] = close(total, count)

            for shift in range(1, n_lon):
                early_copy(shift).wait_send()
        for chunk in range(stay if last else chunks):
            for s, side in enumerate(sides):
                when(side[3], lambda: y_arrival(step, chunk, s).wait_recv())
                late_part(step, chunk, s)
                if step < STEPS - 2:
                    y_start(step + 1, chunk, s)
                elif not last and chunk < stay:
                    y_start(step + 1, chunk, s, jnp.logical_not(odd_lon))
        if not last:
            for part in range(1, len(faces)):
                pack_and_send(step + 1, part)
    for s, side in enumerate(sides):
        for chunk in range(stay):
            when(side[3], lambda: y_copy(STEPS - 1, chunk, s).wait_send())


def finish(sizes, base, factor, sums_in, end, out, *rest):
    halos, (
        tail, ready, mean_out, scale_out, landing, sums, peer_sums, late_in, y_send, y_recv, send_sem, recv_sem,
    ) = rest[:-12], rest[-12:]
    n_lat, n_lon, _ = sizes
    late, I, K, M = base.shape
    chunks, stay, cuts = K // TILE, kept(K), spans(K)
    lat, lon = lax.axis_index("lat"), lax.axis_index("lon")
    even_lon = lon % 2 == 0
    n_odd = n_lon // 2
    sides = lat_sides(n_lat, lat, end.shape[0])
    peers = [lax.rem(lon + shift, n_lon) for shift in range(1, n_lon)]
    groups = [group for group in (list(range(stay)), list(range(stay, chunks - 1)), [chunks - 1]) if group]
    pieces = [pl.ds(group[0], len(group)) for group in groups]

    def y_copy(s, slot):
        return pltpu.make_async_remote_copy(
            src_ref=out.at[s], dst_ref=landing.at[slot], send_sem=y_send.at[s], recv_sem=y_recv.at[slot],
            device_id={"lat": sides[s][2]}, device_id_type=MESH)

    def sum_copy(piece, p):
        return pltpu.make_async_remote_copy(
            src_ref=sums.at[pieces[piece]], dst_ref=peer_sums.at[p, pieces[piece]],
            send_sem=send_sem.at[piece, p], recv_sem=recv_sem.at[piece, p],
            device_id={"lon": peers[p]}, device_id_type=MESH)

    def send_sums(piece):
        for p in range(n_lon - 1):
            sum_copy(piece, p).start()

    def add(chunk, s, arrived, start):
        here = pl.ds(chunk * TILE, TILE)
        there, came = pl.ds((chunk - stay) * TILE, TILE), pl.ds(chunk * TILE - start, TILE)
        zero = jnp.zeros((TILE, M), jnp.float32)

        def body(b, totals):
            r = pl.ds(b * ROWS, ROWS)
            new = base[s, r, here, :] + factor[s, r, there, :] * arrived[s, r, came, :]
            tail[s, r, there, :] = new
            return tally(new, totals)

        totals = lax.fori_loop(0, I // ROWS, body, (zero, zero))
        for q in range(2):
            sums[chunk, s, q] = totals[q]

    barrier = pltpu.get_barrier_semaphore()
    met = jnp.where(even_lon, n_lon - n_odd - 1, n_lon - 1)
    for _, _, peer, exists, _ in sides:
        when(exists, lambda: pl.semaphore_signal(
            barrier, inc=1, device_id={"lat": peer}, device_id_type=MESH))
        met = met + (1 if exists is None else exists.astype(jnp.int32))
    for peer in peers:
        pl.when(jnp.logical_or(even_lon, peer % 2 == 1))(lambda: pl.semaphore_signal(
            barrier, inc=1, device_id={"lon": peer}, device_id_type=MESH))
    pl.semaphore_wait(barrier, met)
    for s, side in enumerate(sides):
        when(side[3], lambda: y_copy(s, side[4]).start())

    @pl.when(jnp.logical_not(even_lon))
    def _():
        for peer in peers:
            pl.when(peer % 2 == 0)(lambda: pl.semaphore_signal(
                late_in, inc=1, device_id={"lon": peer}, device_id_type=MESH))

    for s, side in enumerate(sides):
        if side[3] is not None:
            @pl.when(jnp.logical_not(side[3]))
            def _():
                @pl.loop(0, I // ROWS)
                def _(b):
                    landing[s, pl.ds(b * ROWS, ROWS)] = jnp.zeros((ROWS,) + landing.shape[2:], jnp.float32)
        for chunk in range(chunks - 1):
            if chunk < stay:
                for q in range(2):
                    sums[chunk, s, q] = sums_in[chunk, s, q]
            else:
                add(chunk, s, halos[0], cuts[0][0])
    pl.when(even_lon)(lambda: pl.semaphore_wait(late_in, n_odd))
    values = {}

    def settle(piece):
        for p in range(n_lon - 1):
            sum_copy(piece, p).wait_recv()
        for chunk in groups[piece]:
            of_sides = []
            for s in range(late):
                total = [sums[chunk, s, q] for q in range(2)]
                for p in range(n_lon - 1):
                    total = [total[q] + peer_sums[p, chunk, s, q] for q in range(2)]
                of_sides.append(close(total, I * n_lon))
            values[chunk] = [jnp.stack(part) for part in zip(*of_sides)]

    for piece in range(len(groups) - 1):
        send_sums(piece)
    for piece, group in enumerate(groups[:-1]):
        settle(piece)
        for chunk in group:
            here = pl.ds(chunk * TILE, TILE)
            for s, side in enumerate(sides):
                offset, scaling = values[chunk][0][s], values[chunk][1][s]

                @pl.loop(0, I // ROWS)
                def _(b):
                    r = pl.ds(b * ROWS, ROWS)
                    if chunk < stay:
                        new = end[side[0], r, here, :]
                    else:
                        new = tail[s, r, pl.ds((chunk - stay) * TILE, TILE), :]
                    ready[s, r, here, :] = (new - offset) * scaling
        for p in range(n_lon - 1):
            sum_copy(piece, p).wait_send()
    for s, side in enumerate(sides):
        when(side[3], lambda: y_copy(s, s).wait_recv())
        add(chunks - 1, s, landing, (chunks - 1) * TILE)
    send_sums(len(groups) - 1)
    for s, side in enumerate(sides):
        when(side[3], lambda: y_copy(s, side[4]).wait_send())

    settle(len(groups) - 1)
    mean_out[...], scale_out[...] = values[chunks - 1]
    for p in range(n_lon - 1):
        sum_copy(len(groups) - 1, p).wait_send()


def write_early(sizes, end, mean, scale, standardized, end_out, held, sem):
    J, I, K, M = end.shape
    lat = lax.axis_index("lat")
    first, number = early_planes(sizes[0], lat, J)
    done = pl.ds(0, kept(K) * TILE)
    copies = [pltpu.make_async_copy(
        end.at[pl.ds(first, number)], end_out.at[pl.ds(first, number)], sem.at[number])]
    for s, side in enumerate(lat_sides(sizes[0], lat, J)):
        copies.append(pltpu.make_async_copy(
            end.at[side[0], :, done, :], end_out.at[side[0], :, done, :], sem.at[number + 1 + s]))
    for copy in copies:
        copy.start()
    for p in range(number):
        j = first + p
        offset, factor = mean[j], scale[j]

        @pl.loop(0, I // ROWS)
        def _(b):
            rows = pl.ds(b * ROWS, ROWS)
            held[p, rows] = (end[j, rows] - offset) * factor

        copies.append(pltpu.make_async_copy(held.at[p], standardized.at[j], sem.at[p]))
        copies[-1].start()
    for copy in copies:
        copy.wait()


def write_late(
    sizes, ready, tail, mean, scale, old_standardized, old_end, standardized, end_out, held, sem,
):
    J, K = end_out.shape[0], end_out.shape[2]
    late, I, high, M = tail.shape
    copies = []
    for s, side in enumerate(lat_sides(sizes[0], lax.axis_index("lat"), J)):
        j = side[0]

        def copy(source, target, rows, n):
            copies.append(pltpu.make_async_copy(source, target.at[j, :, rows, :], sem.at[s, n]))
            copies[-1].start()

        copy(ready.at[s], standardized, pl.ds(0, K - TILE), 0)
        copy(tail.at[s], end_out, pl.ds(K - high, high), 1)
        offset, scaling = mean[s], scale[s]

        @pl.loop(0, I // ROWS)
        def _(b):
            rows = pl.ds(b * ROWS, ROWS)
            held[s, rows] = (tail[s, rows, pl.ds(high - TILE, TILE), :] - offset) * scaling

        copy(held.at[s], standardized, pl.ds(K - TILE, TILE), 2)
    for copy in copies:
        copy.wait()


def cross(sizes, block):
    n_lat = sizes[0]
    if n_lat == 2:
        return lax.ppermute(block, "lat", [(0, 1), (1, 0)])
    up = lax.ppermute(block[1:], "lat", [(a, a + 1) for a in range(n_lat - 1)])
    down = lax.ppermute(block[:1], "lat", [(a + 1, a) for a in range(n_lat - 1)])
    return jnp.concatenate([up, down])


def shards(sizes, tracer, conductance, source):
    n_lat, n_lon, n_lev = sizes
    J, I, K, M = tracer.shape
    chunks = K // TILE
    f32 = jnp.float32
    dma = pltpu.SemaphoreType.DMA
    peers = max(n_lon - 1, 1)
    late = len(lat_sides(n_lat, 0, J))
    early = early_planes(n_lat, 0, J)[1]
    stay = kept(K)
    hbm, vmem = pl.BlockSpec(memory_space=pltpu.HBM), pl.BlockSpec(memory_space=pltpu.VMEM)
    cuts = spans(K)
    scratch = [
        (J, I + 2, K, M), (J, I + 2, K, M), (J, I, K, M), (J, I, K, M), (2, late, I, K, M),
        (2, J, I, 1, M), (2, J, I, 1, M), (2, J, I, 1, M), (2, J, I, 1, M),
        (early, 2, K, M), (peers, early, 2, K, M),
    ]
    limit = sum(4 * math.prod(shape) for shape in scratch) + (2 << 20)
    end, mean, scale, base, factor, sums, *outs = pl.pallas_call(
        functools.partial(kernel, sizes),
        out_shape=[
            pltpu.VMEM((J, I, K, M), f32),
            pltpu.VMEM((J, K, M), f32),
            pltpu.VMEM((J, K, M), f32),
            pltpu.VMEM((late, I, K, M), f32),
            pltpu.VMEM((late, I, K - stay * TILE, M), f32),
            pltpu.VMEM((stay, late, 2, TILE, M), f32),
        ] + [pltpu.VMEM((late, I, high - low, M), f32) for low, high in cuts],
        in_specs=[hbm] * 3,
        out_specs=[vmem] * (6 + len(cuts)),
        scratch_shapes=[pltpu.VMEM(shape, f32) for shape in scratch] + [
            pltpu.SemaphoreType.REGULAR,
            pltpu.SemaphoreType.REGULAR,
            dma((3,)),
            dma((chunks, late)),
            dma((STEPS, chunks, late)),
            dma((STEPS, chunks, late)),
            dma((STEPS, 2, 1 + late)),
            dma((STEPS, 2, 1 + late)),
            dma((STEPS, 2, 1 + late)),
            dma((STEPS, 2, 1 + late)),
            dma((peers,)),
            dma((peers,)),
        ],
        compiler_params=pltpu.CompilerParams(
            collective_id=0, has_side_effects=True, vmem_limit_bytes=limit),
    )(tracer, conductance, source)
    halos = [cross(sizes, out) for out in outs[:-1]]
    whole = jax.ShapeDtypeStruct((J, I, K, M), f32)

    standardized, end_out = pl.pallas_call(
        functools.partial(write_early, sizes),
        out_shape=[whole] * 2,
        in_specs=[vmem] * 3,
        out_specs=[hbm] * 2,
        scratch_shapes=[pltpu.VMEM((early, I, K, M), f32), dma((early + 1 + late,))],
        compiler_params=pltpu.CompilerParams(vmem_limit_bytes=16 << 20),
        cost_estimate=pl.CostEstimate(
            flops=1 << 32, bytes_accessed=8 * early * I * K * M, transcendentals=0),
    )(end, mean, scale)
    out_of = (late, I, K - stay * TILE, M)
    tail, ready, mean, scale = pl.pallas_call(
        functools.partial(finish, sizes),
        out_shape=[pltpu.VMEM(out_of, f32), pltpu.VMEM((late, I, K - TILE, M), f32)]
        + [pltpu.VMEM((late, TILE, M), f32)] * 2,
        in_specs=[vmem] * (5 + len(halos)),
        out_specs=[vmem] * 4,
        scratch_shapes=[
            pltpu.VMEM((late, I, TILE, M), f32),
            pltpu.VMEM((chunks, late, 2, TILE, M), f32),
            pltpu.VMEM((peers, chunks, late, 2, TILE, M), f32),
            pltpu.SemaphoreType.REGULAR,
            dma((late,)),
            dma((late,)),
            dma((3, peers)),
            dma((3, peers)),
        ],
        compiler_params=pltpu.CompilerParams(
            collective_id=1, has_side_effects=True, vmem_limit_bytes=8 << 20),
    )(base, factor, sums, end, outs[-1], *halos)
    return pl.pallas_call(
        functools.partial(write_late, sizes),
        out_shape=[whole] * 2,
        in_specs=[vmem] * 4 + [hbm] * 2,
        out_specs=[hbm] * 2,
        input_output_aliases={4: 0, 5: 1},
        scratch_shapes=[pltpu.VMEM((late, I, TILE, M), f32), dma((late, 3))],
        compiler_params=pltpu.CompilerParams(vmem_limit_bytes=12 << 20),
    )(ready, tail, mean, scale, standardized, end_out)


def solution(mesh):
    placed = P("lat", "lon", "lev", None)
    sizes = tuple(mesh.shape[axis] for axis in ("lat", "lon", "lev"))
    return jax.shard_map(
        functools.partial(shards, sizes),
        mesh=mesh,
        in_specs=(placed, placed, placed),
        out_specs=(placed, placed),
        check_vma=False,
    )
```

```python
import functools
import math

import jax
import jax.numpy as jnp
from jax import lax
from jax.experimental import pallas as pl
from jax.experimental.pallas import tpu as pltpu
from jax.sharding import PartitionSpec as P

STEPS = 3
GUESS = 1.0
TILE = 8
ROWS = 8
TURN = 32
MESH = pl.DeviceIdType.MESH


def lat_sides(n_lat, lat, J):
    if n_lat == 2:
        return [(jnp.where(lat == 0, J - 1, 0), jnp.where(lat == 0, J - 2, 1), 1 - lat, None, 0)]
    return [(0, 1, lat - 1, lat > 0, 1), (J - 1, J - 2, lat + 1, lat < n_lat - 1, 0)]


def early_planes(n_lat, lat, J):
    if n_lat == 2:
        return jnp.where(lat == 0, 0, 1), J - 1
    return 1, J - 2


def kept(K):
    return K // TILE // 2


def spans(K):
    start, last = kept(K) * TILE, K - TILE
    return [(low, high) for low, high in ((start, last), (last, K)) if high > low]


def close(total, count):
    offset = total[0] / count
    variance = total[1] / count - offset * offset
    return GUESS + offset, lax.rsqrt(variance + 0.0001)


def tally(new, totals):
    moved = new - GUESS
    return totals[0] + jnp.sum(moved, axis=0), totals[1] + jnp.sum(moved * moved, axis=0)


def when(condition, act):
    if condition is None:
        act()
    else:
        pl.when(condition)(act)


def kernel(sizes, tracer, conductance, source, end, mean_out, scale_out, base, factor, sums_late, *rest):
    cuts = spans(tracer.shape[2])
    outs = rest[:len(cuts)]
    (
        even, odd, cond, sour, y_halo, z_lower, z_upper, z_first, z_last, sums_early, peer_early,
        peer_in, all_in,
        load_sem, first_sem, y_send, y_recv, x_send, x_recv, z_send, z_recv, early_send, early_recv,
    ) = rest[len(cuts):]
    n_lat, n_lon, n_lev = sizes
    J, I, K, M = tracer.shape
    chunks = K // TILE
    blocks = I // ROWS
    count = I * n_lon
    lat, lon, lev = lax.axis_index("lat"), lax.axis_index("lon"), lax.axis_index("lev")
    below = {"lon": lon > 0, "lev": lev > 0}
    above = {"lon": lon < n_lon - 1, "lev": lev < n_lev - 1}
    index = {"lon": lon, "lev": lev}
    field = [even, odd]
    sides = lat_sides(n_lat, lat, J)
    first, number = early_planes(n_lat, lat, J)
    stay = kept(K)
    odd_lon = lon % 2 == 1
    rows_in = pl.ds(1, I)

    def levels(chunk):
        return pl.ds(chunk * TILE, TILE)

    def target(axis, way):
        return {axis: index[axis] + (1 if way == 0 else -1)}

    def y_copy(step, chunk, s):
        plane, _, peer, _, slot = sides[s]
        return pltpu.make_async_remote_copy(
            src_ref=field[step % 2].at[plane, rows_in, levels(chunk), :],
            dst_ref=y_halo.at[step % 2, slot, :, levels(chunk), :],
            send_sem=y_send.at[step % 2, chunk, s], recv_sem=y_recv.at[step % 2, chunk, slot],
            device_id={"lat": peer}, device_id_type=MESH)

    def y_arrival(step, chunk, s):
        plane, _, peer, _, _ = sides[s]
        return pltpu.make_async_remote_copy(
            src_ref=field[step % 2].at[plane, rows_in, levels(chunk), :],
            dst_ref=y_halo.at[step % 2, s, :, levels(chunk), :],
            send_sem=y_send.at[step % 2, chunk, s], recv_sem=y_recv.at[step % 2, chunk, s],
            device_id={"lat": peer}, device_id_type=MESH)

    faces = [pl.ds(first, number)] + [pl.ds(side[0], 1) for side in sides]

    def x_copy(step, way, part):
        buf = field[step % 2]
        return pltpu.make_async_remote_copy(
            src_ref=buf.at[faces[part], I if way == 0 else 1],
            dst_ref=buf.at[faces[part], 0 if way == 0 else I + 1],
            send_sem=x_send.at[step % 2, way, part], recv_sem=x_recv.at[step % 2, way, part],
            device_id=target("lon", way), device_id_type=MESH)

    def z_copy(step, way, part):
        src = z_last if way == 0 else z_first
        dst = z_lower if way == 0 else z_upper
        return pltpu.make_async_remote_copy(
            src_ref=src.at[step % 2, faces[part]], dst_ref=dst.at[step % 2, faces[part]],
            send_sem=z_send.at[step % 2, way, part], recv_sem=z_recv.at[step % 2, way, part],
            device_id=target("lev", way), device_id_type=MESH)

    def early_copy(shift):
        return pltpu.make_async_remote_copy(
            src_ref=sums_early, dst_ref=peer_early.at[shift - 1],
            send_sem=early_send.at[shift - 1], recv_sem=early_recv.at[shift - 1],
            device_id={"lon": lax.rem(lon + shift, n_lon)}, device_id_type=MESH)

    def sends(axis, way, act):
        pl.when((above if way == 0 else below)[axis])(act)

    def arrives(axis, way, act):
        pl.when((below if way == 0 else above)[axis])(act)

    first_loads = [[
        pltpu.make_async_copy(
            tracer.at[side[0], :, levels(chunk), :], even.at[side[0], rows_in, levels(chunk), :],
            first_sem.at[chunk, s])
        for s, side in enumerate(sides)] for chunk in range(chunks)]
    loads = [
        pltpu.make_async_copy(
            tracer.at[pl.ds(first, number)], even.at[pl.ds(first, number), rows_in], load_sem.at[0]),
        pltpu.make_async_copy(conductance, cond, load_sem.at[1]),
        pltpu.make_async_copy(source, sour, load_sem.at[2]),
    ]
    for chunk in range(chunks):
        for load in first_loads[chunk]:
            load.start()
    even_lat = lat % 2 == 0
    around = n_lon - 1 + below["lev"].astype(jnp.int32) + above["lev"].astype(jnp.int32)
    met = jnp.where(even_lat, around, 0)
    barrier = pltpu.get_barrier_semaphore()

    def signal_around(semaphore):
        for shift in range(1, n_lon):
            pl.semaphore_signal(semaphore, inc=1, device_id={"lon": lax.rem(lon + shift, n_lon)},
                                device_id_type=MESH)
        for way in (0, 1):
            sends("lev", way, lambda: pl.semaphore_signal(
                semaphore, inc=1, device_id=target("lev", way), device_id_type=MESH))

    for _, _, peer, exists, _ in sides:
        when(exists, lambda: pl.semaphore_signal(
            barrier, inc=1, device_id={"lat": peer}, device_id_type=MESH))
        met = met + (1 if exists is None else exists.astype(jnp.int32))
    pl.when(even_lat)(lambda: signal_around(barrier))
    loads[0].start()
    pl.semaphore_wait(barrier, met)

    for chunk in range(chunks):
        for s, side in enumerate(sides):
            first_loads[chunk][s].wait()
            when(side[3], lambda: y_copy(0, chunk, s).start())
    loads[1].start()
    loads[2].start()

    @pl.when(even_lat)
    def _():
        signal_around(peer_in)

    for s, side in enumerate(sides):
        if side[3] is not None:
            def no_y():
                @pl.loop(0, blocks)
                def _(b):
                    for p in range(2):
                        y_halo[p, s, pl.ds(b * ROWS, ROWS)] = jnp.zeros((ROWS, K, M), jnp.float32)
            pl.when(jnp.logical_not(side[3]))(no_y)
    for way in (0, 1):
        def no_x():
            for buf in field:
                for j in range(J):
                    buf[j, 0 if way == 0 else I + 1] = jnp.zeros((K, M), jnp.float32)
        pl.when(jnp.logical_not((below if way == 0 else above)["lon"]))(no_x)

        def no_z():
            @pl.loop(0, blocks)
            def _(b):
                for p in range(2):
                    for j in range(J):
                        (z_lower if way == 0 else z_upper)[p, j, pl.ds(b * ROWS, ROWS)] = (
                            jnp.zeros((ROWS, 1, M), jnp.float32))
        pl.when(jnp.logical_not((below if way == 0 else above)["lev"]))(no_z)

    def pack_and_send(step, part):
        buf = field[step % 2]
        start, extent = (first, number) if part == 0 else (sides[part - 1][0], 1)
        for way in (0, 1):
            sends("lon", way, lambda: x_copy(step, way, part).start())

        @pl.loop(0, extent * blocks)
        def _(q):
            j, r = start + q // blocks, (q % blocks) * ROWS
            z_first[step % 2, j, pl.ds(r, ROWS)] = buf[j, pl.ds(1 + r, ROWS), pl.ds(0, 1), :]
            z_last[step % 2, j, pl.ds(r, ROWS)] = buf[j, pl.ds(1 + r, ROWS), pl.ds(K - 1, 1), :]

        for way in (0, 1):
            sends("lev", way, lambda: z_copy(step, way, part).start())

    def faces_sent(step):
        for part in range(len(faces)):
            for way in (0, 1):
                sends("lon", way, lambda: x_copy(step, way, part).wait_send())
                sends("lev", way, lambda: z_copy(step, way, part).wait_send())

    def faces_arrive(step, part):
        for way in (0, 1):
            arrives("lon", way, lambda: x_copy(step, way, part).wait_recv())
            arrives("lev", way, lambda: z_copy(step, way, part).wait_recv())

    def next_rows(step, chunk, j, r, inward):
        buf = field[step % 2]
        here = levels(chunk)
        rows = pl.ds(1 + r, ROWS)
        mid = buf[j, rows, here, :]
        k = lax.broadcasted_iota(jnp.int32, mid.shape, 1)
        if chunk == 0:
            edge = jnp.broadcast_to(z_lower[step % 2, j, pl.ds(r, ROWS)], mid.shape)
        else:
            edge = pltpu.roll(buf[j, rows, levels(chunk - 1), :], 1, 1)
        k_lower = jnp.where(k == 0, edge, pltpu.roll(mid, 1, 1))
        if chunk == chunks - 1:
            edge = jnp.broadcast_to(z_upper[step % 2, j, pl.ds(r, ROWS)], mid.shape)
        else:
            edge = pltpu.roll(buf[j, rows, levels(chunk + 1), :], TILE - 1, 1)
        k_upper = jnp.where(k == TILE - 1, edge, pltpu.roll(mid, TILE - 1, 1))
        if inward is None:
            across = buf[j - 1, rows, here, :] + buf[j + 1, rows, here, :]
        else:
            across = buf[inward, rows, here, :]
        spread = (
            across + buf[j, pl.ds(r, ROWS), here, :] + buf[j, pl.ds(2 + r, ROWS), here, :]
            + k_lower + k_upper - 6.0 * mid)
        return mid + cond[j, pl.ds(r, ROWS), here, :] * spread + sour[j, pl.ds(r, ROWS), here, :]

    zero = jnp.zeros((TILE, M), jnp.float32)

    def early_plane(step, chunk, j, inward):
        def body(b, totals):
            r = b * ROWS
            new = next_rows(step, chunk, j, r, inward)
            if step < STEPS - 1:
                field[(step + 1) % 2][j, pl.ds(1 + r, ROWS), levels(chunk), :] = new
                return totals
            end[j, pl.ds(r, ROWS), levels(chunk), :] = new
            return tally(new, totals)

        if step < STEPS - 1:
            lax.fori_loop(0, blocks, lambda b, _: body(b, 0), 0)
        else:
            totals = lax.fori_loop(0, blocks, body, (zero, zero))
            for q in range(2):
                sums_early[j - first, q, levels(chunk), :] = totals[q]

    def early_part(step, chunk):
        @pl.loop(1, J - 1)
        def _(j):
            early_plane(step, chunk, j, None)

        if step == STEPS - 1 and chunk == max(chunks - 2, 0):
            for held in range(stay):
                for s in range(len(sides)):
                    y_start(step, held, s, odd_lon)
        if n_lat == 2:
            early_plane(step, chunk, jnp.where(lat == 0, 0, J - 1), jnp.where(lat == 0, 1, J - 2))

    def base_part(step, chunk):
        for s, (plane, inward, _, _, _) in enumerate(sides):
            @pl.loop(0, blocks)
            def _(b):
                r = b * ROWS
                base[s, pl.ds(r, ROWS), levels(chunk), :] = next_rows(step, chunk, plane, r, inward)

    def late_part(step, chunk, s):
        plane = sides[s][0]
        here, turn = levels(chunk), math.gcd(I, TURN)

        def body(b, totals):
            r = pl.ds(b * turn, turn)
            new = base[s, r, here, :] + cond[plane, r, here, :] * y_halo[step % 2, s, r, here, :]
            if step < STEPS - 1:
                field[(step + 1) % 2][plane, pl.ds(1 + b * turn, turn), here, :] = new
                if step == STEPS - 2:
                    for out, (low, high) in zip(outs, cuts):
                        if low <= chunk * TILE < high:
                            out[s, r, pl.ds(chunk * TILE - low, TILE), :] = new
                return totals
            end[plane, r, here, :] = new
            return tally(new, totals)

        if step < STEPS - 1:
            lax.fori_loop(0, I // turn, lambda b, _: body(b, 0), 0)
        else:
            totals = lax.fori_loop(0, I // turn, body, (zero, zero))
            for q in range(2):
                sums_late[chunk, s, q] = totals[q]

    def y_start(step, chunk, s, condition=None):
        exists = sides[s][3]
        if condition is not None and exists is not None:
            condition = jnp.logical_and(condition, exists)
        when(exists if condition is None else condition, lambda: y_copy(step, chunk, s).start())

    @pl.when(even_lat)
    def _():
        pl.semaphore_wait(peer_in, around)
        pl.when(lat < n_lat - 1)(lambda: pl.semaphore_signal(
            all_in, inc=1, device_id={"lat": lat + 1}, device_id_type=MESH))

    @pl.when(jnp.logical_not(even_lat))
    def _():
        pl.semaphore_wait(all_in, 1)

    loads[0].wait()
    for part in range(len(faces)):
        pack_and_send(0, part)
    loads[1].wait()
    loads[2].wait()
    for step in range(STEPS):
        last = step == STEPS - 1
        if step >= 1:
            faces_sent(step - 1)
        faces_arrive(step, 0)
        for chunk in range(chunks):
            early_part(step, chunk)
        if last:
            for shift in range(1, n_lon):
                early_copy(shift).start()
        else:
            pack_and_send(step + 1, 0)
        for part in range(1, len(faces)):
            faces_arrive(step, part)
        for chunk in range(chunks):
            base_part(step, chunk)
        if step >= 1:
            for s, side in enumerate(sides):
                for chunk in range(chunks):
                    when(side[3], lambda: y_copy(step - 1, chunk, s).wait_send())
        if last:
            for s, side in enumerate(sides):
                @pl.loop(0, blocks)
                def _(b):
                    rows = pl.ds(b * ROWS, ROWS)
                    factor[s, rows] = cond[side[0], rows, pl.ds(stay * TILE, K - stay * TILE), :]
            faces_sent(step)
            for shift in range(1, n_lon):
                early_copy(shift).wait_recv()

            @pl.loop(0, number)
            def _(p):
                total = [sums_early[p, q] for q in range(2)]
                for shift in range(1, n_lon):
                    total = [total[q] + peer_early[shift - 1, p, q] for q in range(2)]
                mean_out[first + p], scale_out[first + p] = close(total, count)

            for shift in range(1, n_lon):
                early_copy(shift).wait_send()
        for chunk in range(stay if last else chunks):
            for s, side in enumerate(sides):
                when(side[3], lambda: y_arrival(step, chunk, s).wait_recv())
                late_part(step, chunk, s)
                if step < STEPS - 2:
                    y_start(step + 1, chunk, s)
                elif not last and chunk < stay:
                    y_start(step + 1, chunk, s, jnp.logical_not(odd_lon))
        if not last:
            for part in range(1, len(faces)):
                pack_and_send(step + 1, part)
    for s, side in enumerate(sides):
        for chunk in range(stay):
            when(side[3], lambda: y_copy(STEPS - 1, chunk, s).wait_send())


def finish(sizes, base, factor, sums_in, end, out, *rest):
    halos, (
        tail, ready, mean_out, scale_out, landing, sums, peer_sums, late_in, y_send, y_recv, send_sem, recv_sem,
    ) = rest[:-12], rest[-12:]
    n_lat, n_lon, _ = sizes
    late, I, K, M = base.shape
    chunks, stay, cuts = K // TILE, kept(K), spans(K)
    lat, lon = lax.axis_index("lat"), lax.axis_index("lon")
    even_lon = lon % 2 == 0
    n_odd = n_lon // 2
    sides = lat_sides(n_lat, lat, end.shape[0])
    peers = [lax.rem(lon + shift, n_lon) for shift in range(1, n_lon)]
    groups = [group for group in (list(range(stay)), list(range(stay, chunks - 1)), [chunks - 1]) if group]
    pieces = [pl.ds(group[0], len(group)) for group in groups]

    def y_copy(s, slot):
        return pltpu.make_async_remote_copy(
            src_ref=out.at[s], dst_ref=landing.at[slot], send_sem=y_send.at[s], recv_sem=y_recv.at[slot],
            device_id={"lat": sides[s][2]}, device_id_type=MESH)

    def sum_copy(piece, p):
        return pltpu.make_async_remote_copy(
            src_ref=sums.at[pieces[piece]], dst_ref=peer_sums.at[p, pieces[piece]],
            send_sem=send_sem.at[piece, p], recv_sem=recv_sem.at[piece, p],
            device_id={"lon": peers[p]}, device_id_type=MESH)

    def send_sums(piece):
        for p in range(n_lon - 1):
            sum_copy(piece, p).start()

    def add(chunk, s, arrived, start):
        here = pl.ds(chunk * TILE, TILE)
        there, came = pl.ds((chunk - stay) * TILE, TILE), pl.ds(chunk * TILE - start, TILE)
        zero, turn = jnp.zeros((TILE, M), jnp.float32), math.gcd(I, TURN)

        def body(b, totals):
            r = pl.ds(b * turn, turn)
            new = base[s, r, here, :] + factor[s, r, there, :] * arrived[s, r, came, :]
            tail[s, r, there, :] = new
            return tally(new, totals)

        totals = lax.fori_loop(0, I // turn, body, (zero, zero))
        for q in range(2):
            sums[chunk, s, q] = totals[q]

    barrier = pltpu.get_barrier_semaphore()
    met = jnp.where(even_lon, n_lon - n_odd - 1, n_lon - 1)
    for _, _, peer, exists, _ in sides:
        when(exists, lambda: pl.semaphore_signal(
            barrier, inc=1, device_id={"lat": peer}, device_id_type=MESH))
        met = met + (1 if exists is None else exists.astype(jnp.int32))
    for peer in peers:
        pl.when(jnp.logical_or(even_lon, peer % 2 == 1))(lambda: pl.semaphore_signal(
            barrier, inc=1, device_id={"lon": peer}, device_id_type=MESH))
    pl.semaphore_wait(barrier, met)
    for s, side in enumerate(sides):
        when(side[3], lambda: y_copy(s, side[4]).start())

    @pl.when(jnp.logical_not(even_lon))
    def _():
        for peer in peers:
            pl.when(peer % 2 == 0)(lambda: pl.semaphore_signal(
                late_in, inc=1, device_id={"lon": peer}, device_id_type=MESH))

    for s, side in enumerate(sides):
        if side[3] is not None:
            @pl.when(jnp.logical_not(side[3]))
            def _():
                @pl.loop(0, I // ROWS)
                def _(b):
                    landing[s, pl.ds(b * ROWS, ROWS)] = jnp.zeros((ROWS,) + landing.shape[2:], jnp.float32)
        for chunk in range(chunks - 1):
            if chunk < stay:
                for q in range(2):
                    sums[chunk, s, q] = sums_in[chunk, s, q]
            else:
                add(chunk, s, halos[0], cuts[0][0])
    pl.when(even_lon)(lambda: pl.semaphore_wait(late_in, n_odd))
    values = {}

    def settle(piece):
        for p in range(n_lon - 1):
            sum_copy(piece, p).wait_recv()
        for chunk in groups[piece]:
            of_sides = []
            for s in range(late):
                total = [sums[chunk, s, q] for q in range(2)]
                for p in range(n_lon - 1):
                    total = [total[q] + peer_sums[p, chunk, s, q] for q in range(2)]
                of_sides.append(close(total, I * n_lon))
            values[chunk] = [jnp.stack(part) for part in zip(*of_sides)]

    for piece in range(len(groups) - 1):
        send_sums(piece)
    for piece, group in enumerate(groups[:-1]):
        settle(piece)
        for chunk in group:
            here = pl.ds(chunk * TILE, TILE)
            for s, side in enumerate(sides):
                offset, scaling = values[chunk][0][s], values[chunk][1][s]

                @pl.loop(0, I // ROWS)
                def _(b):
                    r = pl.ds(b * ROWS, ROWS)
                    if chunk < stay:
                        new = end[side[0], r, here, :]
                    else:
                        new = tail[s, r, pl.ds((chunk - stay) * TILE, TILE), :]
                    ready[s, r, here, :] = (new - offset) * scaling
        for p in range(n_lon - 1):
            sum_copy(piece, p).wait_send()
    for s, side in enumerate(sides):
        when(side[3], lambda: y_copy(s, s).wait_recv())
        add(chunks - 1, s, landing, (chunks - 1) * TILE)
    send_sums(len(groups) - 1)
    for s, side in enumerate(sides):
        when(side[3], lambda: y_copy(s, side[4]).wait_send())

    settle(len(groups) - 1)
    mean_out[...], scale_out[...] = values[chunks - 1]
    for p in range(n_lon - 1):
        sum_copy(len(groups) - 1, p).wait_send()


def write_early(sizes, end, mean, scale, standardized, end_out, held, sem):
    J, I, K, M = end.shape
    lat = lax.axis_index("lat")
    first, number = early_planes(sizes[0], lat, J)
    done = pl.ds(0, kept(K) * TILE)
    copies = [pltpu.make_async_copy(
        end.at[pl.ds(first, number)], end_out.at[pl.ds(first, number)], sem.at[number])]
    for s, side in enumerate(lat_sides(sizes[0], lat, J)):
        copies.append(pltpu.make_async_copy(
            end.at[side[0], :, done, :], end_out.at[side[0], :, done, :], sem.at[number + 1 + s]))
    for copy in copies:
        copy.start()
    for p in range(number):
        j = first + p
        offset, factor = mean[j], scale[j]

        @pl.loop(0, I // ROWS)
        def _(b):
            rows = pl.ds(b * ROWS, ROWS)
            held[p, rows] = (end[j, rows] - offset) * factor

        copies.append(pltpu.make_async_copy(held.at[p], standardized.at[j], sem.at[p]))
        copies[-1].start()
    for copy in copies:
        copy.wait()


def write_late(
    sizes, ready, tail, mean, scale, old_standardized, old_end, standardized, end_out, held, sem,
):
    J, K = end_out.shape[0], end_out.shape[2]
    late, I, high, M = tail.shape
    copies = []
    for s, side in enumerate(lat_sides(sizes[0], lax.axis_index("lat"), J)):
        j = side[0]

        def copy(source, target, rows, n):
            copies.append(pltpu.make_async_copy(source, target.at[j, :, rows, :], sem.at[s, n]))
            copies[-1].start()

        copy(ready.at[s], standardized, pl.ds(0, K - TILE), 0)
        copy(tail.at[s], end_out, pl.ds(K - high, high), 1)
        offset, scaling = mean[s], scale[s]

        @pl.loop(0, I // ROWS)
        def _(b):
            rows = pl.ds(b * ROWS, ROWS)
            held[s, rows] = (tail[s, rows, pl.ds(high - TILE, TILE), :] - offset) * scaling

        copy(held.at[s], standardized, pl.ds(K - TILE, TILE), 2)
    for copy in copies:
        copy.wait()


def cross(sizes, block):
    n_lat = sizes[0]
    if n_lat == 2:
        return lax.ppermute(block, "lat", [(0, 1), (1, 0)])
    up = lax.ppermute(block[1:], "lat", [(a, a + 1) for a in range(n_lat - 1)])
    down = lax.ppermute(block[:1], "lat", [(a + 1, a) for a in range(n_lat - 1)])
    return jnp.concatenate([up, down])


def shards(sizes, tracer, conductance, source):
    n_lat, n_lon, n_lev = sizes
    J, I, K, M = tracer.shape
    chunks = K // TILE
    f32 = jnp.float32
    dma = pltpu.SemaphoreType.DMA
    peers = max(n_lon - 1, 1)
    late = len(lat_sides(n_lat, 0, J))
    early = early_planes(n_lat, 0, J)[1]
    stay = kept(K)
    hbm, vmem = pl.BlockSpec(memory_space=pltpu.HBM), pl.BlockSpec(memory_space=pltpu.VMEM)
    cuts = spans(K)
    scratch = [
        (J, I + 2, K, M), (J, I + 2, K, M), (J, I, K, M), (J, I, K, M), (2, late, I, K, M),
        (2, J, I, 1, M), (2, J, I, 1, M), (2, J, I, 1, M), (2, J, I, 1, M),
        (early, 2, K, M), (peers, early, 2, K, M),
    ]
    limit = sum(4 * math.prod(shape) for shape in scratch) + (2 << 20)
    end, mean, scale, base, factor, sums, *outs = pl.pallas_call(
        functools.partial(kernel, sizes),
        out_shape=[
            pltpu.VMEM((J, I, K, M), f32),
            pltpu.VMEM((J, K, M), f32),
            pltpu.VMEM((J, K, M), f32),
            pltpu.VMEM((late, I, K, M), f32),
            pltpu.VMEM((late, I, K - stay * TILE, M), f32),
            pltpu.VMEM((stay, late, 2, TILE, M), f32),
        ] + [pltpu.VMEM((late, I, high - low, M), f32) for low, high in cuts],
        in_specs=[hbm] * 3,
        out_specs=[vmem] * (6 + len(cuts)),
        scratch_shapes=[pltpu.VMEM(shape, f32) for shape in scratch] + [
            pltpu.SemaphoreType.REGULAR,
            pltpu.SemaphoreType.REGULAR,
            dma((3,)),
            dma((chunks, late)),
            dma((2, chunks, late)),
            dma((2, chunks, late)),
            dma((2, 2, 1 + late)),
            dma((2, 2, 1 + late)),
            dma((2, 2, 1 + late)),
            dma((2, 2, 1 + late)),
            dma((peers,)),
            dma((peers,)),
        ],
        compiler_params=pltpu.CompilerParams(
            collective_id=0, has_side_effects=True, vmem_limit_bytes=limit),
    )(tracer, conductance, source)
    halos = [cross(sizes, out) for out in outs[:-1]]
    whole = jax.ShapeDtypeStruct((J, I, K, M), f32)

    standardized, end_out = pl.pallas_call(
        functools.partial(write_early, sizes),
        out_shape=[whole] * 2,
        in_specs=[vmem] * 3,
        out_specs=[hbm] * 2,
        scratch_shapes=[pltpu.VMEM((early, I, K, M), f32), dma((early + 1 + late,))],
        compiler_params=pltpu.CompilerParams(vmem_limit_bytes=16 << 20),
        cost_estimate=pl.CostEstimate(
            flops=1 << 32, bytes_accessed=8 * early * I * K * M, transcendentals=0),
    )(end, mean, scale)
    out_of = (late, I, K - stay * TILE, M)
    tail, ready, mean, scale = pl.pallas_call(
        functools.partial(finish, sizes),
        out_shape=[pltpu.VMEM(out_of, f32), pltpu.VMEM((late, I, K - TILE, M), f32)]
        + [pltpu.VMEM((late, TILE, M), f32)] * 2,
        in_specs=[vmem] * (5 + len(halos)),
        out_specs=[vmem] * 4,
        scratch_shapes=[
            pltpu.VMEM((late, I, TILE, M), f32),
            pltpu.VMEM((chunks, late, 2, TILE, M), f32),
            pltpu.VMEM((peers, chunks, late, 2, TILE, M), f32),
            pltpu.SemaphoreType.REGULAR,
            dma((late,)),
            dma((late,)),
            dma((3, peers)),
            dma((3, peers)),
        ],
        compiler_params=pltpu.CompilerParams(
            collective_id=1, has_side_effects=True, vmem_limit_bytes=8 << 20),
    )(base, factor, sums, end, outs[-1], *halos)
    return pl.pallas_call(
        functools.partial(write_late, sizes),
        out_shape=[whole] * 2,
        in_specs=[vmem] * 4 + [hbm] * 2,
        out_specs=[hbm] * 2,
        input_output_aliases={4: 0, 5: 1},
        scratch_shapes=[pltpu.VMEM((late, I, TILE, M), f32), dma((late, 3))],
        compiler_params=pltpu.CompilerParams(vmem_limit_bytes=12 << 20),
    )(ready, tail, mean, scale, standardized, end_out)


def solution(mesh):
    placed = P("lat", "lon", "lev", None)
    sizes = tuple(mesh.shape[axis] for axis in ("lat", "lon", "lev"))
    return jax.shard_map(
        functools.partial(shards, sizes),
        mesh=mesh,
        in_specs=(placed, placed, placed),
        out_specs=(placed, placed),
        check_vma=False,
    )
```

```python
import functools
import math

import jax
import jax.numpy as jnp
from jax import lax
from jax.experimental import pallas as pl
from jax.experimental.pallas import tpu as pltpu
from jax.sharding import PartitionSpec as P

STEPS = 3
GUESS = 1.0
TILE = 8
ROWS = 8
TURN = 32
MESH = pl.DeviceIdType.MESH


def lat_sides(n_lat, lat, J):
    if n_lat == 2:
        return [(jnp.where(lat == 0, J - 1, 0), jnp.where(lat == 0, J - 2, 1), 1 - lat, None, 0)]
    return [(0, 1, lat - 1, lat > 0, 1), (J - 1, J - 2, lat + 1, lat < n_lat - 1, 0)]


def early_planes(n_lat, lat, J):
    if n_lat == 2:
        return jnp.where(lat == 0, 0, 1), J - 1
    return 1, J - 2


def kept(K):
    return K // TILE // 2


def spans(K):
    start, last = kept(K) * TILE, K - TILE
    return [(low, high) for low, high in ((start, last), (last, K)) if high > low]


def close(total, count):
    offset = total[0] / count
    variance = total[1] / count - offset * offset
    return GUESS + offset, lax.rsqrt(variance + 0.0001)


def tally(new, totals):
    moved = new - GUESS
    return totals[0] + jnp.sum(moved, axis=0), totals[1] + jnp.sum(moved * moved, axis=0)


def when(condition, act):
    if condition is None:
        act()
    else:
        pl.when(condition)(act)


def kernel(sizes, tracer, conductance, source, end, mean_out, scale_out, base, factor, sums_late, *rest):
    cuts = spans(tracer.shape[2])
    outs = rest[:len(cuts)]
    (
        even, odd, cond, sour, y_halo, z_lower, z_upper, z_first, z_last, sums_early, peer_early,
        peer_in, all_in,
        load_sem, first_sem, head_sem, head_send, head_recv, y_send, y_recv, x_send, x_recv, z_send, z_recv, early_send, early_recv,
    ) = rest[len(cuts):]
    n_lat, n_lon, n_lev = sizes
    J, I, K, M = tracer.shape
    chunks = K // TILE
    blocks = I // ROWS
    count = I * n_lon
    lat, lon, lev = lax.axis_index("lat"), lax.axis_index("lon"), lax.axis_index("lev")
    below = {"lon": lon > 0, "lev": lev > 0}
    above = {"lon": lon < n_lon - 1, "lev": lev < n_lev - 1}
    index = {"lon": lon, "lev": lev}
    field = [even, odd]
    sides = lat_sides(n_lat, lat, J)
    first, number = early_planes(n_lat, lat, J)
    stay = kept(K)
    odd_lon = lon % 2 == 1
    rows_in = pl.ds(1, I)

    def levels(chunk):
        return pl.ds(chunk * TILE, TILE)

    def target(axis, way):
        return {axis: index[axis] + (1 if way == 0 else -1)}

    def y_copy(step, chunk, s):
        plane, _, peer, _, slot = sides[s]
        skip = I // 4 if step == 0 and chunk == 0 else 0
        rows = pl.ds(skip, I - skip)
        return pltpu.make_async_remote_copy(
            src_ref=field[step % 2].at[plane, pl.ds(1 + skip, I - skip), levels(chunk), :],
            dst_ref=y_halo.at[step % 2, slot, rows, levels(chunk), :],
            send_sem=y_send.at[step % 2, chunk, s], recv_sem=y_recv.at[step % 2, chunk, slot],
            device_id={"lat": peer}, device_id_type=MESH)

    def y_arrival(step, chunk, s):
        plane, _, peer, _, _ = sides[s]
        skip = I // 4 if step == 0 and chunk == 0 else 0
        rows = pl.ds(skip, I - skip)
        return pltpu.make_async_remote_copy(
            src_ref=field[step % 2].at[plane, pl.ds(1 + skip, I - skip), levels(chunk), :],
            dst_ref=y_halo.at[step % 2, s, rows, levels(chunk), :],
            send_sem=y_send.at[step % 2, chunk, s], recv_sem=y_recv.at[step % 2, chunk, s],
            device_id={"lat": peer}, device_id_type=MESH)

    faces = [pl.ds(first, number)] + [pl.ds(side[0], 1) for side in sides]

    head = pl.ds(0, I // 4)

    def head_load(s):
        return pltpu.make_async_copy(
            tracer.at[sides[s][0], head, levels(0), :], even.at[sides[s][0], pl.ds(1, I // 4), levels(0), :],
            head_sem.at[s])

    def head_copy(s, slot):
        plane, _, peer, _, _ = sides[s]
        return pltpu.make_async_remote_copy(
            src_ref=even.at[plane, pl.ds(1, I // 4), levels(0), :], dst_ref=y_halo.at[0, slot, head, levels(0), :],
            send_sem=head_send.at[s], recv_sem=head_recv.at[slot],
            device_id={"lat": peer}, device_id_type=MESH)

    def x_copy(step, way, part):
        buf = field[step % 2]
        return pltpu.make_async_remote_copy(
            src_ref=buf.at[faces[part], I if way == 0 else 1],
            dst_ref=buf.at[faces[part], 0 if way == 0 else I + 1],
            send_sem=x_send.at[step % 2, way, part], recv_sem=x_recv.at[step % 2, way, part],
            device_id=target("lon", way), device_id_type=MESH)

    def z_copy(step, way, part):
        src = z_last if way == 0 else z_first
        dst = z_lower if way == 0 else z_upper
        return pltpu.make_async_remote_copy(
            src_ref=src.at[step % 2, faces[part]], dst_ref=dst.at[step % 2, faces[part]],
            send_sem=z_send.at[step % 2, way, part], recv_sem=z_recv.at[step % 2, way, part],
            device_id=target("lev", way), device_id_type=MESH)

    def early_copy(shift):
        return pltpu.make_async_remote_copy(
            src_ref=sums_early, dst_ref=peer_early.at[shift - 1],
            send_sem=early_send.at[shift - 1], recv_sem=early_recv.at[shift - 1],
            device_id={"lon": lax.rem(lon + shift, n_lon)}, device_id_type=MESH)

    def sends(axis, way, act):
        pl.when((above if way == 0 else below)[axis])(act)

    def arrives(axis, way, act):
        pl.when((below if way == 0 else above)[axis])(act)

    def first_load(chunk, s):
        skip = I // 4 if chunk == 0 else 0
        return pltpu.make_async_copy(
            tracer.at[sides[s][0], pl.ds(skip, I - skip), levels(chunk), :],
            even.at[sides[s][0], pl.ds(1 + skip, I - skip), levels(chunk), :], first_sem.at[chunk, s])

    first_loads = [[first_load(chunk, s) for s in range(len(sides))] for chunk in range(chunks)]
    for s in range(len(sides)):
        head_load(s).start()
    loads = [
        pltpu.make_async_copy(
            tracer.at[pl.ds(first, number)], even.at[pl.ds(first, number), rows_in], load_sem.at[0]),
        pltpu.make_async_copy(conductance, cond, load_sem.at[1]),
        pltpu.make_async_copy(source, sour, load_sem.at[2]),
    ]
    for chunk in range(chunks):
        for load in first_loads[chunk]:
            load.start()
    even_lat = lat % 2 == 0
    around = n_lon - 1 + below["lev"].astype(jnp.int32) + above["lev"].astype(jnp.int32)
    met = jnp.where(even_lat, around, 0)
    barrier = pltpu.get_barrier_semaphore()

    def signal_around(semaphore):
        for shift in range(1, n_lon):
            pl.semaphore_signal(semaphore, inc=1, device_id={"lon": lax.rem(lon + shift, n_lon)},
                                device_id_type=MESH)
        for way in (0, 1):
            sends("lev", way, lambda: pl.semaphore_signal(
                semaphore, inc=1, device_id=target("lev", way), device_id_type=MESH))

    for _, _, peer, exists, _ in sides:
        when(exists, lambda: pl.semaphore_signal(
            barrier, inc=1, device_id={"lat": peer}, device_id_type=MESH))
        met = met + (1 if exists is None else exists.astype(jnp.int32))
    pl.when(even_lat)(lambda: signal_around(barrier))
    loads[0].start()
    pl.semaphore_wait(barrier, met)

    for s, side in enumerate(sides):
        head_load(s).wait()
        when(side[3], lambda: head_copy(s, side[4]).start())
    for chunk in range(chunks):
        for s, side in enumerate(sides):
            first_loads[chunk][s].wait()
            when(side[3], lambda: y_copy(0, chunk, s).start())
    loads[1].start()
    loads[2].start()

    @pl.when(even_lat)
    def _():
        signal_around(peer_in)

    for s, side in enumerate(sides):
        if side[3] is not None:
            def no_y():
                @pl.loop(0, blocks)
                def _(b):
                    for p in range(2):
                        y_halo[p, s, pl.ds(b * ROWS, ROWS)] = jnp.zeros((ROWS, K, M), jnp.float32)
            pl.when(jnp.logical_not(side[3]))(no_y)
    for way in (0, 1):
        def no_x():
            for buf in field:
                for j in range(J):
                    buf[j, 0 if way == 0 else I + 1] = jnp.zeros((K, M), jnp.float32)
        pl.when(jnp.logical_not((below if way == 0 else above)["lon"]))(no_x)

        def no_z():
            @pl.loop(0, blocks)
            def _(b):
                for p in range(2):
                    for j in range(J):
                        (z_lower if way == 0 else z_upper)[p, j, pl.ds(b * ROWS, ROWS)] = (
                            jnp.zeros((ROWS, 1, M), jnp.float32))
        pl.when(jnp.logical_not((below if way == 0 else above)["lev"]))(no_z)

    def pack_and_send(step, part):
        buf = field[step % 2]
        start, extent = (first, number) if part == 0 else (sides[part - 1][0], 1)
        for way in (0, 1):
            sends("lon", way, lambda: x_copy(step, way, part).start())

        @pl.loop(0, extent * blocks)
        def _(q):
            j, r = start + q // blocks, (q % blocks) * ROWS
            z_first[step % 2, j, pl.ds(r, ROWS)] = buf[j, pl.ds(1 + r, ROWS), pl.ds(0, 1), :]
            z_last[step % 2, j, pl.ds(r, ROWS)] = buf[j, pl.ds(1 + r, ROWS), pl.ds(K - 1, 1), :]

        for way in (0, 1):
            sends("lev", way, lambda: z_copy(step, way, part).start())

    def faces_sent(step):
        for part in range(len(faces)):
            for way in (0, 1):
                sends("lon", way, lambda: x_copy(step, way, part).wait_send())
                sends("lev", way, lambda: z_copy(step, way, part).wait_send())

    def faces_arrive(step, part):
        for way in (0, 1):
            arrives("lon", way, lambda: x_copy(step, way, part).wait_recv())
            arrives("lev", way, lambda: z_copy(step, way, part).wait_recv())

    def next_rows(step, chunk, j, r, inward):
        buf = field[step % 2]
        here = levels(chunk)
        rows = pl.ds(1 + r, ROWS)
        mid = buf[j, rows, here, :]
        k = lax.broadcasted_iota(jnp.int32, mid.shape, 1)
        if chunk == 0:
            edge = jnp.broadcast_to(z_lower[step % 2, j, pl.ds(r, ROWS)], mid.shape)
        else:
            edge = pltpu.roll(buf[j, rows, levels(chunk - 1), :], 1, 1)
        k_lower = jnp.where(k == 0, edge, pltpu.roll(mid, 1, 1))
        if chunk == chunks - 1:
            edge = jnp.broadcast_to(z_upper[step % 2, j, pl.ds(r, ROWS)], mid.shape)
        else:
            edge = pltpu.roll(buf[j, rows, levels(chunk + 1), :], TILE - 1, 1)
        k_upper = jnp.where(k == TILE - 1, edge, pltpu.roll(mid, TILE - 1, 1))
        if inward is None:
            across = buf[j - 1, rows, here, :] + buf[j + 1, rows, here, :]
        else:
            across = buf[inward, rows, here, :]
        spread = (
            across + buf[j, pl.ds(r, ROWS), here, :] + buf[j, pl.ds(2 + r, ROWS), here, :]
            + k_lower + k_upper - 6.0 * mid)
        return mid + cond[j, pl.ds(r, ROWS), here, :] * spread + sour[j, pl.ds(r, ROWS), here, :]

    zero = jnp.zeros((TILE, M), jnp.float32)

    def early_plane(step, chunk, j, inward):
        def body(b, totals):
            r = b * ROWS
            new = next_rows(step, chunk, j, r, inward)
            if step < STEPS - 1:
                field[(step + 1) % 2][j, pl.ds(1 + r, ROWS), levels(chunk), :] = new
                return totals
            end[j, pl.ds(r, ROWS), levels(chunk), :] = new
            return tally(new, totals)

        if step < STEPS - 1:
            lax.fori_loop(0, blocks, lambda b, _: body(b, 0), 0)
        else:
            totals = lax.fori_loop(0, blocks, body, (zero, zero))
            for q in range(2):
                sums_early[j - first, q, levels(chunk), :] = totals[q]

    def early_part(step, chunk):
        @pl.loop(1, J - 1)
        def _(j):
            early_plane(step, chunk, j, None)

        if step == STEPS - 1 and chunk == max(chunks - 2, 0):
            for held in range(stay):
                for s in range(len(sides)):
                    y_start(step, held, s, odd_lon)
        if n_lat == 2:
            early_plane(step, chunk, jnp.where(lat == 0, 0, J - 1), jnp.where(lat == 0, 1, J - 2))

    def base_part(step, chunk):
        for s, (plane, inward, _, _, _) in enumerate(sides):
            @pl.loop(0, blocks)
            def _(b):
                r = b * ROWS
                base[s, pl.ds(r, ROWS), levels(chunk), :] = next_rows(step, chunk, plane, r, inward)

    def late_part(step, chunk, s):
        plane = sides[s][0]
        here, turn = levels(chunk), math.gcd(I, TURN)

        def body(b, totals):
            r = pl.ds(b * turn, turn)
            new = base[s, r, here, :] + cond[plane, r, here, :] * y_halo[step % 2, s, r, here, :]
            if step < STEPS - 1:
                field[(step + 1) % 2][plane, pl.ds(1 + b * turn, turn), here, :] = new
                if step == STEPS - 2:
                    for out, (low, high) in zip(outs, cuts):
                        if low <= chunk * TILE < high:
                            out[s, r, pl.ds(chunk * TILE - low, TILE), :] = new
                return totals
            end[plane, r, here, :] = new
            return tally(new, totals)

        if step < STEPS - 1:
            lax.fori_loop(0, I // turn, lambda b, _: body(b, 0), 0)
        else:
            totals = lax.fori_loop(0, I // turn, body, (zero, zero))
            for q in range(2):
                sums_late[chunk, s, q] = totals[q]

    def y_start(step, chunk, s, condition=None):
        exists = sides[s][3]
        if condition is not None and exists is not None:
            condition = jnp.logical_and(condition, exists)
        when(exists if condition is None else condition, lambda: y_copy(step, chunk, s).start())

    @pl.when(even_lat)
    def _():
        pl.semaphore_wait(peer_in, around)
        pl.when(lat < n_lat - 1)(lambda: pl.semaphore_signal(
            all_in, inc=1, device_id={"lat": lat + 1}, device_id_type=MESH))

    @pl.when(jnp.logical_not(even_lat))
    def _():
        pl.semaphore_wait(all_in, 1)

    loads[0].wait()
    for part in range(len(faces)):
        pack_and_send(0, part)
    loads[1].wait()
    loads[2].wait()
    for step in range(STEPS):
        last = step == STEPS - 1
        if step >= 1:
            faces_sent(step - 1)
        faces_arrive(step, 0)
        for chunk in range(chunks):
            early_part(step, chunk)
        if last:
            for shift in range(1, n_lon):
                early_copy(shift).start()
        else:
            pack_and_send(step + 1, 0)
        for part in range(1, len(faces)):
            faces_arrive(step, part)
        for chunk in range(chunks):
            base_part(step, chunk)
        if step == 1:
            for s, side in enumerate(sides):
                when(side[3], lambda: head_copy(s, side[4]).wait_send())
        if step >= 1:
            for s, side in enumerate(sides):
                for chunk in range(chunks):
                    when(side[3], lambda: y_copy(step - 1, chunk, s).wait_send())
        if last:
            for s, side in enumerate(sides):
                @pl.loop(0, blocks)
                def _(b):
                    rows = pl.ds(b * ROWS, ROWS)
                    factor[s, rows] = cond[side[0], rows, pl.ds(stay * TILE, K - stay * TILE), :]
            faces_sent(step)
            for shift in range(1, n_lon):
                early_copy(shift).wait_recv()

            @pl.loop(0, number)
            def _(p):
                total = [sums_early[p, q] for q in range(2)]
                for shift in range(1, n_lon):
                    total = [total[q] + peer_early[shift - 1, p, q] for q in range(2)]
                mean_out[first + p], scale_out[first + p] = close(total, count)

            for shift in range(1, n_lon):
                early_copy(shift).wait_send()
        for chunk in range(stay if last else chunks):
            for s, side in enumerate(sides):
                if step == 0 and chunk == 0:
                    when(side[3], lambda: head_copy(s, s).wait_recv())
                when(side[3], lambda: y_arrival(step, chunk, s).wait_recv())
                late_part(step, chunk, s)
                if step < STEPS - 2:
                    y_start(step + 1, chunk, s)
                elif not last and chunk < stay:
                    y_start(step + 1, chunk, s, jnp.logical_not(odd_lon))
        if not last:
            for part in range(1, len(faces)):
                pack_and_send(step + 1, part)
    for s, side in enumerate(sides):
        for chunk in range(stay):
            when(side[3], lambda: y_copy(STEPS - 1, chunk, s).wait_send())


def finish(sizes, base, factor, sums_in, end, out, *rest):
    halos, (
        tail, ready, mean_out, scale_out, landing, sums, peer_sums, late_in, y_send, y_recv, send_sem, recv_sem,
    ) = rest[:-12], rest[-12:]
    n_lat, n_lon, _ = sizes
    late, I, K, M = base.shape
    chunks, stay, cuts = K // TILE, kept(K), spans(K)
    lat, lon = lax.axis_index("lat"), lax.axis_index("lon")
    even_lon = lon % 2 == 0
    n_odd = n_lon // 2
    sides = lat_sides(n_lat, lat, end.shape[0])
    peers = [lax.rem(lon + shift, n_lon) for shift in range(1, n_lon)]
    groups = [group for group in (list(range(stay)), list(range(stay, chunks - 1)), [chunks - 1]) if group]
    pieces = [pl.ds(group[0], len(group)) for group in groups]

    def y_copy(s, slot):
        return pltpu.make_async_remote_copy(
            src_ref=out.at[s], dst_ref=landing.at[slot], send_sem=y_send.at[s], recv_sem=y_recv.at[slot],
            device_id={"lat": sides[s][2]}, device_id_type=MESH)

    def sum_copy(piece, p):
        return pltpu.make_async_remote_copy(
            src_ref=sums.at[pieces[piece]], dst_ref=peer_sums.at[p, pieces[piece]],
            send_sem=send_sem.at[piece, p], recv_sem=recv_sem.at[piece, p],
            device_id={"lon": peers[p]}, device_id_type=MESH)

    def send_sums(piece):
        for p in range(n_lon - 1):
            sum_copy(piece, p).start()

    def add(chunk, s, arrived, start):
        here = pl.ds(chunk * TILE, TILE)
        there, came = pl.ds((chunk - stay) * TILE, TILE), pl.ds(chunk * TILE - start, TILE)
        zero, turn = jnp.zeros((TILE, M), jnp.float32), math.gcd(I, TURN)

        def body(b, totals):
            r = pl.ds(b * turn, turn)
            new = base[s, r, here, :] + factor[s, r, there, :] * arrived[s, r, came, :]
            tail[s, r, there, :] = new
            return tally(new, totals)

        totals = lax.fori_loop(0, I // turn, body, (zero, zero))
        for q in range(2):
            sums[chunk, s, q] = totals[q]

    barrier = pltpu.get_barrier_semaphore()
    met = jnp.where(even_lon, n_lon - n_odd - 1, n_lon - 1)
    for _, _, peer, exists, _ in sides:
        when(exists, lambda: pl.semaphore_signal(
            barrier, inc=1, device_id={"lat": peer}, device_id_type=MESH))
        met = met + (1 if exists is None else exists.astype(jnp.int32))
    for peer in peers:
        pl.when(jnp.logical_or(even_lon, peer % 2 == 1))(lambda: pl.semaphore_signal(
            barrier, inc=1, device_id={"lon": peer}, device_id_type=MESH))
    pl.semaphore_wait(barrier, met)
    for s, side in enumerate(sides):
        when(side[3], lambda: y_copy(s, side[4]).start())

    @pl.when(jnp.logical_not(even_lon))
    def _():
        for peer in peers:
            pl.when(peer % 2 == 0)(lambda: pl.semaphore_signal(
                late_in, inc=1, device_id={"lon": peer}, device_id_type=MESH))

    for s, side in enumerate(sides):
        if side[3] is not None:
            @pl.when(jnp.logical_not(side[3]))
            def _():
                @pl.loop(0, I // ROWS)
                def _(b):
                    landing[s, pl.ds(b * ROWS, ROWS)] = jnp.zeros((ROWS,) + landing.shape[2:], jnp.float32)
        for chunk in range(chunks - 1):
            if chunk < stay:
                for q in range(2):
                    sums[chunk, s, q] = sums_in[chunk, s, q]
            else:
                add(chunk, s, halos[0], cuts[0][0])
    pl.when(even_lon)(lambda: pl.semaphore_wait(late_in, n_odd))
    values = {}

    def settle(piece):
        for p in range(n_lon - 1):
            sum_copy(piece, p).wait_recv()
        for chunk in groups[piece]:
            of_sides = []
            for s in range(late):
                total = [sums[chunk, s, q] for q in range(2)]
                for p in range(n_lon - 1):
                    total = [total[q] + peer_sums[p, chunk, s, q] for q in range(2)]
                of_sides.append(close(total, I * n_lon))
            values[chunk] = [jnp.stack(part) for part in zip(*of_sides)]

    for piece in range(len(groups) - 1):
        send_sums(piece)
    for piece, group in enumerate(groups[:-1]):
        settle(piece)
        for chunk in group:
            here = pl.ds(chunk * TILE, TILE)
            for s, side in enumerate(sides):
                offset, scaling = values[chunk][0][s], values[chunk][1][s]

                @pl.loop(0, I // ROWS)
                def _(b):
                    r = pl.ds(b * ROWS, ROWS)
                    if chunk < stay:
                        new = end[side[0], r, here, :]
                    else:
                        new = tail[s, r, pl.ds((chunk - stay) * TILE, TILE), :]
                    ready[s, r, here, :] = (new - offset) * scaling
        for p in range(n_lon - 1):
            sum_copy(piece, p).wait_send()
    for s, side in enumerate(sides):
        when(side[3], lambda: y_copy(s, s).wait_recv())
        add(chunks - 1, s, landing, (chunks - 1) * TILE)
    send_sums(len(groups) - 1)
    for s, side in enumerate(sides):
        when(side[3], lambda: y_copy(s, side[4]).wait_send())

    settle(len(groups) - 1)
    mean_out[...], scale_out[...] = values[chunks - 1]
    for p in range(n_lon - 1):
        sum_copy(len(groups) - 1, p).wait_send()


def write_early(sizes, end, mean, scale, standardized, end_out, held, sem):
    J, I, K, M = end.shape
    lat = lax.axis_index("lat")
    first, number = early_planes(sizes[0], lat, J)
    done = pl.ds(0, kept(K) * TILE)
    copies = [pltpu.make_async_copy(
        end.at[pl.ds(first, number)], end_out.at[pl.ds(first, number)], sem.at[number])]
    for s, side in enumerate(lat_sides(sizes[0], lat, J)):
        copies.append(pltpu.make_async_copy(
            end.at[side[0], :, done, :], end_out.at[side[0], :, done, :], sem.at[number + 1 + s]))
    for copy in copies:
        copy.start()
    for p in range(number):
        j = first + p
        offset, factor = mean[j], scale[j]

        @pl.loop(0, I // ROWS)
        def _(b):
            rows = pl.ds(b * ROWS, ROWS)
            held[p, rows] = (end[j, rows] - offset) * factor

        copies.append(pltpu.make_async_copy(held.at[p], standardized.at[j], sem.at[p]))
        copies[-1].start()
    for copy in copies:
        copy.wait()


def write_late(
    sizes, ready, tail, mean, scale, old_standardized, old_end, standardized, end_out, held, sem,
):
    J, K = end_out.shape[0], end_out.shape[2]
    late, I, high, M = tail.shape
    copies = []
    for s, side in enumerate(lat_sides(sizes[0], lax.axis_index("lat"), J)):
        j = side[0]

        def copy(source, target, rows, n):
            copies.append(pltpu.make_async_copy(source, target.at[j, :, rows, :], sem.at[s, n]))
            copies[-1].start()

        copy(ready.at[s], standardized, pl.ds(0, K - TILE), 0)
        copy(tail.at[s], end_out, pl.ds(K - high, high), 1)
        offset, scaling = mean[s], scale[s]

        @pl.loop(0, I // ROWS)
        def _(b):
            rows = pl.ds(b * ROWS, ROWS)
            held[s, rows] = (tail[s, rows, pl.ds(high - TILE, TILE), :] - offset) * scaling

        copy(held.at[s], standardized, pl.ds(K - TILE, TILE), 2)
    for copy in copies:
        copy.wait()


def cross(sizes, block):
    n_lat = sizes[0]
    if n_lat == 2:
        return lax.ppermute(block, "lat", [(0, 1), (1, 0)])
    up = lax.ppermute(block[1:], "lat", [(a, a + 1) for a in range(n_lat - 1)])
    down = lax.ppermute(block[:1], "lat", [(a + 1, a) for a in range(n_lat - 1)])
    return jnp.concatenate([up, down])


def shards(sizes, tracer, conductance, source):
    n_lat, n_lon, n_lev = sizes
    J, I, K, M = tracer.shape
    chunks = K // TILE
    f32 = jnp.float32
    dma = pltpu.SemaphoreType.DMA
    peers = max(n_lon - 1, 1)
    late = len(lat_sides(n_lat, 0, J))
    early = early_planes(n_lat, 0, J)[1]
    stay = kept(K)
    hbm, vmem = pl.BlockSpec(memory_space=pltpu.HBM), pl.BlockSpec(memory_space=pltpu.VMEM)
    cuts = spans(K)
    scratch = [
        (J, I + 2, K, M), (J, I + 2, K, M), (J, I, K, M), (J, I, K, M), (2, late, I, K, M),
        (2, J, I, 1, M), (2, J, I, 1, M), (2, J, I, 1, M), (2, J, I, 1, M),
        (early, 2, K, M), (peers, early, 2, K, M),
    ]
    limit = sum(4 * math.prod(shape) for shape in scratch) + (2 << 20)
    end, mean, scale, base, factor, sums, *outs = pl.pallas_call(
        functools.partial(kernel, sizes),
        out_shape=[
            pltpu.VMEM((J, I, K, M), f32),
            pltpu.VMEM((J, K, M), f32),
            pltpu.VMEM((J, K, M), f32),
            pltpu.VMEM((late, I, K, M), f32),
            pltpu.VMEM((late, I, K - stay * TILE, M), f32),
            pltpu.VMEM((stay, late, 2, TILE, M), f32),
        ] + [pltpu.VMEM((late, I, high - low, M), f32) for low, high in cuts],
        in_specs=[hbm] * 3,
        out_specs=[vmem] * (6 + len(cuts)),
        scratch_shapes=[pltpu.VMEM(shape, f32) for shape in scratch] + [
            pltpu.SemaphoreType.REGULAR,
            pltpu.SemaphoreType.REGULAR,
            dma((3,)),
            dma((chunks, late)),
            dma((late,)),
            dma((late,)),
            dma((late,)),
            dma((2, chunks, late)),
            dma((2, chunks, late)),
            dma((2, 2, 1 + late)),
            dma((2, 2, 1 + late)),
            dma((2, 2, 1 + late)),
            dma((2, 2, 1 + late)),
            dma((peers,)),
            dma((peers,)),
        ],
        compiler_params=pltpu.CompilerParams(
            collective_id=0, has_side_effects=True, vmem_limit_bytes=limit),
    )(tracer, conductance, source)
    halos = [cross(sizes, out) for out in outs[:-1]]
    whole = jax.ShapeDtypeStruct((J, I, K, M), f32)

    standardized, end_out = pl.pallas_call(
        functools.partial(write_early, sizes),
        out_shape=[whole] * 2,
        in_specs=[vmem] * 3,
        out_specs=[hbm] * 2,
        scratch_shapes=[pltpu.VMEM((early, I, K, M), f32), dma((early + 1 + late,))],
        compiler_params=pltpu.CompilerParams(vmem_limit_bytes=16 << 20),
        cost_estimate=pl.CostEstimate(
            flops=1 << 32, bytes_accessed=8 * early * I * K * M, transcendentals=0),
    )(end, mean, scale)
    out_of = (late, I, K - stay * TILE, M)
    tail, ready, mean, scale = pl.pallas_call(
        functools.partial(finish, sizes),
        out_shape=[pltpu.VMEM(out_of, f32), pltpu.VMEM((late, I, K - TILE, M), f32)]
        + [pltpu.VMEM((late, TILE, M), f32)] * 2,
        in_specs=[vmem] * (5 + len(halos)),
        out_specs=[vmem] * 4,
        scratch_shapes=[
            pltpu.VMEM((late, I, TILE, M), f32),
            pltpu.VMEM((chunks, late, 2, TILE, M), f32),
            pltpu.VMEM((peers, chunks, late, 2, TILE, M), f32),
            pltpu.SemaphoreType.REGULAR,
            dma((late,)),
            dma((late,)),
            dma((3, peers)),
            dma((3, peers)),
        ],
        compiler_params=pltpu.CompilerParams(
            collective_id=1, has_side_effects=True, vmem_limit_bytes=8 << 20),
    )(base, factor, sums, end, outs[-1], *halos)
    return pl.pallas_call(
        functools.partial(write_late, sizes),
        out_shape=[whole] * 2,
        in_specs=[vmem] * 4 + [hbm] * 2,
        out_specs=[hbm] * 2,
        input_output_aliases={4: 0, 5: 1},
        scratch_shapes=[pltpu.VMEM((late, I, TILE, M), f32), dma((late, 3))],
        compiler_params=pltpu.CompilerParams(vmem_limit_bytes=12 << 20),
    )(ready, tail, mean, scale, standardized, end_out)


def solution(mesh):
    placed = P("lat", "lon", "lev", None)
    sizes = tuple(mesh.shape[axis] for axis in ("lat", "lon", "lev"))
    return jax.shard_map(
        functools.partial(shards, sizes),
        mesh=mesh,
        in_specs=(placed, placed, placed),
        out_specs=(placed, placed),
        check_vma=False,
    )
```

```python
import functools
import math

import jax
import jax.numpy as jnp
from jax import lax
from jax.experimental import pallas as pl
from jax.experimental.pallas import tpu as pltpu
from jax.sharding import PartitionSpec as P

STEPS = 3
GUESS = 1.0
TILE = 8
ROWS = 8
TURN = 32
MESH = pl.DeviceIdType.MESH


def lat_sides(n_lat, lat, J):
    if n_lat == 2:
        return [(jnp.where(lat == 0, J - 1, 0), jnp.where(lat == 0, J - 2, 1), 1 - lat, None, 0)]
    return [(0, 1, lat - 1, lat > 0, 1), (J - 1, J - 2, lat + 1, lat < n_lat - 1, 0)]


def early_planes(n_lat, lat, J):
    if n_lat == 2:
        return jnp.where(lat == 0, 0, 1), J - 1
    return 1, J - 2


def kept(K):
    return K // TILE // 2


def spans(K):
    start, last = kept(K) * TILE, K - TILE
    return [(low, high) for low, high in ((start, last), (last, K)) if high > low]


def close(total, count):
    offset = total[0] / count
    variance = total[1] / count - offset * offset
    return GUESS + offset, lax.rsqrt(variance + 0.0001)


def tally(new, totals):
    moved = new - GUESS
    return totals[0] + jnp.sum(moved, axis=0), totals[1] + jnp.sum(moved * moved, axis=0)


def when(condition, act):
    if condition is None:
        act()
    else:
        pl.when(condition)(act)


def kernel(sizes, tracer, conductance, source, end, mean_out, scale_out, base, factor, sums_late, *rest):
    cuts = spans(tracer.shape[2])
    outs = rest[:len(cuts)]
    (
        even, odd, cond, sour, y_halo, z_lower, z_upper, z_first, z_last, sums_early, peer_early,
        peer_in, all_in,
        load_sem, first_sem, head_sem, head_send, head_recv, y_send, y_recv, x_send, x_recv, z_send, z_recv, early_send, early_recv,
    ) = rest[len(cuts):]
    n_lat, n_lon, n_lev = sizes
    J, I, K, M = tracer.shape
    chunks = K // TILE
    blocks = I // ROWS
    count = I * n_lon
    lat, lon, lev = lax.axis_index("lat"), lax.axis_index("lon"), lax.axis_index("lev")
    below = {"lon": lon > 0, "lev": lev > 0}
    above = {"lon": lon < n_lon - 1, "lev": lev < n_lev - 1}
    index = {"lon": lon, "lev": lev}
    field = [even, odd]
    sides = lat_sides(n_lat, lat, J)
    first, number = early_planes(n_lat, lat, J)
    stay = kept(K)
    odd_lon = lon % 2 == 1
    rows_in = pl.ds(1, I)

    def levels(chunk):
        return pl.ds(chunk * TILE, TILE)

    def target(axis, way):
        return {axis: index[axis] + (1 if way == 0 else -1)}

    def y_copy(step, chunk, s):
        plane, _, peer, _, slot = sides[s]
        skip = I // 4 if step == 0 and chunk == 0 else 0
        rows = pl.ds(skip, I - skip)
        return pltpu.make_async_remote_copy(
            src_ref=field[step % 2].at[plane, pl.ds(1 + skip, I - skip), levels(chunk), :],
            dst_ref=y_halo.at[step % 2, slot, rows, levels(chunk), :],
            send_sem=y_send.at[step % 2, chunk, s], recv_sem=y_recv.at[step % 2, chunk, slot],
            device_id={"lat": peer}, device_id_type=MESH)

    def y_arrival(step, chunk, s):
        plane, _, peer, _, _ = sides[s]
        skip = I // 4 if step == 0 and chunk == 0 else 0
        rows = pl.ds(skip, I - skip)
        return pltpu.make_async_remote_copy(
            src_ref=field[step % 2].at[plane, pl.ds(1 + skip, I - skip), levels(chunk), :],
            dst_ref=y_halo.at[step % 2, s, rows, levels(chunk), :],
            send_sem=y_send.at[step % 2, chunk, s], recv_sem=y_recv.at[step % 2, chunk, s],
            device_id={"lat": peer}, device_id_type=MESH)

    faces = [pl.ds(first, number)] + [pl.ds(side[0], 1) for side in sides]

    head = pl.ds(0, I // 4)

    def head_load(s):
        return pltpu.make_async_copy(
            tracer.at[sides[s][0], head, levels(0), :], even.at[sides[s][0], pl.ds(1, I // 4), levels(0), :],
            head_sem.at[s])

    def head_copy(s, slot):
        plane, _, peer, _, _ = sides[s]
        return pltpu.make_async_remote_copy(
            src_ref=even.at[plane, pl.ds(1, I // 4), levels(0), :], dst_ref=y_halo.at[0, slot, head, levels(0), :],
            send_sem=head_send.at[s], recv_sem=head_recv.at[slot],
            device_id={"lat": peer}, device_id_type=MESH)

    def x_copy(step, way, part):
        buf = field[step % 2]
        return pltpu.make_async_remote_copy(
            src_ref=buf.at[faces[part], I if way == 0 else 1],
            dst_ref=buf.at[faces[part], 0 if way == 0 else I + 1],
            send_sem=x_send.at[step % 2, way, part], recv_sem=x_recv.at[step % 2, way, part],
            device_id=target("lon", way), device_id_type=MESH)

    def z_copy(step, way, part):
        src = z_last if way == 0 else z_first
        dst = z_lower if way == 0 else z_upper
        return pltpu.make_async_remote_copy(
            src_ref=src.at[step % 2, faces[part]], dst_ref=dst.at[step % 2, faces[part]],
            send_sem=z_send.at[step % 2, way, part], recv_sem=z_recv.at[step % 2, way, part],
            device_id=target("lev", way), device_id_type=MESH)

    def early_copy(shift):
        return pltpu.make_async_remote_copy(
            src_ref=sums_early, dst_ref=peer_early.at[shift - 1],
            send_sem=early_send.at[shift - 1], recv_sem=early_recv.at[shift - 1],
            device_id={"lon": lax.rem(lon + shift, n_lon)}, device_id_type=MESH)

    def sends(axis, way, act):
        pl.when((above if way == 0 else below)[axis])(act)

    def arrives(axis, way, act):
        pl.when((below if way == 0 else above)[axis])(act)

    def first_load(chunk, s):
        skip = I // 4 if chunk == 0 else 0
        return pltpu.make_async_copy(
            tracer.at[sides[s][0], pl.ds(skip, I - skip), levels(chunk), :],
            even.at[sides[s][0], pl.ds(1 + skip, I - skip), levels(chunk), :], first_sem.at[chunk, s])

    first_loads = [[first_load(chunk, s) for s in range(len(sides))] for chunk in range(chunks)]
    for s in range(len(sides)):
        head_load(s).start()
    loads = [
        pltpu.make_async_copy(
            tracer.at[pl.ds(first, number)], even.at[pl.ds(first, number), rows_in], load_sem.at[0]),
        pltpu.make_async_copy(conductance, cond, load_sem.at[1]),
        pltpu.make_async_copy(source, sour, load_sem.at[2]),
    ]
    for chunk in range(chunks):
        for load in first_loads[chunk]:
            load.start()
    even_lat = lat % 2 == 0
    around = n_lon - 1 + below["lev"].astype(jnp.int32) + above["lev"].astype(jnp.int32)
    met = jnp.where(even_lat, around, 0)
    barrier = pltpu.get_barrier_semaphore()

    def signal_around(semaphore):
        for shift in range(1, n_lon):
            pl.semaphore_signal(semaphore, inc=1, device_id={"lon": lax.rem(lon + shift, n_lon)},
                                device_id_type=MESH)
        for way in (0, 1):
            sends("lev", way, lambda: pl.semaphore_signal(
                semaphore, inc=1, device_id=target("lev", way), device_id_type=MESH))

    for _, _, peer, exists, _ in sides:
        when(exists, lambda: pl.semaphore_signal(
            barrier, inc=1, device_id={"lat": peer}, device_id_type=MESH))
        met = met + (1 if exists is None else exists.astype(jnp.int32))
    pl.when(even_lat)(lambda: signal_around(barrier))
    loads[0].start()
    pl.semaphore_wait(barrier, met)

    for s, side in enumerate(sides):
        head_load(s).wait()
        when(side[3], lambda: head_copy(s, side[4]).start())
    for chunk in range(chunks):
        for s, side in enumerate(sides):
            first_loads[chunk][s].wait()
            when(side[3], lambda: y_copy(0, chunk, s).start())
    loads[1].start()
    loads[2].start()

    @pl.when(even_lat)
    def _():
        signal_around(peer_in)

    for s, side in enumerate(sides):
        if side[3] is not None:
            def no_y():
                @pl.loop(0, blocks)
                def _(b):
                    for p in range(2):
                        y_halo[p, s, pl.ds(b * ROWS, ROWS)] = jnp.zeros((ROWS, K, M), jnp.float32)
            pl.when(jnp.logical_not(side[3]))(no_y)
    for way in (0, 1):
        def no_x():
            for buf in field:
                for j in range(J):
                    buf[j, 0 if way == 0 else I + 1] = jnp.zeros((K, M), jnp.float32)
        pl.when(jnp.logical_not((below if way == 0 else above)["lon"]))(no_x)

        def no_z():
            @pl.loop(0, blocks)
            def _(b):
                for p in range(2):
                    for j in range(J):
                        (z_lower if way == 0 else z_upper)[p, j, pl.ds(b * ROWS, ROWS)] = (
                            jnp.zeros((ROWS, 1, M), jnp.float32))
        pl.when(jnp.logical_not((below if way == 0 else above)["lev"]))(no_z)

    def pack_and_send(step, part):
        buf = field[step % 2]
        start, extent = (first, number) if part == 0 else (sides[part - 1][0], 1)
        for way in (0, 1):
            sends("lon", way, lambda: x_copy(step, way, part).start())

        @pl.loop(0, extent * blocks)
        def _(q):
            j, r = start + q // blocks, (q % blocks) * ROWS
            z_first[step % 2, j, pl.ds(r, ROWS)] = buf[j, pl.ds(1 + r, ROWS), pl.ds(0, 1), :]
            z_last[step % 2, j, pl.ds(r, ROWS)] = buf[j, pl.ds(1 + r, ROWS), pl.ds(K - 1, 1), :]

        for way in (0, 1):
            sends("lev", way, lambda: z_copy(step, way, part).start())

    def faces_sent(step):
        for part in range(len(faces)):
            for way in (0, 1):
                sends("lon", way, lambda: x_copy(step, way, part).wait_send())
                sends("lev", way, lambda: z_copy(step, way, part).wait_send())

    def faces_arrive(step, part):
        for way in (0, 1):
            arrives("lon", way, lambda: x_copy(step, way, part).wait_recv())
            arrives("lev", way, lambda: z_copy(step, way, part).wait_recv())

    def next_rows(step, chunk, j, r, inward):
        buf = field[step % 2]
        here = levels(chunk)
        rows = pl.ds(1 + r, ROWS)
        mid = buf[j, rows, here, :]
        k = lax.broadcasted_iota(jnp.int32, mid.shape, 1)
        if chunk == 0:
            edge = jnp.broadcast_to(z_lower[step % 2, j, pl.ds(r, ROWS)], mid.shape)
        else:
            edge = pltpu.roll(buf[j, rows, levels(chunk - 1), :], 1, 1)
        k_lower = jnp.where(k == 0, edge, pltpu.roll(mid, 1, 1))
        if chunk == chunks - 1:
            edge = jnp.broadcast_to(z_upper[step % 2, j, pl.ds(r, ROWS)], mid.shape)
        else:
            edge = pltpu.roll(buf[j, rows, levels(chunk + 1), :], TILE - 1, 1)
        k_upper = jnp.where(k == TILE - 1, edge, pltpu.roll(mid, TILE - 1, 1))
        if inward is None:
            across = buf[j - 1, rows, here, :] + buf[j + 1, rows, here, :]
        else:
            across = buf[inward, rows, here, :]
        spread = (
            across + buf[j, pl.ds(r, ROWS), here, :] + buf[j, pl.ds(2 + r, ROWS), here, :]
            + k_lower + k_upper - 6.0 * mid)
        return mid + cond[j, pl.ds(r, ROWS), here, :] * spread + sour[j, pl.ds(r, ROWS), here, :]

    zero = jnp.zeros((TILE, M), jnp.float32)

    def early_plane(step, chunk, j, inward):
        def body(b, totals):
            r = b * ROWS
            new = next_rows(step, chunk, j, r, inward)
            if step < STEPS - 1:
                field[(step + 1) % 2][j, pl.ds(1 + r, ROWS), levels(chunk), :] = new
                return totals
            end[j, pl.ds(r, ROWS), levels(chunk), :] = new
            return tally(new, totals)

        if step < STEPS - 1:
            lax.fori_loop(0, blocks, lambda b, _: body(b, 0), 0)
        else:
            totals = lax.fori_loop(0, blocks, body, (zero, zero))
            for q in range(2):
                sums_early[j - first, q, levels(chunk), :] = totals[q]

    def early_part(step, chunk):
        @pl.loop(1, J - 1)
        def _(j):
            early_plane(step, chunk, j, None)

        if step == STEPS - 1 and chunk == max(chunks - 2, 0):
            for held in range(stay):
                for s in range(len(sides)):
                    y_start(step, held, s, odd_lon)
        if n_lat == 2:
            early_plane(step, chunk, jnp.where(lat == 0, 0, J - 1), jnp.where(lat == 0, 1, J - 2))

    def base_part(step, chunk):
        for s, (plane, inward, _, _, _) in enumerate(sides):
            @pl.loop(0, blocks)
            def _(b):
                r = b * ROWS
                base[s, pl.ds(r, ROWS), levels(chunk), :] = next_rows(step, chunk, plane, r, inward)

    def late_part(step, chunk, s):
        plane = sides[s][0]
        here, turn = levels(chunk), math.gcd(I, TURN)

        def body(b, totals):
            r = pl.ds(b * turn, turn)
            new = base[s, r, here, :] + cond[plane, r, here, :] * y_halo[step % 2, s, r, here, :]
            if step < STEPS - 1:
                field[(step + 1) % 2][plane, pl.ds(1 + b * turn, turn), here, :] = new
                if step == STEPS - 2:
                    for out, (low, high) in zip(outs, cuts):
                        if low <= chunk * TILE < high:
                            out[s, r, pl.ds(chunk * TILE - low, TILE), :] = new
                return totals
            end[plane, r, here, :] = new
            return tally(new, totals)

        if step < STEPS - 1:
            lax.fori_loop(0, I // turn, lambda b, _: body(b, 0), 0)
        else:
            totals = lax.fori_loop(0, I // turn, body, (zero, zero))
            for q in range(2):
                sums_late[chunk, s, q] = totals[q]

    def y_start(step, chunk, s, condition=None):
        exists = sides[s][3]
        if condition is not None and exists is not None:
            condition = jnp.logical_and(condition, exists)
        when(exists if condition is None else condition, lambda: y_copy(step, chunk, s).start())

    @pl.when(even_lat)
    def _():
        pl.semaphore_wait(peer_in, around)
        pl.when(lat < n_lat - 1)(lambda: pl.semaphore_signal(
            all_in, inc=1, device_id={"lat": lat + 1}, device_id_type=MESH))

    @pl.when(jnp.logical_not(even_lat))
    def _():
        pl.semaphore_wait(all_in, 1)

    loads[0].wait()
    for part in range(len(faces)):
        pack_and_send(0, part)
    loads[1].wait()
    loads[2].wait()
    for step in range(STEPS):
        last = step == STEPS - 1
        if step >= 1:
            faces_sent(step - 1)
        faces_arrive(step, 0)
        for chunk in range(chunks):
            early_part(step, chunk)
        if last:
            for shift in range(1, n_lon):
                early_copy(shift).start()
        else:
            pack_and_send(step + 1, 0)
        for part in range(1, len(faces)):
            faces_arrive(step, part)
        for chunk in range(chunks):
            base_part(step, chunk)
        if step == 1:
            for s, side in enumerate(sides):
                when(side[3], lambda: head_copy(s, side[4]).wait_send())
        if step >= 1:
            for s, side in enumerate(sides):
                for chunk in range(chunks):
                    when(side[3], lambda: y_copy(step - 1, chunk, s).wait_send())
        if last:
            for s, side in enumerate(sides):
                @pl.loop(0, blocks)
                def _(b):
                    rows = pl.ds(b * ROWS, ROWS)
                    factor[s, rows] = cond[side[0], rows, pl.ds(stay * TILE, K - stay * TILE), :]
            faces_sent(step)
            for shift in range(1, n_lon):
                early_copy(shift).wait_recv()

            @pl.loop(0, number)
            def _(p):
                total = [sums_early[p, q] for q in range(2)]
                for shift in range(1, n_lon):
                    total = [total[q] + peer_early[shift - 1, p, q] for q in range(2)]
                mean_out[first + p], scale_out[first + p] = close(total, count)

            for shift in range(1, n_lon):
                early_copy(shift).wait_send()
        for chunk in range(stay if last else chunks):
            for s, side in enumerate(sides):
                if step == 0 and chunk == 0:
                    when(side[3], lambda: head_copy(s, s).wait_recv())
                when(side[3], lambda: y_arrival(step, chunk, s).wait_recv())
                late_part(step, chunk, s)
                if step < STEPS - 2:
                    y_start(step + 1, chunk, s)
                elif not last and chunk < stay:
                    y_start(step + 1, chunk, s, jnp.logical_not(odd_lon))
        if not last:
            for part in range(1, len(faces)):
                pack_and_send(step + 1, part)
    for s, side in enumerate(sides):
        for chunk in range(stay):
            when(side[3], lambda: y_copy(STEPS - 1, chunk, s).wait_send())


def finish(sizes, base, factor, sums_in, end, out, *rest):
    halos, (
        tail, ready, mean_out, scale_out, landing, sums, peer_sums, late_in, y_send, y_recv, send_sem, recv_sem,
    ) = rest[:-12], rest[-12:]
    n_lat, n_lon, _ = sizes
    late, I, K, M = base.shape
    chunks, stay, cuts = K // TILE, kept(K), spans(K)
    lat, lon = lax.axis_index("lat"), lax.axis_index("lon")
    even_lon = lon % 2 == 0
    n_odd = n_lon // 2
    sides = lat_sides(n_lat, lat, end.shape[0])
    peers = [lax.rem(lon + shift, n_lon) for shift in range(1, n_lon)]
    groups = [group for group in (list(range(stay)), list(range(stay, chunks - 1)), [chunks - 1]) if group]
    pieces = [pl.ds(group[0], len(group)) for group in groups]

    def y_copy(s, slot):
        return pltpu.make_async_remote_copy(
            src_ref=out.at[s], dst_ref=landing.at[slot], send_sem=y_send.at[s], recv_sem=y_recv.at[slot],
            device_id={"lat": sides[s][2]}, device_id_type=MESH)

    def sum_copy(piece, p):
        return pltpu.make_async_remote_copy(
            src_ref=sums.at[pieces[piece]], dst_ref=peer_sums.at[p, pieces[piece]],
            send_sem=send_sem.at[piece, p], recv_sem=recv_sem.at[piece, p],
            device_id={"lon": peers[p]}, device_id_type=MESH)

    def send_sums(piece):
        for p in range(n_lon - 1):
            sum_copy(piece, p).start()

    def add(chunk, s, arrived, start):
        here = pl.ds(chunk * TILE, TILE)
        there, came = pl.ds((chunk - stay) * TILE, TILE), pl.ds(chunk * TILE - start, TILE)
        zero, turn = jnp.zeros((TILE, M), jnp.float32), math.gcd(I, TURN)

        def body(b, totals):
            r = pl.ds(b * turn, turn)
            new = base[s, r, here, :] + factor[s, r, there, :] * arrived[s, r, came, :]
            tail[s, r, there, :] = new
            return tally(new, totals)

        totals = lax.fori_loop(0, I // turn, body, (zero, zero))
        for q in range(2):
            sums[chunk, s, q] = totals[q]

    barrier = pltpu.get_barrier_semaphore()
    met = jnp.where(even_lon, 0, n_lon - 1)
    for _, _, peer, exists, _ in sides:
        when(exists, lambda: pl.semaphore_signal(
            barrier, inc=1, device_id={"lat": peer}, device_id_type=MESH))
        met = met + (1 if exists is None else exists.astype(jnp.int32))
    for peer in peers:
        pl.when(peer % 2 == 1)(lambda: pl.semaphore_signal(
            barrier, inc=1, device_id={"lon": peer}, device_id_type=MESH))
    pl.semaphore_wait(barrier, met)
    for s, side in enumerate(sides):
        when(side[3], lambda: y_copy(s, side[4]).start())

    @pl.when(jnp.logical_not(even_lon))
    def _():
        for peer in peers:
            pl.when(peer % 2 == 0)(lambda: pl.semaphore_signal(
                late_in, inc=1, device_id={"lon": peer}, device_id_type=MESH))

    for s, side in enumerate(sides):
        if side[3] is not None:
            @pl.when(jnp.logical_not(side[3]))
            def _():
                @pl.loop(0, I // ROWS)
                def _(b):
                    landing[s, pl.ds(b * ROWS, ROWS)] = jnp.zeros((ROWS,) + landing.shape[2:], jnp.float32)
        for chunk in range(chunks - 1):
            if chunk < stay:
                for q in range(2):
                    sums[chunk, s, q] = sums_in[chunk, s, q]
            else:
                add(chunk, s, halos[0], cuts[0][0])
    pl.when(even_lon)(lambda: pl.semaphore_wait(late_in, n_odd))
    values = {}

    def settle(piece):
        for p in range(n_lon - 1):
            sum_copy(piece, p).wait_recv()
        for chunk in groups[piece]:
            of_sides = []
            for s in range(late):
                total = [sums[chunk, s, q] for q in range(2)]
                for p in range(n_lon - 1):
                    total = [total[q] + peer_sums[p, chunk, s, q] for q in range(2)]
                of_sides.append(close(total, I * n_lon))
            values[chunk] = [jnp.stack(part) for part in zip(*of_sides)]

    for piece in range(len(groups) - 1):
        send_sums(piece)
    for piece, group in enumerate(groups[:-1]):
        settle(piece)
        for chunk in group:
            here = pl.ds(chunk * TILE, TILE)
            for s, side in enumerate(sides):
                offset, scaling = values[chunk][0][s], values[chunk][1][s]

                @pl.loop(0, I // ROWS)
                def _(b):
                    r = pl.ds(b * ROWS, ROWS)
                    if chunk < stay:
                        new = end[side[0], r, here, :]
                    else:
                        new = tail[s, r, pl.ds((chunk - stay) * TILE, TILE), :]
                    ready[s, r, here, :] = (new - offset) * scaling
        for p in range(n_lon - 1):
            sum_copy(piece, p).wait_send()
    for s, side in enumerate(sides):
        when(side[3], lambda: y_copy(s, s).wait_recv())
        add(chunks - 1, s, landing, (chunks - 1) * TILE)
    send_sums(len(groups) - 1)
    for s, side in enumerate(sides):
        when(side[3], lambda: y_copy(s, side[4]).wait_send())

    settle(len(groups) - 1)
    mean_out[...], scale_out[...] = values[chunks - 1]
    for p in range(n_lon - 1):
        sum_copy(len(groups) - 1, p).wait_send()


def write_early(sizes, end, mean, scale, standardized, end_out, held, sem):
    J, I, K, M = end.shape
    lat = lax.axis_index("lat")
    first, number = early_planes(sizes[0], lat, J)
    done = pl.ds(0, kept(K) * TILE)
    copies = [pltpu.make_async_copy(
        end.at[pl.ds(first, number)], end_out.at[pl.ds(first, number)], sem.at[number])]
    for s, side in enumerate(lat_sides(sizes[0], lat, J)):
        copies.append(pltpu.make_async_copy(
            end.at[side[0], :, done, :], end_out.at[side[0], :, done, :], sem.at[number + 1 + s]))
    for copy in copies:
        copy.start()
    for p in range(number):
        j = first + p
        offset, factor = mean[j], scale[j]

        @pl.loop(0, I // ROWS)
        def _(b):
            rows = pl.ds(b * ROWS, ROWS)
            held[p, rows] = (end[j, rows] - offset) * factor

        copies.append(pltpu.make_async_copy(held.at[p], standardized.at[j], sem.at[p]))
        copies[-1].start()
    for copy in copies:
        copy.wait()


def write_late(
    sizes, ready, tail, mean, scale, old_standardized, old_end, standardized, end_out, held, sem,
):
    J, K = end_out.shape[0], end_out.shape[2]
    late, I, high, M = tail.shape
    copies = []
    for s, side in enumerate(lat_sides(sizes[0], lax.axis_index("lat"), J)):
        j = side[0]

        def copy(source, target, rows, n):
            copies.append(pltpu.make_async_copy(source, target.at[j, :, rows, :], sem.at[s, n]))
            copies[-1].start()

        copy(ready.at[s], standardized, pl.ds(0, K - TILE), 0)
        copy(tail.at[s], end_out, pl.ds(K - high, high), 1)
        offset, scaling = mean[s], scale[s]

        @pl.loop(0, I // ROWS)
        def _(b):
            rows = pl.ds(b * ROWS, ROWS)
            held[s, rows] = (tail[s, rows, pl.ds(high - TILE, TILE), :] - offset) * scaling

        copy(held.at[s], standardized, pl.ds(K - TILE, TILE), 2)
    for copy in copies:
        copy.wait()


def cross(sizes, block):
    n_lat = sizes[0]
    if n_lat == 2:
        return lax.ppermute(block, "lat", [(0, 1), (1, 0)])
    up = lax.ppermute(block[1:], "lat", [(a, a + 1) for a in range(n_lat - 1)])
    down = lax.ppermute(block[:1], "lat", [(a + 1, a) for a in range(n_lat - 1)])
    return jnp.concatenate([up, down])


def shards(sizes, tracer, conductance, source):
    n_lat, n_lon, n_lev = sizes
    J, I, K, M = tracer.shape
    chunks = K // TILE
    f32 = jnp.float32
    dma = pltpu.SemaphoreType.DMA
    peers = max(n_lon - 1, 1)
    late = len(lat_sides(n_lat, 0, J))
    early = early_planes(n_lat, 0, J)[1]
    stay = kept(K)
    hbm, vmem = pl.BlockSpec(memory_space=pltpu.HBM), pl.BlockSpec(memory_space=pltpu.VMEM)
    cuts = spans(K)
    scratch = [
        (J, I + 2, K, M), (J, I + 2, K, M), (J, I, K, M), (J, I, K, M), (2, late, I, K, M),
        (2, J, I, 1, M), (2, J, I, 1, M), (2, J, I, 1, M), (2, J, I, 1, M),
        (early, 2, K, M), (peers, early, 2, K, M),
    ]
    limit = sum(4 * math.prod(shape) for shape in scratch) + (2 << 20)
    end, mean, scale, base, factor, sums, *outs = pl.pallas_call(
        functools.partial(kernel, sizes),
        out_shape=[
            pltpu.VMEM((J, I, K, M), f32),
            pltpu.VMEM((J, K, M), f32),
            pltpu.VMEM((J, K, M), f32),
            pltpu.VMEM((late, I, K, M), f32),
            pltpu.VMEM((late, I, K - stay * TILE, M), f32),
            pltpu.VMEM((stay, late, 2, TILE, M), f32),
        ] + [pltpu.VMEM((late, I, high - low, M), f32) for low, high in cuts],
        in_specs=[hbm] * 3,
        out_specs=[vmem] * (6 + len(cuts)),
        scratch_shapes=[pltpu.VMEM(shape, f32) for shape in scratch] + [
            pltpu.SemaphoreType.REGULAR,
            pltpu.SemaphoreType.REGULAR,
            dma((3,)),
            dma((chunks, late)),
            dma((late,)),
            dma((late,)),
            dma((late,)),
            dma((2, chunks, late)),
            dma((2, chunks, late)),
            dma((2, 2, 1 + late)),
            dma((2, 2, 1 + late)),
            dma((2, 2, 1 + late)),
            dma((2, 2, 1 + late)),
            dma((peers,)),
            dma((peers,)),
        ],
        compiler_params=pltpu.CompilerParams(
            collective_id=0, has_side_effects=True, vmem_limit_bytes=limit),
    )(tracer, conductance, source)
    halos = [cross(sizes, out) for out in outs[:-1]]
    whole = jax.ShapeDtypeStruct((J, I, K, M), f32)

    standardized, end_out = pl.pallas_call(
        functools.partial(write_early, sizes),
        out_shape=[whole] * 2,
        in_specs=[vmem] * 3,
        out_specs=[hbm] * 2,
        scratch_shapes=[pltpu.VMEM((early, I, K, M), f32), dma((early + 1 + late,))],
        compiler_params=pltpu.CompilerParams(vmem_limit_bytes=16 << 20),
        cost_estimate=pl.CostEstimate(
            flops=1 << 32, bytes_accessed=8 * early * I * K * M, transcendentals=0),
    )(end, mean, scale)
    out_of = (late, I, K - stay * TILE, M)
    tail, ready, mean, scale = pl.pallas_call(
        functools.partial(finish, sizes),
        out_shape=[pltpu.VMEM(out_of, f32), pltpu.VMEM((late, I, K - TILE, M), f32)]
        + [pltpu.VMEM((late, TILE, M), f32)] * 2,
        in_specs=[vmem] * (5 + len(halos)),
        out_specs=[vmem] * 4,
        scratch_shapes=[
            pltpu.VMEM((late, I, TILE, M), f32),
            pltpu.VMEM((chunks, late, 2, TILE, M), f32),
            pltpu.VMEM((peers, chunks, late, 2, TILE, M), f32),
            pltpu.SemaphoreType.REGULAR,
            dma((late,)),
            dma((late,)),
            dma((3, peers)),
            dma((3, peers)),
        ],
        compiler_params=pltpu.CompilerParams(
            collective_id=1, has_side_effects=True, vmem_limit_bytes=8 << 20),
    )(base, factor, sums, end, outs[-1], *halos)
    return pl.pallas_call(
        functools.partial(write_late, sizes),
        out_shape=[whole] * 2,
        in_specs=[vmem] * 4 + [hbm] * 2,
        out_specs=[hbm] * 2,
        input_output_aliases={4: 0, 5: 1},
        scratch_shapes=[pltpu.VMEM((late, I, TILE, M), f32), dma((late, 3))],
        compiler_params=pltpu.CompilerParams(vmem_limit_bytes=12 << 20),
    )(ready, tail, mean, scale, standardized, end_out)


def solution(mesh):
    placed = P("lat", "lon", "lev", None)
    sizes = tuple(mesh.shape[axis] for axis in ("lat", "lon", "lev"))
    return jax.shard_map(
        functools.partial(shards, sizes),
        mesh=mesh,
        in_specs=(placed, placed, placed),
        out_specs=(placed, placed),
        check_vma=False,
    )
```
